64 devices in a mesh: dp: 4 (over x, y), sp: 16 (over z, core).
Axes of the slice: x: 2, y: 2, z: 8, core: 2. Of those that a mesh axis runs over, the one named last changes fastest.
The devices are a block of a 4x4x8 slice.
Arguments:
- hidden: bfloat16 [8192, 4096], P(('dp', 'sp')), parts along dimension 0
- ln_gain: bfloat16 [4096], replicated
- w_q: bfloat16 [4096, 4096], replicated
- w_k: bfloat16 [4096, 1024], replicated
- w_v: bfloat16 [4096, 1024], replicated
- w_o: bfloat16 [4096, 4096], replicated
- q_gain: bfloat16 [128], replicated
- k_gain: bfloat16 [128], replicated
Outputs:
- output: bfloat16 [8192, 4096], P(('dp', 'sp')), parts along dimension 0
There are 4 independent parts. The reference program is written for one: setup_inputs(seed, part) draws one part's arguments, and reference() takes and returns one part's arrays. A program takes and returns all parts, laid end to end along the dimension named above; an argument that names none is the same for every part.
All inputs are finite; a program needn't handle non-finite values.
Results may differ from the reference program's by a relative error of at most 0.00695388.
Values are sent between devices in bfloat16 or wider.
A program may use at most 768 MiB of HBM per device.

```python
import math
import jax
import jax.numpy as jnp
from jax import lax

D = 4096
HEADS = 32
KV_HEADS = 8
HEAD = 128
SEQ = 2048
EPS = 1e-6
THETA = 1000000.0


def setup_inputs(seed: int = 0, part: int = 0) -> dict:
    keys = jax.random.split(jax.random.key(seed), 7)
    part_key = jax.random.fold_in(jax.random.key(seed + 1), part)
    gain_scale = math.log(SEQ / 8.0) ** 0.25
    hidden = jax.random.normal(part_key, (SEQ, D), jnp.float32)
    ln_gain = 1.0 + 0.3 * jax.random.normal(keys[0], (D,), jnp.float32)
    w_q = jax.random.normal(keys[1], (D, HEADS * HEAD), jnp.float32) * D ** -0.5
    w_k = jax.random.normal(keys[2], (D, KV_HEADS * HEAD), jnp.float32) * D ** -0.5
    w_v = jax.random.normal(keys[3], (D, KV_HEADS * HEAD), jnp.float32) * D ** -0.5
    w_o = jax.random.normal(keys[4], (HEADS * HEAD, D), jnp.float32) * (2.0 * (HEADS * HEAD) ** -0.5)
    q_gain = gain_scale * (1.0 + 0.2 * jax.random.normal(keys[5], (HEAD,), jnp.float32))
    k_gain = gain_scale * (1.0 + 0.2 * jax.random.normal(keys[6], (HEAD,), jnp.float32))
    return {
        'hidden': hidden.astype(jnp.bfloat16),
        'ln_gain': ln_gain.astype(jnp.bfloat16),
        'w_q': w_q.astype(jnp.bfloat16),
        'w_k': w_k.astype(jnp.bfloat16),
        'w_v': w_v.astype(jnp.bfloat16),
        'w_o': w_o.astype(jnp.bfloat16),
        'q_gain': q_gain.astype(jnp.bfloat16),
        'k_gain': k_gain.astype(jnp.bfloat16),
    }


def head_norm(values, gain):
    return values * lax.rsqrt(jnp.mean(values * values, axis=-1, keepdims=True) + EPS) * gain.astype(jnp.float32)


def rotate(values, positions):
    half = HEAD // 2
    inv_freq = jnp.power(THETA, -(jnp.arange(half, dtype=jnp.float32) * (2.0 / HEAD)))
    angles = positions.astype(jnp.float32)[:, None] * inv_freq[None, :]
    cos_pos = jnp.cos(angles)[:, None, :]
    sin_pos = jnp.sin(angles)[:, None, :]
    first_half = values[..., :half]
    second_half = values[..., half:]
    return jnp.concatenate([first_half * cos_pos - second_half * sin_pos, second_half * cos_pos + first_half * sin_pos], axis=-1)


def attend(q_all, k_all, v_all):
    limit = 2 ** 25 // (HEADS * SEQ)
    block_rows = min(SEQ, 2 ** max(3, min(9, limit.bit_length() - 1)))
    num_blocks = SEQ // block_rows
    group = HEADS // KV_HEADS
    q_blocks = q_all.reshape(num_blocks, block_rows, KV_HEADS, group, HEAD)
    key_pos = jnp.arange(SEQ)
    k_f32 = k_all.astype(jnp.float32)
    v_f32 = v_all.astype(jnp.float32)

    def one_block(block_args):
        q_block, block_idx = block_args
        scores = jnp.einsum('qkgd,skd->kgqs', q_block.astype(jnp.float32), k_f32) * (HEAD ** -0.5)
        q_pos = block_idx * block_rows + jnp.arange(block_rows)
        visible = q_pos[:, None] >= key_pos[None, :]
        scores = jnp.where(visible, scores, -jnp.inf)
        attn_prob = jax.nn.softmax(scores, axis=-1).astype(jnp.bfloat16)
        mixed = jnp.einsum('kgqs,skd->qkgd', attn_prob.astype(jnp.float32), v_f32)
        return mixed.astype(jnp.bfloat16)

    outputs = lax.map(one_block, (q_blocks, jnp.arange(num_blocks)))
    return outputs.reshape(SEQ, HEADS, HEAD)


def reference(hidden, ln_gain, w_q, w_k, w_v, w_o, q_gain, k_gain):
    hidden_f32 = hidden.astype(jnp.float32)
    normed = (hidden_f32 * lax.rsqrt(jnp.mean(hidden_f32 * hidden_f32, axis=-1, keepdims=True) + EPS) * ln_gain.astype(jnp.float32)).astype(jnp.bfloat16)
    positions = jnp.arange(SEQ)
    q_raw = jnp.dot(normed, w_q, preferred_element_type=jnp.float32).reshape(SEQ, HEADS, HEAD)
    k_raw = jnp.dot(normed, w_k, preferred_element_type=jnp.float32).reshape(SEQ, KV_HEADS, HEAD)
    v_all = jnp.dot(normed, w_v, preferred_element_type=jnp.float32).astype(jnp.bfloat16).reshape(SEQ, KV_HEADS, HEAD)
    q_all = rotate(head_norm(q_raw, q_gain), positions).astype(jnp.bfloat16)
    k_all = rotate(head_norm(k_raw, k_gain), positions).astype(jnp.bfloat16)
    mixed = attend(q_all, k_all, v_all)
    result = hidden_f32 + jnp.dot(mixed.reshape(SEQ, HEADS * HEAD), w_o, preferred_element_type=jnp.float32)
    return result.astype(jnp.bfloat16)
```

```python
import functools
import jax
import jax.numpy as jnp
from jax import lax
from jax.experimental import pallas as pl
from jax.experimental.pallas import tpu as pltpu
from jax.sharding import PartitionSpec as P

EPS = 1e-6
THETA = 1000000.0
LOG2E = 1.4426950408889634
CORES = 2
BF16 = jnp.bfloat16
F32 = jnp.float32


def dot(a, b):
    return jnp.dot(a, b, preferred_element_type=F32)


def kernel(group_size, x_hbm, wq, wk, wv, wo, ln_gain, q_gain_t, k_gain, cos_k, sin_k, cos_t, sin_t, out_ref,
           x_buf, h_buf, w_buf, wo_buf, kv, stage, q_t, o_t, m_buf, l_buf, o_all, o_send,
           x_sem, w_sem, wo_sem, h_ssem, h_rsem, d2d_ssem, d2d_rsem, first_ssem, first_rsem, ring_ssem, ring_rsem, o_ssem, o_rsem):
    chips = group_size // CORES
    me = lax.axis_index('sp')
    chip = me // CORES
    core = me % CORES
    partner = chip * CORES + (1 - core)
    rows = x_buf.shape[0]
    dim = x_buf.shape[1]
    head = k_gain.shape[1]
    half_head = head // 2
    width = w_buf.shape[2]
    local_heads = kv.shape[1]
    group = width // head
    chip_rows = rows * CORES
    far = chips // 2

    def device(c, k):
        return {'sp': c * CORES + k}

    def neighbour(dirn):
        return (chip + chips + 1 - 2 * dirn) % chips

    barrier = pltpu.get_barrier_semaphore()
    pl.semaphore_signal(barrier, inc=1, device_id={'sp': partner})
    for dirn in range(2):
        for k in range(CORES):
            pl.semaphore_signal(barrier, inc=1, device_id=device(neighbour(dirn), k))

    x_copy = pltpu.make_async_copy(x_hbm, x_buf, x_sem)
    x_copy.start()

    def kv_copies(idx):
        pair = (idx % 2) * 2 + idx // 2
        cols = pl.ds(pl.multiple_of(pair * (width // 2), width // 2), width // 2)
        slot = idx % 3
        return (pltpu.make_async_copy(wk.at[:, cols], w_buf.at[slot, :, pl.ds(0, width // 2)], w_sem.at[slot, 0]),
                pltpu.make_async_copy(wv.at[:, cols], w_buf.at[slot, :, pl.ds(width // 2, width // 2)], w_sem.at[slot, 1]))

    def q_copies(idx):
        cols = pl.ds(pl.multiple_of((core * local_heads + idx) * width, width), width)
        slot = (idx + 4) % 3
        return tuple(pltpu.make_async_copy(wq.at[pl.ds(r * (dim // 2), dim // 2), cols],
                                           w_buf.at[slot, pl.ds(r * (dim // 2), dim // 2), :], w_sem.at[slot, r]) for r in range(2))

    def wo_copy(b):
        return pltpu.make_async_copy(wo.at[pl.ds(b * width, width), :], wo_buf.at[pl.ds(b * width, width), :], wo_sem.at[b])

    for idx in range(3):
        for copy in kv_copies(idx):
            copy.start()

    x_copy.wait()
    step_rows = 16

    def norm_rows(r, carry):
        sl = pl.ds(pl.multiple_of(r * step_rows, step_rows), step_rows)
        xf = x_buf[sl, :].astype(F32)
        scale = lax.rsqrt(jnp.mean(xf * xf, axis=-1, keepdims=True) + EPS)
        h_buf[core, sl, :] = (xf * scale * ln_gain[...]).astype(BF16)
        return carry

    lax.fori_loop(0, rows // step_rows, norm_rows, 0)

    pl.semaphore_wait(barrier, 1 + 2 * CORES)
    h_copy = pltpu.make_async_remote_copy(h_buf.at[core], h_buf.at[core], h_ssem, h_rsem, device_id={'sp': partner})
    h_copy.start()

    def down_reach(j):
        return far - 1 + j // 2

    def first_copies(idx, e):
        owner = idx % 2
        j = (idx // 2) * 2 + e
        src = stage.at[idx, e]
        dst = kv.at[chip, j, core]
        up = pltpu.make_async_remote_copy(src, dst, first_ssem.at[0, idx, e], first_rsem.at[0, j, core], device_id=device(neighbour(0), owner))
        down = pltpu.make_async_remote_copy(src, dst, first_ssem.at[1, idx, e], first_rsem.at[1, j, core], device_id=device(neighbour(1), owner))
        across = pltpu.make_async_remote_copy(src, dst, d2d_ssem.at[j], d2d_rsem.at[j], device_id={'sp': partner})
        return ((up, chip < chips - 1), (down, chip < down_reach(j)), (across, owner != core))

    def project_kv(idx, carry):
        slot = idx % 3
        for copy in kv_copies(idx):
            copy.wait()
        raw = dot(h_buf[core], w_buf[slot])

        @pl.when(idx == 0)
        def _():
            for copy in kv_copies(3):
                copy.start()

        @pl.when(idx > 0)
        def _():
            for copy in q_copies(idx - 1):
                copy.start()

        for e in range(2):
            t = raw[:, e * head:(e + 1) * head]
            t = t * lax.rsqrt(jnp.mean(t * t, axis=-1, keepdims=True) + EPS) * k_gain[...]
            k_val = (t * cos_k[...] + pltpu.roll(t, half_head, 1) * sin_k[...]).astype(BF16)
            v_val = raw[:, width // 2 + e * head:width // 2 + (e + 1) * head].T.astype(BF16)
            stage[idx, e, 0] = k_val
            stage[idx, e, 1] = v_val

            @pl.when(idx % 2 == core)
            def _():
                kv[chip, (idx // 2) * 2 + e, core, 0] = k_val
                kv[chip, (idx // 2) * 2 + e, core, 1] = v_val

        for e in range(2):
            for copy, cond in first_copies(idx, e):
                pl.when(cond)(copy.start)
        return carry

    lax.fori_loop(0, 4, project_kv, 0)
    for b in range(wo_sem.shape[0]):
        wo_copy(b).start()
    h_copy.wait_recv()

    def project_q(idx, carry):
        slot = (idx + 4) % 3
        for copy in q_copies(idx):
            copy.wait()
        raw = dot(h_buf[...].reshape(chip_rows, dim), w_buf[slot])

        @pl.when(idx == 0)
        def _():
            for copy in q_copies(3):
                copy.start()

        for g in range(group):
            t = raw[:, g * head:(g + 1) * head].T
            t = t * lax.rsqrt(jnp.mean(t * t, axis=0, keepdims=True) + EPS) * q_gain_t[...]
            t1 = t[:half_head]
            t2 = t[half_head:]
            c = cos_t[...]
            s = sin_t[...]
            q_t[idx, :, g * chip_rows:(g + 1) * chip_rows] = jnp.concatenate([t1 * c - t2 * s, t2 * c + t1 * s], axis=0).astype(BF16)
        return carry

    lax.fori_loop(0, local_heads, project_q, 0)

    score_scale = (head ** -0.5) * LOG2E

    def attend(item, j, first):
        keys = kv[item, j, :, 0].reshape(chip_rows, head)
        vals = jnp.concatenate([kv[item, j, 0, 1], kv[item, j, 1, 1]], axis=1)
        for g in range(group):
            cols = slice(g * chip_rows, (g + 1) * chip_rows)
            scores = dot(keys, q_t[j, :, cols])
            if first:
                key_pos = lax.broadcasted_iota(jnp.int32, scores.shape, 0)
                q_pos = lax.broadcasted_iota(jnp.int32, scores.shape, 1)
                scores = jnp.where(key_pos <= q_pos, scores, -jnp.inf)
                m_new = jnp.max(scores, axis=0, keepdims=True)
            else:
                m_old = m_buf[j, :, cols]
                m_new = jnp.maximum(m_old, jnp.max(scores, axis=0, keepdims=True))
            prob = jnp.exp2((scores - m_new) * score_scale)
            total = jnp.sum(prob, axis=0, keepdims=True)
            mixed = dot(vals, prob.astype(BF16))
            m_buf[j, :, cols] = m_new
            if first:
                l_buf[j, :, cols] = total
                o_t[j, :, cols] = mixed
            else:
                alpha = jnp.exp2((m_old - m_new) * score_scale)
                l_buf[j, :, cols] = l_buf[j, :, cols] * alpha + total
                o_t[j, :, cols] = o_t[j, :, cols] * alpha + mixed

    def diagonal(j, carry):
        pltpu.make_async_remote_copy(kv.at[chip, j, 0], kv.at[chip, j, 1 - core], d2d_ssem.at[j], d2d_rsem.at[j], device_id={'sp': partner}).wait_recv()
        attend(chip, j, True)
        return carry

    lax.fori_loop(0, local_heads, diagonal, 0)

    def event(ev):
        dirn = ev % 2
        j = (ev // 2) % local_heads
        d = (ev // 2) // local_heads + 1
        reach = far - (dirn + j // 2) % 2
        item = (chip + chips + (2 * dirn - 1) * d) % chips
        valid = (d <= reach) & (((dirn == 0) & (item < chip)) | ((dirn == 1) & (item < reach)))
        forward = valid & (d + 1 <= reach) & ((dirn == 1) | (chip < chips - 1))
        return dirn, j, d, item, valid, forward

    def ring_copy(dirn, j, d, item):
        return pltpu.make_async_remote_copy(kv.at[item, j], kv.at[item, j], ring_ssem.at[dirn, d - 1, j], ring_rsem.at[dirn, d - 1, j],
                                            device_id=device(neighbour(dirn), core))

    def ring_step(ev, carry):
        dirn, j, d, item, valid, forward = event(ev)

        @pl.when(valid & (d == 1))
        def _():
            for k in range(CORES):
                pltpu.make_async_remote_copy(stage.at[0, 0], kv.at[item, j, k], first_ssem.at[0, 0, 0], first_rsem.at[dirn, j, k],
                                             device_id={'sp': partner}).wait_recv()

        @pl.when(valid & (d > 1))
        def _():
            ring_copy(dirn, j, d - 1, item).wait_recv()

        @pl.when(forward)
        def _():
            ring_copy(dirn, j, d, item).start()

        @pl.when(valid & (item < chip))
        def _():
            attend(item, j, False)

        return carry

    events = 2 * local_heads * far
    lax.fori_loop(0, events, ring_step, 0)

    def o_copy(j):
        cols = pl.ds(pl.multiple_of(j * width, width), width)
        return pltpu.make_async_remote_copy(o_send.at[:, cols], o_all.at[core, :, cols], o_ssem.at[j], o_rsem.at[j], device_id={'sp': partner})

    for j in range(local_heads):
        inv = 1.0 / l_buf[j]
        for g in range(group):
            cols = slice(g * chip_rows, (g + 1) * chip_rows)
            o_val = (o_t[j, :, cols] * inv[:, cols]).T.astype(BF16)
            mine = jnp.where(core == 0, o_val[:rows], o_val[rows:])
            other = jnp.where(core == 0, o_val[rows:], o_val[:rows])
            out_cols = slice(j * width + g * head, j * width + (g + 1) * head)
            o_all[core, :, out_cols] = mine
            o_send[:, out_cols] = other
        o_copy(j).start()

    for b in range(wo_sem.shape[0]):
        wo_copy(b).wait()
    for j in range(local_heads):
        o_copy(j).wait_recv()

    mixed_dim = local_heads * width

    def finish(n, carry):
        cols = pl.ds(pl.multiple_of(n * width, width), width)
        total = dot(o_all[0], wo_buf[:mixed_dim, cols]) + dot(o_all[1], wo_buf[mixed_dim:, cols])
        out_ref[:, cols] = (x_buf[:, cols].astype(F32) + total).astype(BF16)
        return carry

    lax.fori_loop(0, dim // width, finish, 0)

    h_copy.wait_send()
    for j in range(local_heads):
        o_copy(j).wait_send()

    def drain_first(idx, carry):
        for e in range(2):
            for copy, cond in first_copies(idx, e):
                pl.when(cond)(copy.wait_send)
        return carry

    lax.fori_loop(0, 4, drain_first, 0)

    def drain_ring(ev, carry):
        dirn, j, d, item, valid, forward = event(ev)

        @pl.when(forward)
        def _():
            ring_copy(dirn, j, d, item).wait_send()

        return carry

    lax.fori_loop(0, events, drain_ring, 0)


def solution(mesh):
    group_size = mesh.shape['sp']

    def device_step(hidden, ln_gain, w_q, w_k, w_v, w_o, q_gain, k_gain):
        rows, dim = hidden.shape
        head = q_gain.shape[0]
        half = head // 2
        chips = group_size // CORES
        local_heads = w_k.shape[1] // head // CORES
        width = w_q.shape[1] // CORES // local_heads
        chip_rows = rows * CORES
        me = lax.axis_index('sp')
        inv_freq = jnp.power(THETA, -(jnp.arange(half, dtype=F32) * (2.0 / head)))
        angles = ((me // CORES) * chip_rows + jnp.arange(chip_rows)).astype(F32)[None, :] * inv_freq[:, None]
        cos_t = jnp.cos(angles)
        sin_t = jnp.sin(angles)
        own = (me * rows + jnp.arange(rows)).astype(F32)[:, None] * inv_freq[None, :]
        cos_own = jnp.cos(own)
        sin_own = jnp.sin(own)
        cos_k = jnp.concatenate([cos_own, cos_own], axis=1)
        sin_k = jnp.concatenate([-sin_own, sin_own], axis=1)
        q_gain_t = jnp.broadcast_to(q_gain.astype(F32)[:, None], (head, chip_rows))
        vmem = pl.BlockSpec(memory_space=pltpu.VMEM)
        hbm = pl.BlockSpec(memory_space=pl.ANY)
        dma = pltpu.SemaphoreType.DMA
        return pl.pallas_call(
            functools.partial(kernel, group_size),
            out_shape=jax.ShapeDtypeStruct((rows, dim), BF16),
            in_specs=[hbm] * 5 + [vmem] * 7,
            out_specs=vmem,
            scratch_shapes=[
                pltpu.VMEM((rows, dim), BF16),
                pltpu.VMEM((CORES, rows, dim), BF16),
                pltpu.VMEM((3, dim, width), BF16),
                pltpu.VMEM(w_o.shape, BF16),
                pltpu.VMEM((chips, local_heads, CORES, 2, rows, head), BF16),
                pltpu.VMEM((4, 2, 2, rows, head), BF16),
                pltpu.VMEM((local_heads, head, width // head * chip_rows), BF16),
                pltpu.VMEM((local_heads, head, width // head * chip_rows), F32),
                pltpu.VMEM((local_heads, 1, width // head * chip_rows), F32),
                pltpu.VMEM((local_heads, 1, width // head * chip_rows), F32),
                pltpu.VMEM((CORES, rows, local_heads * width), BF16),
                pltpu.VMEM((rows, local_heads * width), BF16),
                dma, dma((3, 2)), dma((w_o.shape[0] // width,)), dma, dma,
                dma((local_heads,)), dma((local_heads,)),
                dma((2, 4, 2)), dma((2, local_heads, CORES)),
                dma((2, chips // 2, local_heads)), dma((2, chips // 2, local_heads)),
                dma((local_heads,)), dma((local_heads,)),
            ],
            compiler_params=pltpu.CompilerParams(collective_id=0, has_side_effects=True, vmem_limit_bytes=67043328),
        )(hidden, w_q, w_k, w_v, w_o, ln_gain.astype(F32)[None, :], q_gain_t, k_gain.astype(F32)[None, :], cos_k, sin_k, cos_t, sin_t)

    row_spec = P(('dp', 'sp'), None)
    return jax.shard_map(device_step, mesh=mesh, in_specs=(row_spec, P(), P(), P(), P(), P(), P(), P()), out_specs=row_spec, check_vma=False)
```

```python
import functools
import jax
import jax.numpy as jnp
import numpy as np
from jax import lax
from jax.experimental import pallas as pl
from jax.experimental.pallas import tpu as pltpu
from jax.sharding import PartitionSpec as P

EPS = 1e-6
THETA = 1000000.0
LOG2E = 1.4426950408889634
CORES = 2
BF16 = jnp.bfloat16
F32 = jnp.float32


def dot(a, b):
    return jnp.dot(a, b, preferred_element_type=F32)


def slot_table(values):
    return sum(v << (2 * s) for s, v in enumerate(values))


UP_HEAD = (0, 1, 2, 3, 0, 1, 2, 0, 1, 3, 0, 1, 2, 3)
UP_HOP = (0, 0, 0, 0, 1, 1, 1, 2, 2, 1, 3, 3, 2, 2)
DOWN_HEAD = (0, 1, 2, 3, 2, 3, 0, 1, 2, 3, 0, 1, 2, 3)
DOWN_HOP = (0, 0, 0, 0, 1, 1, 1, 1, 2, 2, 2, 2, 3, 3)
SLOTS = len(UP_HEAD)
TABLES = tuple(slot_table(t) for t in (UP_HEAD, UP_HOP, DOWN_HEAD, DOWN_HOP))
DRAIN_LAG = 7


def kernel(group_size, x_hbm, wq, wk, wv, wo, ln_hbm, q_gain_hbm, k_gain_hbm, cos_hbm, sin_hbm, out_hbm,
           x_buf, h_buf, w_buf, wo_buf, kv, stage, q_t, o_t, m_buf, l_buf, o_all, o_send, acc,
           ln_buf, gain_buf, cos_t, sin_t, gain_t, cos_k, sin_k,
           x_sem, small_sem, w_sem, wo_sem, h_ssem, h_rsem, d2d_ssem, d2d_rsem, first_ssem, first_rsem, ring_ssem, ring_rsem, o_ssem, o_rsem, out_sem):
    chips = group_size // CORES
    me = lax.axis_index('sp')
    chip = me // CORES
    core = me % CORES
    partner = chip * CORES + (1 - core)
    rows, dim = x_buf.shape
    head = gain_buf.shape[2]
    half_head = head // 2
    width = w_buf.shape[2]
    local_heads = kv.shape[1]
    group = width // head
    chip_rows = rows * CORES
    far = chips // 2
    mixed_dim = local_heads * width

    def device(c, k):
        return {'sp': c * CORES + k}

    def neighbour(dirn):
        return (chip + chips + 1 - 2 * dirn) % chips

    x_parts = x_sem.shape[0]
    part_rows = rows // x_parts

    def x_copy(r):
        sl = pl.ds(r * part_rows, part_rows)
        return pltpu.make_async_copy(x_hbm.at[sl, :], x_buf.at[sl, :], x_sem.at[r])

    chip_cols = pl.ds(pl.multiple_of(chip * chip_rows, chip_rows), chip_rows)
    small = (pltpu.make_async_copy(ln_hbm, ln_buf, small_sem.at[0]),
             pltpu.make_async_copy(q_gain_hbm, gain_buf.at[0], small_sem.at[1]),
             pltpu.make_async_copy(k_gain_hbm, gain_buf.at[1], small_sem.at[2]),
             pltpu.make_async_copy(cos_hbm.at[:, chip_cols], cos_t, small_sem.at[3]),
             pltpu.make_async_copy(sin_hbm.at[:, chip_cols], sin_t, small_sem.at[4]))

    def kv_copies(idx):
        pair = (idx % 2) * 2 + idx // 2
        cols = pl.ds(pl.multiple_of(pair * (width // 2), width // 2), width // 2)
        slot = idx % 3
        return (pltpu.make_async_copy(wk.at[:, cols], w_buf.at[slot, :, pl.ds(0, width // 2)], w_sem.at[slot, 0]),
                pltpu.make_async_copy(wv.at[:, cols], w_buf.at[slot, :, pl.ds(width // 2, width // 2)], w_sem.at[slot, 1]))

    def q_copies(idx):
        cols = pl.ds(pl.multiple_of((core * local_heads + idx) * width, width), width)
        slot = (idx + 4) % 3
        return tuple(pltpu.make_async_copy(wq.at[pl.ds(r * (dim // 2), dim // 2), cols],
                                           w_buf.at[slot, pl.ds(r * (dim // 2), dim // 2), :], w_sem.at[slot, r]) for r in range(2))

    def wo_copy(b):
        return pltpu.make_async_copy(wo.at[pl.ds(b * width, width), :], wo_buf.at[pl.ds(b * width, width), :], wo_sem.at[b])

    for copy in small[:1]:
        copy.start()
    for r in range(x_parts):
        x_copy(r).start()
    for copy in small[1:]:
        copy.start()
    for copy in kv_copies(0):
        copy.start()

    barrier = pltpu.get_barrier_semaphore()
    pl.semaphore_signal(barrier, inc=1, device_id={'sp': partner})
    for dirn in range(2):
        for k in range(CORES):
            pl.semaphore_signal(barrier, inc=1, device_id=device(neighbour(dirn), k))

    small[0].wait()
    for r in range(x_parts):
        x_copy(r).wait()
        if r == x_parts - 1:
            for idx in range(1, 3):
                for copy in kv_copies(idx):
                    copy.start()
        step_rows = 16
        for t in range(part_rows // step_rows):
            sl = slice(r * part_rows + t * step_rows, r * part_rows + (t + 1) * step_rows)
            xf = x_buf[sl, :].astype(F32)
            scale = lax.rsqrt(jnp.mean(xf * xf, axis=-1, keepdims=True) + EPS)
            h_buf[core, sl, :] = (xf * scale * ln_buf[...].astype(F32)).astype(BF16)

    for copy in small[1:]:
        copy.wait()
    gain_t[...] = jnp.broadcast_to(gain_buf[0].astype(F32), (chip_rows, head)).T
    own_cols = pl.ds(pl.multiple_of(core * rows, rows), rows)
    cos_own = cos_t[:, own_cols].T
    sin_own = sin_t[:, own_cols].T
    cos_k[...] = jnp.concatenate([cos_own, cos_own], axis=1)
    sin_k[...] = jnp.concatenate([-sin_own, sin_own], axis=1)

    pl.semaphore_wait(barrier, 1 + 2 * CORES)
    h_copy = pltpu.make_async_remote_copy(h_buf.at[core], h_buf.at[core], h_ssem, h_rsem, device_id={'sp': partner})

    def down_reach(j):
        return far - 1 + j // 2

    def first_copies(idx, e):
        owner = idx % 2
        j = (idx // 2) * 2 + e
        src = stage.at[idx, e]
        dst = kv.at[chip, j, core]
        up = pltpu.make_async_remote_copy(src, dst, first_ssem.at[0, idx, e], first_rsem.at[0, j, core], device_id=device(neighbour(0), owner))
        down = pltpu.make_async_remote_copy(src, dst, first_ssem.at[1, idx, e], first_rsem.at[1, j, core], device_id=device(neighbour(1), owner))
        across = pltpu.make_async_remote_copy(src, dst, d2d_ssem.at[j], d2d_rsem.at[j], device_id={'sp': partner})
        return ((up, chip < chips - 1), (down, chip < down_reach(j)), (across, owner != core))

    def project_kv(idx, carry):
        slot = idx % 3
        for copy in kv_copies(idx):
            copy.wait()
        raw = dot(h_buf[core], w_buf[slot])

        @pl.when(idx == 0)
        def _():
            for copy in kv_copies(3):
                copy.start()

        @pl.when(idx > 0)
        def _():
            for copy in q_copies(idx - 1):
                copy.start()

        for e in range(2):
            t = raw[:, e * head:(e + 1) * head]
            t = t * lax.rsqrt(jnp.mean(t * t, axis=-1, keepdims=True) + EPS) * gain_buf[1].astype(F32)
            k_val = (t * cos_k[...] + pltpu.roll(t, half_head, 1) * sin_k[...]).astype(BF16)
            v_val = raw[:, width // 2 + e * head:width // 2 + (e + 1) * head].T.astype(BF16)
            stage[idx, e, 0] = k_val
            stage[idx, e, 1] = v_val

            @pl.when(idx % 2 == core)
            def _():
                kv[chip, (idx // 2) * 2 + e, core, 0] = k_val
                kv[chip, (idx // 2) * 2 + e, core, 1] = v_val

        for e in range(2):
            for copy, cond in first_copies(idx, e):
                pl.when(cond)(copy.start)

        @pl.when(idx == 0)
        def _():
            h_copy.start()

        return carry

    lax.fori_loop(0, 4, project_kv, 0)
    h_copy.wait_recv()

    def event(s, dirn):
        j = lax.shift_right_logical(jnp.int32(TABLES[2 * dirn]), 2 * s) % 4
        d = lax.shift_right_logical(jnp.int32(TABLES[2 * dirn + 1]), 2 * s) % 4 + 1
        if dirn == 0:
            reach = far - j // 2
            item = (chip + chips - d) % chips
            valid = (d <= reach) & (item < chip)
            forward = valid & (d + 1 <= reach) & (chip < chips - 1)
        else:
            reach = far - 1 + j // 2
            item = (chip + d) % chips
            valid = (d <= reach) & (item < reach)
            forward = valid & (d + 1 <= reach)
        return j, d, item, valid, forward

    def ring_copy(dirn, j, d, item):
        return pltpu.make_async_remote_copy(kv.at[item, j], kv.at[item, j], ring_ssem.at[dirn, d - 1, j], ring_rsem.at[dirn, d - 1, j],
                                            device_id=device(neighbour(dirn), core))

    def poll_first(s):
        for dirn in range(2):
            j, d, item, valid, forward = event(s, dirn)

            @pl.when(valid)
            def _():
                for k in range(CORES):
                    pltpu.make_async_remote_copy(stage.at[0, 0], kv.at[item, j, k], first_ssem.at[0, 0, 0], first_rsem.at[dirn, j, k],
                                                 device_id={'sp': partner}).wait_recv()

            @pl.when(forward)
            def _():
                ring_copy(dirn, j, d, item).start()

    def poll(s):
        for dirn in range(2):
            j, d, item, valid, forward = event(s, dirn)

            @pl.when(valid)
            def _():
                ring_copy(dirn, j, d - 1, item).wait_recv()

            @pl.when(forward)
            def _():
                ring_copy(dirn, j, d, item).start()

    def drain(s):
        for dirn in range(2):
            j, d, item, valid, forward = event(s, dirn)

            @pl.when(forward)
            def _():
                ring_copy(dirn, j, d, item).wait_send()

    def project_q(idx, carry):
        slot = (idx + 4) % 3
        for copy in q_copies(idx):
            copy.wait()
        raw = dot(h_buf[...].reshape(chip_rows, dim), w_buf[slot])

        @pl.when(idx == 0)
        def _():
            for copy in q_copies(3):
                copy.start()

        @pl.when(idx > 0)
        def _():
            poll_first(idx - 1)

        for g in range(group):
            t = raw[:, g * head:(g + 1) * head].T
            t = t * lax.rsqrt(jnp.mean(t * t, axis=0, keepdims=True) + EPS) * gain_t[...]
            t1 = t[:half_head]
            t2 = t[half_head:]
            c = cos_t[...]
            s = sin_t[...]
            q_t[idx, :, g * chip_rows:(g + 1) * chip_rows] = jnp.concatenate([t1 * c - t2 * s, t2 * c + t1 * s], axis=0).astype(BF16)
        return carry

    lax.fori_loop(0, local_heads, project_q, 0)
    for b in range(wo_sem.shape[0]):
        wo_copy(b).start()

    score_scale = (head ** -0.5) * LOG2E

    def attend(item, j, first):
        keys = kv[item, j, :, 0].reshape(chip_rows, head)
        vals = jnp.concatenate([kv[item, j, 0, 1], kv[item, j, 1, 1]], axis=1)
        all_scores = [dot(keys, q_t[j, :, g * chip_rows:(g + 1) * chip_rows]) for g in range(group)]
        for g in range(group):
            cols = slice(g * chip_rows, (g + 1) * chip_rows)
            scores = all_scores[g]
            if first:
                key_pos = lax.broadcasted_iota(jnp.int32, scores.shape, 0)
                q_pos = lax.broadcasted_iota(jnp.int32, scores.shape, 1)
                scores = jnp.where(key_pos <= q_pos, scores, -jnp.inf)
                m_new = jnp.broadcast_to(jnp.max(scores, axis=0, keepdims=True), (8, chip_rows))
            else:
                m_old = m_buf[j, :, cols]
                m_new = jnp.maximum(m_old, jnp.max(scores, axis=0, keepdims=True))
            blocks = scores.reshape(chip_rows // 8, 8, chip_rows)
            prob = jnp.exp2((blocks - m_new[None]) * score_scale)
            total = jnp.sum(prob, axis=0)
            mixed = dot(vals, prob.reshape(chip_rows, chip_rows).astype(BF16))
            m_buf[j, :, cols] = m_new
            if first:
                l_buf[j, :, cols] = total
                o_t[j, :, cols] = mixed
            else:
                alpha = jnp.exp2((m_old - m_new) * score_scale)
                l_buf[j, :, cols] = l_buf[j, :, cols] * alpha + total
                old = o_t[j, :, cols].reshape(head // 8, 8, chip_rows)
                o_t[j, :, cols] = (old * alpha[None]).reshape(head, chip_rows) + mixed

    def diagonal(j, carry):
        pltpu.make_async_remote_copy(kv.at[chip, j, 0], kv.at[chip, j, 1 - core], d2d_ssem.at[j], d2d_rsem.at[j], device_id={'sp': partner}).wait_recv()
        attend(chip, j, True)
        return carry

    lax.fori_loop(0, local_heads, diagonal, 0)
    poll_first(local_heads - 1)

    def ring_step(s, carry):
        @pl.when(s >= local_heads)
        def _():
            poll(s)

        @pl.when(s >= DRAIN_LAG)
        def _():
            drain(s - DRAIN_LAG)

        def one(dirn, inner):
            up = event(s, 0)
            down = event(s, 1)
            j, item, valid = (jnp.where(dirn == 0, up[k], down[k]) for k in (0, 2, 3))

            @pl.when(valid & (item < chip))
            def _():
                attend(item, j, False)

            return inner

        lax.fori_loop(0, 2, one, 0)
        return carry

    def o_copy(j):
        cols = pl.ds(j * width, width)
        return pltpu.make_async_remote_copy(o_send.at[:, cols], o_all.at[core, :, cols], o_ssem.at[j], o_rsem.at[j], device_id={'sp': partner})

    def close_head(j):
        inv = 1.0 / jnp.sum(l_buf[j], axis=0, keepdims=True)
        for g in range(group):
            cols = slice(g * chip_rows, (g + 1) * chip_rows)
            o_val = (o_t[j, :, cols] * inv[:, cols]).T.astype(BF16)
            out_cols = slice(j * width + g * head, j * width + (g + 1) * head)
            o_all[core, :, out_cols] = jnp.where(core == 0, o_val[:rows], o_val[rows:])
            o_send[:, out_cols] = jnp.where(core == 0, o_val[rows:], o_val[:rows])
        o_copy(j).start()

    def out_copy(n):
        cols = pl.ds(n * width, width)
        return pltpu.make_async_copy(acc.at[:, cols], out_hbm.at[:, cols], out_sem.at[n])

    def project_out(first_head, last_head, start, end):
        for j in range(first_head, last_head):
            for c in range(CORES):
                wo_copy(c * local_heads + j).wait()
        for j in range(first_head, last_head):
            o_copy(j).wait_recv()
        depth = slice(first_head * width, last_head * width)

        def block(n, carry):
            cols = pl.ds(pl.multiple_of(n * width, width), width)
            total = x_buf[:, cols].astype(F32) if start else acc[:, cols]
            for c in range(CORES):
                total = total + dot(o_all[c, :, depth], wo_buf[c * mixed_dim + depth.start:c * mixed_dim + depth.stop, cols])
            acc[:, cols] = total
            if end:
                out_copy(n).start()
            return carry

        lax.fori_loop(0, dim // width, block, 0)

    lax.fori_loop(0, SLOTS - 2, ring_step, 0)
    close_head(0)
    close_head(1)
    lax.fori_loop(SLOTS - 2, SLOTS - 1, ring_step, 0)
    close_head(2)
    project_out(0, 2, True, False)
    lax.fori_loop(SLOTS - 1, SLOTS, ring_step, 0)
    close_head(3)
    project_out(2, 3, False, False)
    project_out(3, 4, False, True)

    h_copy.wait_send()
    for j in range(local_heads):
        o_copy(j).wait_send()

    def drain_first(idx, carry):
        for e in range(2):
            for copy, cond in first_copies(idx, e):
                pl.when(cond)(copy.wait_send)
        return carry

    lax.fori_loop(0, 4, drain_first, 0)
    for s in range(SLOTS - DRAIN_LAG, SLOTS):
        drain(s)
    for n in range(dim // width):
        out_copy(n).wait()


def solution(mesh):
    group_size = mesh.shape['sp']

    def device_step(hidden, ln_gain, w_q, w_k, w_v, w_o, q_gain, k_gain):
        rows, dim = hidden.shape
        head = q_gain.shape[0]
        half = head // 2
        chips = group_size // CORES
        local_heads = w_k.shape[1] // head // CORES
        width = w_q.shape[1] // CORES // local_heads
        chip_rows = rows * CORES
        inv_freq = THETA ** -(np.arange(half, dtype=np.float64) * (2.0 / head))
        angles = inv_freq[:, None] * np.arange(rows * group_size)[None, :]
        cos_all = jnp.asarray(np.cos(angles).astype(np.float32))
        sin_all = jnp.asarray(np.sin(angles).astype(np.float32))
        hbm = pl.BlockSpec(memory_space=pl.ANY)
        dma = pltpu.SemaphoreType.DMA
        wide = width // head * chip_rows
        total = pl.pallas_call(
            functools.partial(kernel, group_size),
            out_shape=jax.ShapeDtypeStruct((rows, dim), F32),
            in_specs=[hbm] * 10,
            out_specs=hbm,
            scratch_shapes=[
                pltpu.VMEM((rows, dim), BF16),
                pltpu.VMEM((CORES, rows, dim), BF16),
                pltpu.VMEM((3, dim, width), BF16),
                pltpu.VMEM(w_o.shape, BF16),
                pltpu.VMEM((chips, local_heads, CORES, 2, rows, head), BF16),
                pltpu.VMEM((4, 2, 2, rows, head), BF16),
                pltpu.VMEM((local_heads, head, wide), BF16),
                pltpu.VMEM((local_heads, head, wide), F32),
                pltpu.VMEM((local_heads, 8, wide), F32),
                pltpu.VMEM((local_heads, 8, wide), F32),
                pltpu.VMEM((CORES, rows, local_heads * width), BF16),
                pltpu.VMEM((rows, local_heads * width), BF16),
                pltpu.VMEM((rows, dim), F32),
                pltpu.VMEM((1, dim), BF16),
                pltpu.VMEM((2, 1, head), BF16),
                pltpu.VMEM((half, chip_rows), F32),
                pltpu.VMEM((half, chip_rows), F32),
                pltpu.VMEM((head, chip_rows), F32),
                pltpu.VMEM((rows, head), F32),
                pltpu.VMEM((rows, head), F32),
                dma((4,)), dma((5,)), dma((3, 2)), dma((w_o.shape[0] // width,)), dma, dma,
                dma((local_heads,)), dma((local_heads,)),
                dma((2, 4, 2)), dma((2, local_heads, CORES)),
                dma((2, chips // 2, local_heads)), dma((2, chips // 2, local_heads)),
                dma((local_heads,)), dma((local_heads,)), dma((dim // width,)),
            ],
            compiler_params=pltpu.CompilerParams(collective_id=0, has_side_effects=True, vmem_limit_bytes=67043328),
        )(hidden, w_q, w_k, w_v, w_o, ln_gain[None, :], q_gain[None, :], k_gain[None, :], cos_all, sin_all)
        return total.astype(BF16)

    row_spec = P(('dp', 'sp'), None)
    return jax.shard_map(device_step, mesh=mesh, in_specs=(row_spec, P(), P(), P(), P(), P(), P(), P()), out_specs=row_spec, check_vma=False)
```

```python
import functools
import jax
import jax.numpy as jnp
import numpy as np
from jax import lax
from jax.experimental import pallas as pl
from jax.experimental.pallas import tpu as pltpu
from jax.sharding import PartitionSpec as P

EPS = 1e-6
THETA = 1000000.0
LOG2E = 1.4426950408889634
CORES = 2
LANES = 128
VMEM_LIMIT = 62 * 2 ** 20
BF16 = jnp.bfloat16
F32 = jnp.float32


def dot(a, b):
    return jnp.dot(a, b, preferred_element_type=F32)


def slot_table(values):
    return sum(v << (2 * s) for s, v in enumerate(values))


UP_HEAD = (0, 1, 2, 3, 0, 1, 2, 0, 1, 3, 0, 1, 2, 3)
UP_HOP = (0, 0, 0, 0, 1, 1, 1, 2, 2, 1, 3, 3, 2, 2)
DOWN_HEAD = (0, 1, 2, 3, 2, 3, 0, 1, 2, 3, 0, 1, 2, 3)
DOWN_HOP = (0, 0, 0, 0, 1, 1, 1, 1, 2, 2, 2, 2, 3, 3)
SLOTS = len(UP_HEAD)
TABLES = tuple(slot_table(t) for t in (UP_HEAD, UP_HOP, DOWN_HEAD, DOWN_HOP))
DRAIN_LAG = 7


def kernel(group_size, x_hbm, wq, wk, wv, wo, ln_hbm, q_gain_hbm, k_gain_hbm, cos_hbm, sin_hbm, out_ref,
           x_buf, h_buf, w_buf, wo_buf, kv, stage, q_t, o_t, m_buf, l_buf, o_all, o_send, acc,
           ln_buf, gain_buf, cos_t, sin_t, gain_t, cos_k, sin_k,
           x_sem, small_sem, w_sem, wo_sem, h_ssem, h_rsem, d2d_ssem, d2d_rsem, first_ssem, first_rsem, ring_ssem, ring_rsem, o_ssem, o_rsem):
    chips = group_size // CORES
    me = lax.axis_index('sp')
    chip = me // CORES
    core = me % CORES
    partner = chip * CORES + (1 - core)
    rows, dim = x_buf.shape
    head = gain_buf.shape[2]
    half_head = head // 2
    width = w_buf.shape[2]
    local_heads = kv.shape[1]
    group = width // head
    chip_rows = rows * CORES
    far = chips // 2
    mixed_dim = local_heads * width
    lanes = ln_buf.shape[1]

    def device(c, k):
        return {'sp': c * CORES + k}

    def neighbour(dirn):
        return (chip + chips + 1 - 2 * dirn) % chips

    x_parts = x_sem.shape[0]
    part_rows = rows // x_parts

    def x_copy(r):
        sl = pl.ds(r * part_rows, part_rows)
        return pltpu.make_async_copy(x_hbm.at[sl, :], x_buf.at[sl, :], x_sem.at[r])

    chip_cols = pl.ds(pl.multiple_of(chip * chip_rows, chip_rows), chip_rows)
    small = (pltpu.make_async_copy(ln_hbm, ln_buf, small_sem.at[0]),
             pltpu.make_async_copy(q_gain_hbm, gain_buf.at[0], small_sem.at[1]),
             pltpu.make_async_copy(k_gain_hbm, gain_buf.at[1], small_sem.at[2]),
             pltpu.make_async_copy(cos_hbm.at[:, chip_cols], cos_t, small_sem.at[3]),
             pltpu.make_async_copy(sin_hbm.at[:, chip_cols], sin_t, small_sem.at[4]))

    def kv_copies(idx):
        pair = (idx % 2) * 2 + idx // 2
        cols = pl.ds(pl.multiple_of(pair * (width // 2), width // 2), width // 2)
        slot = idx % 3
        return (pltpu.make_async_copy(wk.at[:, cols], w_buf.at[slot, :, pl.ds(0, width // 2)], w_sem.at[slot, 0]),
                pltpu.make_async_copy(wv.at[:, cols], w_buf.at[slot, :, pl.ds(width // 2, width // 2)], w_sem.at[slot, 1]))

    def q_copies(idx):
        cols = pl.ds(pl.multiple_of((core * local_heads + idx) * width, width), width)
        slot = (idx + 4) % 3
        return tuple(pltpu.make_async_copy(wq.at[pl.ds(r * (dim // 2), dim // 2), cols],
                                           w_buf.at[slot, pl.ds(r * (dim // 2), dim // 2), :], w_sem.at[slot, r]) for r in range(2))

    def wo_copy(b):
        return pltpu.make_async_copy(wo.at[pl.ds(b * width, width), :], wo_buf.at[pl.ds(b * width, width), :], wo_sem.at[b])

    for copy in small[:1]:
        copy.start()
    for r in range(x_parts):
        x_copy(r).start()
    for copy in small[1:]:
        copy.start()
    for copy in kv_copies(0):
        copy.start()

    barrier = pltpu.get_barrier_semaphore()
    pl.semaphore_signal(barrier, inc=1, device_id={'sp': partner})
    for dirn in range(2):
        for k in range(CORES):
            pl.semaphore_signal(barrier, inc=1, device_id=device(neighbour(dirn), k))

    small[0].wait()
    for r in range(x_parts):
        x_copy(r).wait()
        if r == x_parts - 1:
            for idx in range(1, 3):
                for copy in kv_copies(idx):
                    copy.start()
        step_rows = 16
        for t in range(part_rows // step_rows):
            sl = slice(r * part_rows + t * step_rows, r * part_rows + (t + 1) * step_rows)
            xf = x_buf[sl, :].astype(F32)
            scale = lax.rsqrt(jnp.mean(xf * xf, axis=-1, keepdims=True) + EPS)
            for b in range(dim // lanes):
                cols = slice(b * lanes, (b + 1) * lanes)
                h_buf[core, sl, cols] = (xf[:, cols] * scale * ln_buf[b:b + 1, :].astype(F32)).astype(BF16)

    for copy in small[1:]:
        copy.wait()
    gain_t[...] = jnp.broadcast_to(gain_buf[0].astype(F32), (chip_rows, head)).T
    own_cols = pl.ds(pl.multiple_of(core * rows, rows), rows)
    cos_own = cos_t[:, own_cols].T
    sin_own = sin_t[:, own_cols].T
    cos_k[...] = jnp.concatenate([cos_own, cos_own], axis=1)
    sin_k[...] = jnp.concatenate([-sin_own, sin_own], axis=1)

    pl.semaphore_wait(barrier, 1 + 2 * CORES)
    h_copy = pltpu.make_async_remote_copy(h_buf.at[core], h_buf.at[core], h_ssem, h_rsem, device_id={'sp': partner})

    def down_reach(j):
        return far - 1 + j // 2

    def first_copies(idx, e):
        owner = idx % 2
        j = (idx // 2) * 2 + e
        src = stage.at[idx, e]
        dst = kv.at[chip, j, core]
        up = pltpu.make_async_remote_copy(src, dst, first_ssem.at[0, idx, e], first_rsem.at[0, j, core], device_id=device(neighbour(0), owner))
        down = pltpu.make_async_remote_copy(src, dst, first_ssem.at[1, idx, e], first_rsem.at[1, j, core], device_id=device(neighbour(1), owner))
        across = pltpu.make_async_remote_copy(src, dst, d2d_ssem.at[j], d2d_rsem.at[j], device_id={'sp': partner})
        return ((up, chip < chips - 1), (down, chip < down_reach(j)), (across, owner != core))

    def project_kv(idx, carry):
        slot = idx % 3
        for copy in kv_copies(idx):
            copy.wait()
        raw = dot(h_buf[core], w_buf[slot])

        @pl.when(idx == 0)
        def _():
            for copy in kv_copies(3):
                copy.start()

        @pl.when(idx > 0)
        def _():
            for copy in q_copies(idx - 1):
                copy.start()

        for e in range(2):
            t = raw[:, e * head:(e + 1) * head]
            t = t * lax.rsqrt(jnp.mean(t * t, axis=-1, keepdims=True) + EPS) * gain_buf[1].astype(F32)
            k_val = (t * cos_k[...] + pltpu.roll(t, half_head, 1) * sin_k[...]).astype(BF16)
            v_val = raw[:, width // 2 + e * head:width // 2 + (e + 1) * head].T.astype(BF16)
            stage[idx, e, 0] = k_val
            stage[idx, e, 1] = v_val

            @pl.when(idx % 2 == core)
            def _():
                kv[chip, (idx // 2) * 2 + e, core, 0] = k_val
                kv[chip, (idx // 2) * 2 + e, core, 1] = v_val

        for e in range(2):
            for copy, cond in first_copies(idx, e):
                pl.when(cond)(copy.start)

        @pl.when(idx == 0)
        def _():
            h_copy.start()

        return carry

    lax.fori_loop(0, 4, project_kv, 0)
    h_copy.wait_recv()

    def event(s, dirn):
        j = lax.shift_right_logical(jnp.int32(TABLES[2 * dirn]), 2 * s) % 4
        d = lax.shift_right_logical(jnp.int32(TABLES[2 * dirn + 1]), 2 * s) % 4 + 1
        if dirn == 0:
            reach = far - j // 2
            item = (chip + chips - d) % chips
            valid = (d <= reach) & (item < chip)
            forward = valid & (d + 1 <= reach) & (chip < chips - 1)
        else:
            reach = far - 1 + j // 2
            item = (chip + d) % chips
            valid = (d <= reach) & (item < reach)
            forward = valid & (d + 1 <= reach)
        return j, d, item, valid, forward

    def ring_copy(dirn, j, d, item):
        return pltpu.make_async_remote_copy(kv.at[item, j], kv.at[item, j], ring_ssem.at[dirn, (d - 1) * local_heads + j], ring_rsem.at[dirn, (d - 1) * local_heads + j],
                                            device_id=device(neighbour(dirn), core))

    def poll_first(s):
        for dirn in range(2):
            j, d, item, valid, forward = event(s, dirn)

            @pl.when(valid)
            def _():
                for k in range(CORES):
                    pltpu.make_async_remote_copy(stage.at[0, 0], kv.at[item, j, k], first_ssem.at[0, 0, 0], first_rsem.at[dirn, j, k],
                                                 device_id={'sp': partner}).wait_recv()

            @pl.when(forward)
            def _():
                ring_copy(dirn, j, d, item).start()

    def poll(s):
        for dirn in range(2):
            j, d, item, valid, forward = event(s, dirn)

            @pl.when(valid)
            def _():
                ring_copy(dirn, j, d - 1, item).wait_recv()

            @pl.when(forward)
            def _():
                ring_copy(dirn, j, d, item).start()

    def drain(s):
        for dirn in range(2):
            j, d, item, valid, forward = event(s, dirn)

            @pl.when(forward)
            def _():
                ring_copy(dirn, j, d, item).wait_send()

    def project_q(idx, carry):
        slot = (idx + 4) % 3
        for copy in q_copies(idx):
            copy.wait()
        raw = dot(h_buf[...].reshape(chip_rows, dim), w_buf[slot])

        @pl.when(idx == 0)
        def _():
            for copy in q_copies(3):
                copy.start()

        @pl.when(idx > 0)
        def _():
            poll_first(idx - 1)

        for g in range(group):
            t = raw[:, g * head:(g + 1) * head].T
            t = t * lax.rsqrt(jnp.mean(t * t, axis=0, keepdims=True) + EPS) * gain_t[...]
            t1 = t[:half_head]
            t2 = t[half_head:]
            c = cos_t[...]
            s = sin_t[...]
            q_t[idx, :, g * chip_rows:(g + 1) * chip_rows] = jnp.concatenate([t1 * c - t2 * s, t2 * c + t1 * s], axis=0).astype(BF16)
        return carry

    lax.fori_loop(0, local_heads, project_q, 0)
    for b in range(wo_sem.shape[0]):
        wo_copy(b).start()

    score_scale = (head ** -0.5) * LOG2E

    def attend(item, j, first):
        keys = kv[item, j, :, 0].reshape(chip_rows, head)
        vals = jnp.concatenate([kv[item, j, 0, 1], kv[item, j, 1, 1]], axis=1)
        all_scores = [dot(keys, q_t[j, :, g * chip_rows:(g + 1) * chip_rows]) for g in range(group)]
        for g in range(group):
            cols = slice(g * chip_rows, (g + 1) * chip_rows)
            scores = all_scores[g]
            if first:
                key_pos = lax.broadcasted_iota(jnp.int32, scores.shape, 0)
                q_pos = lax.broadcasted_iota(jnp.int32, scores.shape, 1)
                scores = jnp.where(key_pos <= q_pos, scores, -jnp.inf)
                m_new = jnp.broadcast_to(jnp.max(scores, axis=0, keepdims=True), (8, chip_rows))
            else:
                m_old = m_buf[j, :, cols]
                m_new = jnp.maximum(m_old, jnp.max(scores, axis=0, keepdims=True))
            blocks = scores.reshape(chip_rows // 8, 8, chip_rows)
            prob = jnp.exp2((blocks - m_new[None]) * score_scale)
            total = jnp.sum(prob, axis=0)
            mixed = dot(vals, prob.reshape(chip_rows, chip_rows).astype(BF16))
            m_buf[j, :, cols] = m_new
            if first:
                l_buf[j, :, cols] = total
                o_t[j, :, cols] = mixed
            else:
                alpha = jnp.exp2((m_old - m_new) * score_scale)
                l_buf[j, :, cols] = l_buf[j, :, cols] * alpha + total
                old = o_t[j, :, cols].reshape(head // 8, 8, chip_rows)
                o_t[j, :, cols] = (old * alpha[None]).reshape(head, chip_rows) + mixed

    def diagonal(j, carry):
        pltpu.make_async_remote_copy(kv.at[chip, j, 0], kv.at[chip, j, 1 - core], d2d_ssem.at[j], d2d_rsem.at[j], device_id={'sp': partner}).wait_recv()
        attend(chip, j, True)
        return carry

    lax.fori_loop(0, local_heads, diagonal, 0)
    poll_first(local_heads - 1)

    def ring_step(s, carry):
        @pl.when(s >= local_heads)
        def _():
            poll(s)

        @pl.when(s >= DRAIN_LAG)
        def _():
            drain(s - DRAIN_LAG)

        def one(dirn, inner):
            up = event(s, 0)
            down = event(s, 1)
            j, item, valid = (jnp.where(dirn == 0, up[k], down[k]) for k in (0, 2, 3))

            @pl.when(valid & (item < chip))
            def _():
                attend(item, j, False)

            return inner

        lax.fori_loop(0, 2, one, 0)
        return carry

    def o_copy(j):
        cols = pl.ds(j * width, width)
        return pltpu.make_async_remote_copy(o_send.at[:, cols], o_all.at[core, :, cols], o_ssem.at[j], o_rsem.at[j], device_id={'sp': partner})

    def close_head(j):
        inv = 1.0 / jnp.sum(l_buf[j], axis=0, keepdims=True)
        for g in range(group):
            cols = slice(g * chip_rows, (g + 1) * chip_rows)
            o_val = (o_t[j, :, cols] * inv[:, cols]).T.astype(BF16)
            out_cols = slice(j * width + g * head, j * width + (g + 1) * head)
            o_all[core, :, out_cols] = jnp.where(core == 0, o_val[:rows], o_val[rows:])
            o_send[:, out_cols] = jnp.where(core == 0, o_val[rows:], o_val[:rows])
        o_copy(j).start()

    def project_out(first_head, last_head, start, end):
        for j in range(first_head, last_head):
            for c in range(CORES):
                wo_copy(c * local_heads + j).wait()
        for j in range(first_head, last_head):
            o_copy(j).wait_recv()
        depth = slice(first_head * width, last_head * width)

        def block(n, carry):
            for w in range(wide // width):
                cols = pl.ds(pl.multiple_of(n * wide + w * width, width), width)
                total = x_buf[:, cols].astype(F32) if start else acc[:, cols]
                for c in range(CORES):
                    total = total + dot(o_all[c, :, depth], wo_buf[c * mixed_dim + depth.start:c * mixed_dim + depth.stop, cols])
                if end:
                    out_ref[:, cols] = total.astype(BF16)
                else:
                    acc[:, cols] = total
            return carry

        wide = dim // 2
        lax.fori_loop(0, dim // wide, block, 0)

    lax.fori_loop(0, SLOTS - 2, ring_step, 0)
    close_head(0)
    close_head(1)
    lax.fori_loop(SLOTS - 2, SLOTS - 1, ring_step, 0)
    close_head(2)
    project_out(0, 2, True, False)
    lax.fori_loop(SLOTS - 1, SLOTS, ring_step, 0)
    close_head(3)
    project_out(2, 3, False, False)
    project_out(3, 4, False, True)

    h_copy.wait_send()
    for j in range(local_heads):
        o_copy(j).wait_send()

    def drain_first(idx, carry):
        for e in range(2):
            for copy, cond in first_copies(idx, e):
                pl.when(cond)(copy.wait_send)
        return carry

    lax.fori_loop(0, 4, drain_first, 0)
    for s in range(SLOTS - DRAIN_LAG, SLOTS):
        drain(s)


def solution(mesh):
    group_size = mesh.shape['sp']

    def device_step(hidden, ln_gain, w_q, w_k, w_v, w_o, q_gain, k_gain):
        rows, dim = hidden.shape
        head = q_gain.shape[0]
        half = head // 2
        chips = group_size // CORES
        local_heads = w_k.shape[1] // head // CORES
        width = w_q.shape[1] // CORES // local_heads
        chip_rows = rows * CORES
        inv_freq = THETA ** -(np.arange(half, dtype=np.float64) * (2.0 / head))
        angles = inv_freq[:, None] * np.arange(rows * group_size)[None, :]
        cos_all = jnp.asarray(np.cos(angles).astype(np.float32))
        sin_all = jnp.asarray(np.sin(angles).astype(np.float32))
        hbm = pl.BlockSpec(memory_space=pl.ANY)
        dma = pltpu.SemaphoreType.DMA
        wide = width // head * chip_rows
        return pl.pallas_call(
            functools.partial(kernel, group_size),
            out_shape=pltpu.VMEM((rows, dim), BF16),
            in_specs=[hbm] * 10,
            out_specs=pl.BlockSpec(memory_space=pltpu.VMEM),
            scratch_shapes=[
                pltpu.VMEM((rows, dim), BF16),
                pltpu.VMEM((CORES, rows, dim), BF16),
                pltpu.VMEM((3, dim, width), BF16),
                pltpu.VMEM(w_o.shape, BF16),
                pltpu.VMEM((chips, local_heads, CORES, 2, rows, head), BF16),
                pltpu.VMEM((4, 2, 2, rows, head), BF16),
                pltpu.VMEM((local_heads, head, wide), BF16),
                pltpu.VMEM((local_heads, head, wide), F32),
                pltpu.VMEM((local_heads, 8, wide), F32),
                pltpu.VMEM((local_heads, 8, wide), F32),
                pltpu.VMEM((CORES, rows, local_heads * width), BF16),
                pltpu.VMEM((rows, local_heads * width), BF16),
                pltpu.VMEM((rows, dim), F32),
                pltpu.VMEM((dim // LANES, LANES), BF16),
                pltpu.VMEM((2, 1, head), BF16),
                pltpu.VMEM((half, chip_rows), F32),
                pltpu.VMEM((half, chip_rows), F32),
                pltpu.VMEM((head, chip_rows), F32),
                pltpu.VMEM((rows, head), F32),
                pltpu.VMEM((rows, head), F32),
                dma((2,)), dma((5,)), dma((3, 2)), dma((w_o.shape[0] // width,)), dma, dma,
                dma((local_heads,)), dma((local_heads,)),
                dma((2, 4, 2)), dma((2, local_heads, CORES)),
                dma((2, (chips // 2 - 1) * local_heads)), dma((2, (chips // 2 - 1) * local_heads)),
                dma((local_heads,)), dma((local_heads,)),
            ],
            compiler_params=pltpu.CompilerParams(collective_id=0, has_side_effects=True, vmem_limit_bytes=VMEM_LIMIT),
        )(hidden, w_q, w_k, w_v, w_o, ln_gain.reshape(-1, LANES), q_gain[None, :], k_gain[None, :], cos_all, sin_all)

    row_spec = P(('dp', 'sp'), None)
    return jax.shard_map(device_step, mesh=mesh, in_specs=(row_spec, P(), P(), P(), P(), P(), P(), P()), out_specs=row_spec, check_vma=False)
```

```python
import functools
import jax
import jax.numpy as jnp
import numpy as np
from jax import lax
from jax.experimental import pallas as pl
from jax.experimental.pallas import tpu as pltpu
from jax.sharding import PartitionSpec as P

EPS = 1e-6
THETA = 1000000.0
LOG2E = 1.4426950408889634
CORES = 2
LANES = 128
VMEM_LIMIT = 62 * 2 ** 20
BF16 = jnp.bfloat16
F32 = jnp.float32


def dot(a, b):
    return jnp.dot(a, b, preferred_element_type=F32)


ORDER = ((0, 1), (1, 1), (2, 1), (3, 1), (0, 2), (1, 2), (0, 3), (1, 3), (2, 2), (0, 4), (1, 4), (3, 2), (2, 3), (3, 3), (2, 4), (3, 4))
SLOTS = len(ORDER)
EARLY = 2
EARLY_CLOSE = 10
EARLY_OUT = 11
THIRD_CLOSE = 14
DEFERRED = ((5, 2), (7, 3))


def slot_table(values):
    return tuple(sum(v << (2 * s) for s, v in enumerate(values[h:h + 8])) for h in (0, 8))


HEAD_TABLE = slot_table([j for j, _ in ORDER])
HOP_TABLE = slot_table([d - 1 for _, d in ORDER])


def lookup(table, s):
    return lax.shift_right_logical(jnp.where(s < 8, table[0], table[1]), 2 * (s % 8)) % 4


def kernel(group_size, x_hbm, wq, wk, wv, wo, ln_hbm, q_gain_hbm, k_gain_hbm, angle_hbm, out_ref,
           x_buf, h_buf, w_buf, wo_buf, kv, stage, q_t, o_t, m_buf, l_buf, o_all, o_send, acc,
           ln_buf, gain_buf, angle_t, gain_t, cos_k, sin_k,
           x_sem, small_sem, w_sem, wo_sem, h_ssem, h_rsem, d2d_ssem, d2d_rsem, first_ssem, first_rsem, ring_ssem, ring_rsem, o_ssem, o_rsem):
    chips = group_size // CORES
    me = lax.axis_index('sp')
    chip = me // CORES
    core = me % CORES
    partner = chip * CORES + (1 - core)
    rows, dim = x_buf.shape
    head = gain_buf.shape[2]
    half_head = head // 2
    width = w_buf.shape[2]
    local_heads = kv.shape[1]
    group = width // head
    chip_rows = rows * CORES
    far = chips // 2
    mixed_dim = local_heads * width
    lanes = ln_buf.shape[1]

    def device(c, k):
        return {'sp': c * CORES + k}

    def neighbour(dirn):
        return (chip + chips + 1 - 2 * dirn) % chips

    x_parts = x_sem.shape[0]
    part_rows = rows // x_parts

    def x_copy(r):
        sl = pl.ds(r * part_rows, part_rows)
        return pltpu.make_async_copy(x_hbm.at[sl, :], x_buf.at[sl, :], x_sem.at[r])

    chip_cols = pl.ds(pl.multiple_of(chip * chip_rows, chip_rows), chip_rows)
    small = (pltpu.make_async_copy(ln_hbm, ln_buf, small_sem.at[0]),
             pltpu.make_async_copy(q_gain_hbm, gain_buf.at[0], small_sem.at[1]),
             pltpu.make_async_copy(k_gain_hbm, gain_buf.at[1], small_sem.at[2]),
             pltpu.make_async_copy(angle_hbm.at[:, :, chip_cols], angle_t, small_sem.at[3]))

    def kv_copies(idx):
        pair = (idx % 2) * 2 + idx // 2
        cols = pl.ds(pl.multiple_of(pair * (width // 2), width // 2), width // 2)
        slot = idx % 3
        return (pltpu.make_async_copy(wk.at[:, cols], w_buf.at[slot, :, pl.ds(0, width // 2)], w_sem.at[slot]),
                pltpu.make_async_copy(wv.at[:, cols], w_buf.at[slot, :, pl.ds(width // 2, width // 2)], w_sem.at[slot]))

    def q_copies(idx):
        cols = pl.ds(pl.multiple_of((core * local_heads + idx) * width, width), width)
        slot = (idx + 4) % 3
        return tuple(pltpu.make_async_copy(wq.at[pl.ds(r * (dim // 2), dim // 2), cols],
                                           w_buf.at[slot, pl.ds(r * (dim // 2), dim // 2), :], w_sem.at[slot]) for r in range(2))

    def w_wait(slot):
        pltpu.make_async_copy(wq.at[:, pl.ds(0, width)], w_buf.at[slot], w_sem.at[slot]).wait()

    stages = ((0, EARLY), (EARLY, EARLY + 1), (EARLY + 1, local_heads))

    def wo_copies(k):
        first, last = stages[k]
        spans = [pl.ds(c * mixed_dim + first * width, (last - first) * width) for c in range(CORES)]
        return [pltpu.make_async_copy(wo.at[span, :], wo_buf.at[span, :], wo_sem.at[k]) for span in spans]

    def wo_wait(k):
        span = pl.ds(0, CORES * (stages[k][1] - stages[k][0]) * width)
        pltpu.make_async_copy(wo.at[span, :], wo_buf.at[span, :], wo_sem.at[k]).wait()

    for copy in small[:1]:
        copy.start()
    for r in range(x_parts):
        x_copy(r).start()
    for copy in small[1:]:
        copy.start()
    for copy in kv_copies(0):
        copy.start()

    barrier = pltpu.get_barrier_semaphore()
    pl.semaphore_signal(barrier, inc=1, device_id={'sp': partner})
    for dirn in range(2):
        for k in range(CORES):
            pl.semaphore_signal(barrier, inc=1, device_id=device(neighbour(dirn), k))

    small[0].wait()
    for r in range(x_parts):
        x_copy(r).wait()
        if r == x_parts - 1:
            for idx in range(1, 3):
                for copy in kv_copies(idx):
                    copy.start()
        step_rows = 16
        for t in range(part_rows // step_rows):
            sl = slice(r * part_rows + t * step_rows, r * part_rows + (t + 1) * step_rows)
            xf = x_buf[sl, :].astype(F32)
            scale = lax.rsqrt(jnp.mean(xf * xf, axis=-1, keepdims=True) + EPS)
            for b in range(dim // lanes):
                cols = slice(b * lanes, (b + 1) * lanes)
                h_buf[core, sl, cols] = (xf[:, cols] * scale * ln_buf[b:b + 1, :].astype(F32)).astype(BF16)

    for copy in small[1:]:
        copy.wait()
    gain_t[...] = jnp.broadcast_to(gain_buf[0].astype(F32), (chip_rows, head)).T
    own_cols = pl.ds(pl.multiple_of(core * rows, rows), rows)
    cos_own = angle_t[0, :, own_cols].T
    sin_own = angle_t[1, :, own_cols].T
    cos_k[...] = jnp.concatenate([cos_own, cos_own], axis=1)
    sin_k[...] = jnp.concatenate([-sin_own, sin_own], axis=1)

    pl.semaphore_wait(barrier, 1 + 2 * CORES)
    h_copy = pltpu.make_async_remote_copy(h_buf.at[core], h_buf.at[core], h_ssem, h_rsem, device_id={'sp': partner})

    def first_copies(idx):
        owner = idx % 2
        pair = idx // 2
        src = stage.at[idx]
        dst = kv.at[chip, pl.ds(pair * 2, 2), core]
        up = pltpu.make_async_remote_copy(src, dst, first_ssem.at[0, idx], first_rsem.at[0, pair, core], device_id=device(neighbour(0), owner))
        down = pltpu.make_async_remote_copy(src, dst, first_ssem.at[1, idx], first_rsem.at[1, pair, core], device_id=device(neighbour(1), owner))
        across = pltpu.make_async_remote_copy(src, dst, d2d_ssem.at[pair], d2d_rsem.at[pair], device_id={'sp': partner})
        return ((up, chip < chips - 1), (down, chip < far), (across, owner != core))

    def project_kv(idx, carry):
        slot = idx % 3
        w_wait(slot)
        raw = dot(h_buf[core], w_buf[slot])

        @pl.when(idx == 0)
        def _():
            for copy in kv_copies(3):
                copy.start()

        @pl.when(idx > 0)
        def _():
            for copy in q_copies(idx - 1):
                copy.start()

        for e in range(2):
            t = raw[:, e * head:(e + 1) * head]
            t = t * lax.rsqrt(jnp.mean(t * t, axis=-1, keepdims=True) + EPS) * gain_buf[1].astype(F32)
            k_val = (t * cos_k[...] + pltpu.roll(t, half_head, 1) * sin_k[...]).astype(BF16)
            v_val = raw[:, width // 2 + e * head:width // 2 + (e + 1) * head].T.astype(BF16)
            stage[idx, e, 0] = k_val
            stage[idx, e, 1] = v_val

            @pl.when(idx % 2 == core)
            def _():
                kv[chip, (idx // 2) * 2 + e, core, 0] = k_val
                kv[chip, (idx // 2) * 2 + e, core, 1] = v_val

        for copy, cond in first_copies(idx):
            pl.when(cond)(copy.start)

        @pl.when(idx == 0)
        def _():
            h_copy.start()

        return carry

    lax.fori_loop(0, 4, project_kv, 0)
    h_copy.wait_recv()

    def item_of(dirn, d):
        return (chip + chips + (2 * dirn - 1) * d) % chips

    def arrives(dirn, d):
        return chip >= d if dirn == 0 else item_of(1, d) < far

    def goes_on(dirn, d):
        return arrives(dirn, d) & (chip < chips - 1) if dirn == 0 else arrives(dirn, d)

    def ring_copy(dirn, j, d, whole):
        item = item_of(dirn, d - 1)
        sem = (d - 2) * local_heads + j
        ref = kv.at[item, j] if whole else kv.at[item, j, dirn]
        return pltpu.make_async_remote_copy(ref, ref, ring_ssem.at[dirn, sem], ring_rsem.at[dirn, sem], device_id=device(neighbour(dirn), core))

    def landed(dirn, j, d, whole):
        item = item_of(dirn, d)
        sem = (d - 2) * local_heads + j
        ref = kv.at[item, j] if whole else kv.at[item, j, dirn]
        return pltpu.make_async_remote_copy(ref, ref, ring_ssem.at[dirn, sem], ring_rsem.at[dirn, sem], device_id=device(neighbour(dirn), core))

    def forward_first(j):
        for dirn in range(2):
            pl.when(goes_on(dirn, 1))(ring_copy(dirn, j, 2, True).start)

    def poll_first(pair):
        for dirn in range(2):
            @pl.when(arrives(dirn, 1))
            def _():
                for k in range(CORES):
                    pltpu.make_async_remote_copy(stage.at[0], kv.at[item_of(dirn, 1), pl.ds(pair * 2, 2), k], first_ssem.at[0, 0],
                                                 first_rsem.at[dirn, pair, k], device_id={'sp': partner}).wait_recv()

    def poll(s):
        j = lookup(HEAD_TABLE, s)
        d = lookup(HOP_TABLE, s) + 1
        for dirn in range(2):
            pl.when(arrives(dirn, d) & (d < far))(landed(dirn, j, d, True).wait_recv)
            pl.when(arrives(dirn, d) & (d == far))(landed(dirn, j, d, False).wait_recv)
            pl.when(goes_on(dirn, d) & (d + 1 < far))(ring_copy(dirn, j, d + 1, True).start)
            pl.when(goes_on(dirn, d) & (d + 1 == far))(ring_copy(dirn, j, d + 1, False).start)

    def drain(j, carry):
        for d in range(1, far):
            for dirn in range(2):
                pl.when(goes_on(dirn, d))(ring_copy(dirn, j, d + 1, d + 1 < far).wait_send)
        return carry

    def project_q(idx, carry):
        slot = (idx + 4) % 3
        w_wait(slot)
        raw = dot(h_buf[...].reshape(chip_rows, dim), w_buf[slot])

        @pl.when(idx == 0)
        def _():
            for copy in q_copies(3):
                copy.start()

        @pl.when(idx == local_heads - 1)
        def _():
            poll_first(0)
            forward_first(0)
            forward_first(1)

        for g in range(group):
            t = raw[:, g * head:(g + 1) * head].T
            t = t * lax.rsqrt(jnp.mean(t * t, axis=0, keepdims=True) + EPS) * gain_t[...]
            t1 = t[:half_head]
            t2 = t[half_head:]
            c = angle_t[0]
            s = angle_t[1]
            q_t[idx, :, g * chip_rows:(g + 1) * chip_rows] = jnp.concatenate([t1 * c - t2 * s, t2 * c + t1 * s], axis=0).astype(BF16)
        return carry

    lax.fori_loop(0, local_heads, project_q, 0)
    for k in range(len(stages)):
        for copy in wo_copies(k):
            copy.start()

    score_scale = (head ** -0.5) * LOG2E

    def attend(items, j, first=False, ahead=2):
        keys = [kv[item, j, :, 0].reshape(chip_rows, head) for item in items]
        vals = jnp.concatenate([kv[item, j, c, 1] for item in items for c in range(CORES)], axis=1)

        def scores_of(g):
            return [dot(k, q_t[j, :, g * chip_rows:(g + 1) * chip_rows]) for k in keys]

        pending = [scores_of(g) for g in range(ahead)]
        for g in range(group):
            cols = slice(g * chip_rows, (g + 1) * chip_rows)
            scores = pending[g]
            if first:
                key_pos = lax.broadcasted_iota(jnp.int32, scores[0].shape, 0)
                q_pos = lax.broadcasted_iota(jnp.int32, scores[0].shape, 1)
                scores = [jnp.where(key_pos <= q_pos, scores[0], -jnp.inf)]
            top = functools.reduce(jnp.maximum, [jnp.max(x.reshape(chip_rows // 8, 8, chip_rows), axis=0) for x in scores])
            top = jnp.max(top, axis=0, keepdims=True)
            if first:
                m_new = jnp.broadcast_to(top, (8, chip_rows))
            else:
                m_old = m_buf[j, :, cols]
                m_new = jnp.maximum(m_old, top)
            probs = [jnp.exp2((x.reshape(chip_rows // 8, 8, chip_rows) - m_new[None]) * score_scale) for x in scores]
            total = functools.reduce(jnp.add, [jnp.sum(p, axis=0) for p in probs])
            if g + ahead < group:
                pending.append(scores_of(g + ahead))
            mixed = dot(vals, jnp.concatenate([p.reshape(chip_rows, chip_rows).astype(BF16) for p in probs], axis=0))
            m_buf[j, :, cols] = m_new
            if first:
                l_buf[j, :, cols] = total
                o_t[j, :, cols] = mixed
            else:
                alpha = jnp.exp2((m_old - m_new) * score_scale)
                l_buf[j, :, cols] = l_buf[j, :, cols] * alpha + total
                old = o_t[j, :, cols].reshape(head // 8, 8, chip_rows)
                o_t[j, :, cols] = (old * alpha[None]).reshape(head, chip_rows) + mixed

    def diagonal(j, carry):
        @pl.when(j % 2 == 0)
        def _():
            pltpu.make_async_remote_copy(stage.at[0], kv.at[chip, pl.ds(j, 2), 1 - core], d2d_ssem.at[j // 2], d2d_rsem.at[j // 2],
                                         device_id={'sp': partner}).wait_recv()

        attend((chip,), j, first=True, ahead=group)
        return carry

    lax.fori_loop(0, local_heads, diagonal, 0)
    poll_first(1)

    def o_copy(k):
        cols = pl.ds(stages[k][0] * width, (stages[k][1] - stages[k][0]) * width)
        return pltpu.make_async_remote_copy(o_send.at[:, cols], o_all.at[core, :, cols], o_ssem.at[k], o_rsem.at[k], device_id={'sp': partner})

    def close_head(j):
        inv = 1.0 / jnp.sum(l_buf[j], axis=0, keepdims=True)
        for g in range(group):
            cols = slice(g * chip_rows, (g + 1) * chip_rows)
            o_val = (o_t[j, :, cols] * inv[:, cols]).T.astype(BF16)
            out_cols = slice(j * width + g * head, j * width + (g + 1) * head)
            o_all[core, :, out_cols] = jnp.where(core == 0, o_val[:rows], o_val[rows:])
            o_send[:, out_cols] = jnp.where(core == 0, o_val[rows:], o_val[:rows])

    def project_out(k, start, end):
        first_head, last_head = stages[k]
        wo_wait(k)
        o_copy(k).wait_recv()
        depth = slice(first_head * width, last_head * width)

        def block(n, carry):
            for w in range(wide // width):
                cols = pl.ds(pl.multiple_of(n * wide + w * width, width), width)
                total = x_buf[:, cols].astype(F32) if start else acc[:, cols]
                for c in range(CORES):
                    total = total + dot(o_all[c, :, depth], wo_buf[c * mixed_dim + depth.start:c * mixed_dim + depth.stop, cols])
                if end:
                    out_ref[:, cols] = total.astype(BF16)
                else:
                    acc[:, cols] = total
            return carry

        wide = dim // 2
        lax.fori_loop(0, dim // wide, block, 0)

    def ring_step(s, carry):
        @pl.when(s >= local_heads)
        def _():
            poll(s)

        for at, j in DEFERRED:
            @pl.when(s == at)
            def _():
                forward_first(j)

        j = lookup(HEAD_TABLE, s)
        d = lookup(HOP_TABLE, s) + 1
        both = (d < far) & (chip + d >= chips)

        @pl.when(both)
        def _():
            attend((item_of(0, d), item_of(1, d)), j)

        @pl.when((chip >= d) & jnp.logical_not(both))
        def _():
            attend((item_of(0, d),), j, ahead=group)

        @pl.when(s == EARLY_CLOSE)
        def _():
            for early in range(EARLY):
                close_head(early)
            o_copy(0).start()

        @pl.when(s == EARLY_OUT)
        def _():
            project_out(0, True, False)

        @pl.when(s == THIRD_CLOSE)
        def _():
            close_head(EARLY)
            o_copy(1).start()

        return carry

    lax.fori_loop(0, SLOTS, ring_step, 0)
    close_head(local_heads - 1)
    o_copy(2).start()
    project_out(1, False, False)
    project_out(2, False, True)

    h_copy.wait_send()
    for k in range(len(stages)):
        o_copy(k).wait_send()

    def drain_first(idx, carry):
        for copy, cond in first_copies(idx):
            pl.when(cond)(copy.wait_send)
        return carry

    lax.fori_loop(0, 4, drain_first, 0)
    lax.fori_loop(0, local_heads, drain, 0)


def solution(mesh):
    group_size = mesh.shape['sp']

    def device_step(hidden, ln_gain, w_q, w_k, w_v, w_o, q_gain, k_gain):
        rows, dim = hidden.shape
        head = q_gain.shape[0]
        half = head // 2
        chips = group_size // CORES
        local_heads = w_k.shape[1] // head // CORES
        width = w_q.shape[1] // CORES // local_heads
        chip_rows = rows * CORES
        inv_freq = THETA ** -(np.arange(half, dtype=np.float64) * (2.0 / head))
        angles = inv_freq[:, None] * np.arange(rows * group_size)[None, :]
        angle_all = jnp.asarray(np.stack([np.cos(angles), np.sin(angles)]).astype(np.float32))
        hbm = pl.BlockSpec(memory_space=pl.ANY)
        dma = pltpu.SemaphoreType.DMA
        wide = width // head * chip_rows
        return pl.pallas_call(
            functools.partial(kernel, group_size),
            out_shape=pltpu.VMEM((rows, dim), BF16),
            in_specs=[hbm] * 9,
            out_specs=pl.BlockSpec(memory_space=pltpu.VMEM),
            scratch_shapes=[
                pltpu.VMEM((rows, dim), BF16),
                pltpu.VMEM((CORES, rows, dim), BF16),
                pltpu.VMEM((3, dim, width), BF16),
                pltpu.VMEM(w_o.shape, BF16),
                pltpu.VMEM((chips, local_heads, CORES, 2, rows, head), BF16),
                pltpu.VMEM((4, 2, 2, rows, head), BF16),
                pltpu.VMEM((local_heads, head, wide), BF16),
                pltpu.VMEM((local_heads, head, wide), F32),
                pltpu.VMEM((local_heads, 8, wide), F32),
                pltpu.VMEM((local_heads, 8, wide), F32),
                pltpu.VMEM((CORES, rows, local_heads * width), BF16),
                pltpu.VMEM((rows, local_heads * width), BF16),
                pltpu.VMEM((rows, dim), F32),
                pltpu.VMEM((dim // LANES, LANES), BF16),
                pltpu.VMEM((2, 1, head), BF16),
                pltpu.VMEM((2, half, chip_rows), F32),
                pltpu.VMEM((head, chip_rows), F32),
                pltpu.VMEM((rows, head), F32),
                pltpu.VMEM((rows, head), F32),
                dma((2,)), dma((4,)), dma((3,)), dma((3,)), dma, dma,
                dma((2,)), dma((2,)),
                dma((2, 4)), dma((2, 2, CORES)),
                dma((2, (chips // 2 - 1) * local_heads)), dma((2, (chips // 2 - 1) * local_heads)),
                dma((3,)), dma((3,)),
            ],
            compiler_params=pltpu.CompilerParams(collective_id=0, has_side_effects=True, vmem_limit_bytes=VMEM_LIMIT),
        )(hidden, w_q, w_k, w_v, w_o, ln_gain.reshape(-1, LANES), q_gain[None, :], k_gain[None, :], angle_all)

    row_spec = P(('dp', 'sp'), None)
    return jax.shard_map(device_step, mesh=mesh, in_specs=(row_spec, P(), P(), P(), P(), P(), P(), P()), out_specs=row_spec, check_vma=False)
```

```python
import functools
import jax
import jax.numpy as jnp
import numpy as np
from jax import lax
from jax.experimental import pallas as pl
from jax.experimental.pallas import tpu as pltpu
from jax.sharding import PartitionSpec as P

EPS = 1e-6
THETA = 1000000.0
LOG2E = 1.4426950408889634
CORES = 2
LANES = 128
VMEM_LIMIT = 62 * 2 ** 20
BF16 = jnp.bfloat16
F32 = jnp.float32


def dot(a, b):
    return jnp.dot(a, b, preferred_element_type=F32)


ORDER = ((0, 1), (1, 1), (2, 1), (3, 1), (0, 2), (1, 2), (0, 3), (1, 3), (2, 2), (0, 4), (1, 4), (3, 2), (2, 3), (3, 3), (2, 4), (3, 4))
SLOTS = len(ORDER)
EARLY = 2
EARLY_CLOSE = 10
EARLY_OUT = 11
THIRD_CLOSE = 14
DEFERRED = ((5, 2), (7, 3))
NEAR, REST, WHOLE = 0, 1, 2


def slot_table(values):
    return tuple(sum(v << (2 * s) for s, v in enumerate(values[h:h + 8])) for h in (0, 8))


HEAD_TABLE = slot_table([j for j, _ in ORDER])
HOP_TABLE = slot_table([d - 1 for _, d in ORDER])


def lookup(table, s):
    return lax.shift_right_logical(jnp.where(s < 8, table[0], table[1]), 2 * (s % 8)) % 4


def kernel(group_size, x_hbm, wq, wk, wv, wo, ln_hbm, q_gain_hbm, k_gain_hbm, angle_hbm, out_ref,
           x_buf, h_buf, w_buf, wo_buf, kv, stage, q_t, o_t, m_buf, l_buf, o_all, o_send, acc,
           ln_buf, gain_buf, angle_t, gain_t, cos_k, sin_k,
           x_sem, small_sem, w_sem, wo_sem, h_ssem, h_rsem, d2d_ssem, d2d_rsem, first_ssem, first_rsem, ring_ssem, ring_rsem, o_ssem, o_rsem):
    chips = group_size // CORES
    me = lax.axis_index('sp')
    chip = me // CORES
    core = me % CORES
    partner = chip * CORES + (1 - core)
    rows, dim = x_buf.shape
    head = gain_buf.shape[2]
    half_head = head // 2
    width = w_buf.shape[2]
    local_heads = kv.shape[1]
    group = width // head
    chip_rows = rows * CORES
    far = chips // 2
    mixed_dim = local_heads * width
    lanes = ln_buf.shape[1]

    def device(c, k):
        return {'sp': c * CORES + k}

    def neighbour(dirn):
        return (chip + chips + 1 - 2 * dirn) % chips

    x_parts = x_sem.shape[0]
    part_rows = rows // x_parts

    def x_copy(r):
        sl = pl.ds(r * part_rows, part_rows)
        return pltpu.make_async_copy(x_hbm.at[sl, :], x_buf.at[sl, :], x_sem.at[r])

    chip_cols = pl.ds(pl.multiple_of(chip * chip_rows, chip_rows), chip_rows)
    small = (pltpu.make_async_copy(ln_hbm, ln_buf, small_sem.at[0]),
             pltpu.make_async_copy(q_gain_hbm, gain_buf.at[0], small_sem.at[1]),
             pltpu.make_async_copy(k_gain_hbm, gain_buf.at[1], small_sem.at[2]),
             pltpu.make_async_copy(angle_hbm.at[:, :, chip_cols], angle_t, small_sem.at[3]))

    def kv_copies(idx):
        pair = (idx % 2) * 2 + idx // 2
        cols = pl.ds(pl.multiple_of(pair * (width // 2), width // 2), width // 2)
        slot = idx % 3
        return (pltpu.make_async_copy(wk.at[:, cols], w_buf.at[slot, :, pl.ds(0, width // 2)], w_sem.at[slot, 0]),
                pltpu.make_async_copy(wv.at[:, cols], w_buf.at[slot, :, pl.ds(width // 2, width // 2)], w_sem.at[slot, 1]))

    def q_copies(idx):
        cols = pl.ds(pl.multiple_of((core * local_heads + idx) * width, width), width)
        slot = (idx + 4) % 3
        return tuple(pltpu.make_async_copy(wq.at[pl.ds(r * (dim // 2), dim // 2), cols],
                                           w_buf.at[slot, pl.ds(r * (dim // 2), dim // 2), :], w_sem.at[slot, r]) for r in range(2))

    stages = ((0, EARLY), (EARLY, EARLY + 1), (EARLY + 1, local_heads))

    def span_of(k, c):
        first, last = stages[k]
        return (CORES * first + c * (last - first)) * width, (last - first) * width

    def wo_copies(k):
        copies = []
        for c in range(CORES):
            at, size = span_of(k, c)
            source = pl.ds(c * mixed_dim + stages[k][0] * width, size)
            copies.append(pltpu.make_async_copy(wo.at[source, :], wo_buf.at[pl.ds(at, size), :], wo_sem.at[k]))
        return copies

    def wo_wait(k):
        at, size = span_of(k, 0)
        span = pl.ds(at, CORES * size)
        pltpu.make_async_copy(wo.at[span, :], wo_buf.at[span, :], wo_sem.at[k]).wait()

    for copy in small[:1]:
        copy.start()
    for r in range(x_parts):
        x_copy(r).start()
    for copy in small[1:]:
        copy.start()
    kv_copies(0)[0].start()

    barrier = pltpu.get_barrier_semaphore()
    pl.semaphore_signal(barrier, inc=1, device_id={'sp': partner})
    for dirn in range(2):
        for k in range(CORES):
            pl.semaphore_signal(barrier, inc=1, device_id=device(neighbour(dirn), k))

    small[0].wait()
    for r in range(x_parts):
        x_copy(r).wait()
        if r == 0:
            kv_copies(0)[1].start()
        if r == x_parts - 1:
            for idx in range(1, 3):
                for copy in kv_copies(idx):
                    copy.start()
        step_rows = 16
        for t in range(part_rows // step_rows):
            sl = slice(r * part_rows + t * step_rows, r * part_rows + (t + 1) * step_rows)
            xf = x_buf[sl, :].astype(F32)
            scale = lax.rsqrt(jnp.mean(xf * xf, axis=-1, keepdims=True) + EPS)
            for b in range(dim // lanes):
                cols = slice(b * lanes, (b + 1) * lanes)
                h_buf[core, sl, cols] = (xf[:, cols] * scale * ln_buf[b:b + 1, :].astype(F32)).astype(BF16)

    for copy in small[1:]:
        copy.wait()
    own_cols = pl.ds(pl.multiple_of(core * rows, rows), rows)
    cos_own = angle_t[0, :, own_cols].T
    sin_own = angle_t[1, :, own_cols].T
    cos_k[...] = jnp.concatenate([cos_own, cos_own], axis=1)
    sin_k[...] = jnp.concatenate([-sin_own, sin_own], axis=1)

    pl.semaphore_wait(barrier, 1 + 2 * CORES)
    h_copy = pltpu.make_async_remote_copy(h_buf.at[core], h_buf.at[core], h_ssem, h_rsem, device_id={'sp': partner})

    def first_copies(idx):
        owner = idx % 2
        pair = idx // 2
        src = stage.at[idx]
        dst = kv.at[chip, pl.ds(pair * 2, 2), core]
        up = pltpu.make_async_remote_copy(src, dst, first_ssem.at[0, idx], first_rsem.at[0, pair, core], device_id=device(neighbour(0), owner))
        down = pltpu.make_async_remote_copy(src, dst, first_ssem.at[1, idx], first_rsem.at[1, pair, core], device_id=device(neighbour(1), owner))
        across = pltpu.make_async_remote_copy(src, dst, d2d_ssem.at[pair], d2d_rsem.at[pair], device_id={'sp': partner})
        return ((up, chip < chips - 1), (down, chip < far), (across, owner != core))

    def project_kv(idx, carry):
        slot = idx % 3
        raws = []
        for part, copy in enumerate(kv_copies(idx)):
            copy.wait()
            cols = slice(part * (width // 2), (part + 1) * (width // 2))
            raws.append(dot(h_buf[core, :, :dim // 2], w_buf[slot, :dim // 2, cols]) + dot(h_buf[core, :, dim // 2:], w_buf[slot, dim // 2:, cols]))
        k_raw, v_raw = raws

        @pl.when(idx == 0)
        def _():
            for copy in kv_copies(3):
                copy.start()

        @pl.when(idx > 0)
        def _():
            for copy in q_copies(idx - 1):
                copy.start()

        for e in range(2):
            t = k_raw[:, e * head:(e + 1) * head]
            t = t * lax.rsqrt(jnp.mean(t * t, axis=-1, keepdims=True) + EPS) * gain_buf[1].astype(F32)
            k_val = (t * cos_k[...] + pltpu.roll(t, half_head, 1) * sin_k[...]).astype(BF16)
            v_val = v_raw[:, e * head:(e + 1) * head].T.astype(BF16)
            stage[idx, e, 0] = k_val
            stage[idx, e, 1] = v_val

            @pl.when(idx % 2 == core)
            def _():
                kv[chip, (idx // 2) * 2 + e, core, 0] = k_val
                kv[chip, (idx // 2) * 2 + e, core, 1] = v_val

        for copy, cond in first_copies(idx):
            pl.when(cond)(copy.start)

        @pl.when(idx == 0)
        def _():
            h_copy.start()

        return carry

    lax.fori_loop(0, 4, project_kv, 0)
    gain_t[...] = jnp.broadcast_to(gain_buf[0].astype(F32), (chip_rows, head)).T
    h_copy.wait_recv()

    def item_of(dirn, d):
        return (chip + chips + (2 * dirn - 1) * d) % chips

    def arrives(dirn, d):
        return chip >= d if dirn == 0 else item_of(1, d) < far

    def goes_on(dirn, d):
        return arrives(dirn, d) & (chip < chips - 1) if dirn == 0 else arrives(dirn, d)

    def ring_copy(dirn, j, d, item, part):
        half = (dirn, 1 - dirn, None)[part]
        sem = (d - 2) * local_heads + j + (2 * local_heads if part == REST else 0)
        ref = kv.at[item, j] if half is None else kv.at[item, j, half]
        return pltpu.make_async_remote_copy(ref, ref, ring_ssem.at[dirn, sem], ring_rsem.at[dirn, sem], device_id=device(neighbour(dirn), core))

    def outgoing(dirn, j, d, part):
        return ring_copy(dirn, j, d, item_of(dirn, d - 1), part)

    def landed(dirn, j, d, part):
        return ring_copy(dirn, j, d, item_of(dirn, d), part)

    def forward_first(j):
        for dirn in range(2):
            pl.when(goes_on(dirn, 1))(outgoing(dirn, j, 2, WHOLE).start)

    def poll_first(pair):
        for dirn in range(2):
            @pl.when(arrives(dirn, 1))
            def _():
                for k in range(CORES):
                    pltpu.make_async_remote_copy(stage.at[0], kv.at[item_of(dirn, 1), pl.ds(pair * 2, 2), k], first_ssem.at[0, 0],
                                                 first_rsem.at[dirn, pair, k], device_id={'sp': partner}).wait_recv()

    def poll(s):
        j = lookup(HEAD_TABLE, s)
        d = lookup(HOP_TABLE, s) + 1
        for dirn in range(2):
            @pl.when(arrives(dirn, 2) & (d == 2))
            def _():
                landed(dirn, j, 2, WHOLE).wait_recv()

            @pl.when(goes_on(dirn, 2) & (d == 2))
            def _():
                outgoing(dirn, j, 3, NEAR).start()
                outgoing(dirn, j, 3, REST).start()

            @pl.when(arrives(dirn, 3) & (d == 3))
            def _():
                landed(dirn, j, 3, NEAR).wait_recv()

            @pl.when(goes_on(dirn, 3) & (d == 3))
            def _():
                outgoing(dirn, j, 4, NEAR).start()

        for dirn in range(2):
            @pl.when(arrives(dirn, 3) & (d == 3))
            def _():
                landed(dirn, j, 3, REST).wait_recv()

            @pl.when(arrives(dirn, 4) & (d == 4))
            def _():
                landed(dirn, j, 4, NEAR).wait_recv()

    def drain(j, carry):
        for dirn in range(2):
            pl.when(goes_on(dirn, 1))(outgoing(dirn, j, 2, WHOLE).wait_send)
            pl.when(goes_on(dirn, 2))(outgoing(dirn, j, 3, NEAR).wait_send)
            pl.when(goes_on(dirn, 2))(outgoing(dirn, j, 3, REST).wait_send)
            pl.when(goes_on(dirn, 3))(outgoing(dirn, j, 4, NEAR).wait_send)
        return carry

    def project_q(idx, carry):
        slot = (idx + 4) % 3
        for copy in q_copies(idx):
            copy.wait()
        raw = dot(h_buf[...].reshape(chip_rows, dim), w_buf[slot])

        @pl.when(idx == 0)
        def _():
            for copy in q_copies(3):
                copy.start()

        @pl.when(idx == local_heads - 1)
        def _():
            poll_first(0)
            forward_first(0)
            forward_first(1)

        for g in range(group):
            t = raw[:, g * head:(g + 1) * head].T
            t = t * lax.rsqrt(jnp.mean(t * t, axis=0, keepdims=True) + EPS) * gain_t[...]
            t1 = t[:half_head]
            t2 = t[half_head:]
            c = angle_t[0]
            s = angle_t[1]
            q_t[idx, :, g * chip_rows:(g + 1) * chip_rows] = jnp.concatenate([t1 * c - t2 * s, t2 * c + t1 * s], axis=0).astype(BF16)
        return carry

    lax.fori_loop(0, local_heads, project_q, 0)
    for k in range(len(stages)):
        for copy in wo_copies(k):
            copy.start()

    score_scale = (head ** -0.5) * LOG2E

    def attend(items, j, first=False, ahead=2):
        keys = [kv[item, j, :, 0].reshape(chip_rows, head) for item in items]
        vals = jnp.concatenate([kv[item, j, c, 1] for item in items for c in range(CORES)], axis=1)

        def scores_of(g):
            return [dot(k, q_t[j, :, g * chip_rows:(g + 1) * chip_rows]) for k in keys]

        pending = [scores_of(g) for g in range(ahead)]
        for g in range(group):
            cols = slice(g * chip_rows, (g + 1) * chip_rows)
            scores = pending[g]
            if first:
                key_pos = lax.broadcasted_iota(jnp.int32, scores[0].shape, 0)
                q_pos = lax.broadcasted_iota(jnp.int32, scores[0].shape, 1)
                scores = [jnp.where(key_pos <= q_pos, scores[0], -jnp.inf)]
            top = functools.reduce(jnp.maximum, [jnp.max(x.reshape(chip_rows // 8, 8, chip_rows), axis=0) for x in scores])
            top = jnp.max(top, axis=0, keepdims=True)
            if first:
                m_new = jnp.broadcast_to(top, (8, chip_rows))
            else:
                m_old = m_buf[j, :, cols]
                m_new = jnp.maximum(m_old, top)
            probs = [jnp.exp2((x.reshape(chip_rows // 8, 8, chip_rows) - m_new[None]) * score_scale) for x in scores]
            total = functools.reduce(jnp.add, [jnp.sum(p, axis=0) for p in probs])
            if g + ahead < group:
                pending.append(scores_of(g + ahead))
            mixed = dot(vals, jnp.concatenate([p.reshape(chip_rows, chip_rows).astype(BF16) for p in probs], axis=0))
            m_buf[j, :, cols] = m_new
            if first:
                l_buf[j, :, cols] = total
                o_t[j, :, cols] = mixed
            else:
                alpha = jnp.exp2((m_old - m_new) * score_scale)
                l_buf[j, :, cols] = l_buf[j, :, cols] * alpha + total
                old = o_t[j, :, cols].reshape(head // 8, 8, chip_rows)
                o_t[j, :, cols] = (old * alpha[None]).reshape(head, chip_rows) + mixed

    def diagonal(j, carry):
        @pl.when(j % 2 == 0)
        def _():
            pltpu.make_async_remote_copy(stage.at[0], kv.at[chip, pl.ds(j, 2), 1 - core], d2d_ssem.at[j // 2], d2d_rsem.at[j // 2],
                                         device_id={'sp': partner}).wait_recv()

        attend((chip,), j, first=True, ahead=group)
        return carry

    lax.fori_loop(0, local_heads, diagonal, 0)
    poll_first(1)

    def o_copy(k):
        at, size = span_of(k, core)
        target = pl.ds(pl.multiple_of(at, head), size)
        return pltpu.make_async_remote_copy(o_send.at[:, pl.ds(stages[k][0] * width, size)], o_all.at[:, target], o_ssem.at[k], o_rsem.at[k],
                                            device_id={'sp': partner})

    def close_head(j):
        k = min(j // EARLY, 1) + max(0, j - EARLY)
        at = span_of(k, core)[0] + (j - stages[k][0]) * width
        inv = 1.0 / jnp.sum(l_buf[j], axis=0, keepdims=True)
        for g in range(group):
            cols = slice(g * chip_rows, (g + 1) * chip_rows)
            o_val = (o_t[j, :, cols] * inv[:, cols]).T.astype(BF16)
            o_all[:, pl.ds(pl.multiple_of(at + g * head, head), head)] = jnp.where(core == 0, o_val[:rows], o_val[rows:])
            o_send[:, j * width + g * head:j * width + (g + 1) * head] = jnp.where(core == 0, o_val[rows:], o_val[:rows])

    def project_out(k, start, end):
        wo_wait(k)
        o_copy(k).wait_recv()
        at, size = span_of(k, 0)
        depth = slice(at, at + CORES * size)

        def block(n, carry):
            for w in range(wide // width):
                cols = pl.ds(pl.multiple_of(n * wide + w * width, width), width)
                total = x_buf[:, cols].astype(F32) if start else acc[:, cols]
                total = total + dot(o_all[:, depth], wo_buf[depth, cols])
                if end:
                    out_ref[:, cols] = total.astype(BF16)
                else:
                    acc[:, cols] = total
            return carry

        wide = dim // 2
        lax.fori_loop(0, dim // wide, block, 0)

    def ring_step(s, carry):
        @pl.when(s >= local_heads)
        def _():
            poll(s)

        for at, j in DEFERRED:
            @pl.when(s == at)
            def _():
                forward_first(j)

        j = lookup(HEAD_TABLE, s)
        d = lookup(HOP_TABLE, s) + 1
        both = (d < far) & (chip + d >= chips)

        @pl.when(both)
        def _():
            attend((item_of(0, d), item_of(1, d)), j)

        @pl.when((chip >= d) & jnp.logical_not(both))
        def _():
            attend((item_of(0, d),), j, ahead=group)

        @pl.when(s == EARLY_CLOSE)
        def _():
            for early in range(EARLY):
                close_head(early)
            o_copy(0).start()

        @pl.when(s == EARLY_OUT)
        def _():
            project_out(0, True, False)

        @pl.when(s == THIRD_CLOSE)
        def _():
            close_head(EARLY)
            o_copy(1).start()

        return carry

    lax.fori_loop(0, SLOTS, ring_step, 0)
    close_head(local_heads - 1)
    o_copy(2).start()
    project_out(1, False, False)
    project_out(2, False, True)

    h_copy.wait_send()
    for k in range(len(stages)):
        o_copy(k).wait_send()

    def drain_first(idx, carry):
        for copy, cond in first_copies(idx):
            pl.when(cond)(copy.wait_send)
        return carry

    lax.fori_loop(0, 4, drain_first, 0)
    lax.fori_loop(0, local_heads, drain, 0)


def solution(mesh):
    group_size = mesh.shape['sp']

    def device_step(hidden, ln_gain, w_q, w_k, w_v, w_o, q_gain, k_gain):
        rows, dim = hidden.shape
        head = q_gain.shape[0]
        half = head // 2
        chips = group_size // CORES
        local_heads = w_k.shape[1] // head // CORES
        width = w_q.shape[1] // CORES // local_heads
        chip_rows = rows * CORES
        inv_freq = THETA ** -(np.arange(half, dtype=np.float64) * (2.0 / head))
        angles = inv_freq[:, None] * np.arange(rows * group_size)[None, :]
        angle_all = jnp.asarray(np.stack([np.cos(angles), np.sin(angles)]).astype(np.float32))
        hbm = pl.BlockSpec(memory_space=pl.ANY)
        dma = pltpu.SemaphoreType.DMA
        wide = width // head * chip_rows
        return pl.pallas_call(
            functools.partial(kernel, group_size),
            out_shape=pltpu.VMEM((rows, dim), BF16),
            in_specs=[hbm] * 9,
            out_specs=pl.BlockSpec(memory_space=pltpu.VMEM),
            scratch_shapes=[
                pltpu.VMEM((rows, dim), BF16),
                pltpu.VMEM((CORES, rows, dim), BF16),
                pltpu.VMEM((3, dim, width), BF16),
                pltpu.VMEM(w_o.shape, BF16),
                pltpu.VMEM((chips, local_heads, CORES, 2, rows, head), BF16),
                pltpu.VMEM((4, 2, 2, rows, head), BF16),
                pltpu.VMEM((local_heads, head, wide), BF16),
                pltpu.VMEM((local_heads, head, wide), F32),
                pltpu.VMEM((local_heads, 8, wide), F32),
                pltpu.VMEM((local_heads, 8, wide), F32),
                pltpu.VMEM((rows, w_o.shape[0]), BF16),
                pltpu.VMEM((rows, local_heads * width), BF16),
                pltpu.VMEM((rows, dim), F32),
                pltpu.VMEM((dim // LANES, LANES), BF16),
                pltpu.VMEM((2, 1, head), BF16),
                pltpu.VMEM((2, half, chip_rows), F32),
                pltpu.VMEM((head, chip_rows), F32),
                pltpu.VMEM((rows, head), F32),
                pltpu.VMEM((rows, head), F32),
                dma((2,)), dma((4,)), dma((3, 2)), dma((3,)), dma, dma,
                dma((2,)), dma((2,)),
                dma((2, 4)), dma((2, 2, CORES)),
                dma((2, 4 * local_heads)), dma((2, 4 * local_heads)),
                dma((3,)), dma((3,)),
            ],
            compiler_params=pltpu.CompilerParams(collective_id=0, has_side_effects=True, vmem_limit_bytes=VMEM_LIMIT),
        )(hidden, w_q, w_k, w_v, w_o, ln_gain.reshape(-1, LANES), q_gain[None, :], k_gain[None, :], angle_all)

    row_spec = P(('dp', 'sp'), None)
    return jax.shard_map(device_step, mesh=mesh, in_specs=(row_spec, P(), P(), P(), P(), P(), P(), P()), out_specs=row_spec, check_vma=False)
```

```python
import functools
import jax
import jax.numpy as jnp
import numpy as np
from jax import lax
from jax.experimental import pallas as pl
from jax.experimental.pallas import tpu as pltpu
from jax.sharding import PartitionSpec as P

EPS = 1e-6
THETA = 1000000.0
LOG2E = 1.4426950408889634
CORES = 2
LANES = 128
VMEM_LIMIT = 62 * 2 ** 20
BF16 = jnp.bfloat16
F32 = jnp.float32


def dot(a, b):
    return jnp.dot(a, b, preferred_element_type=F32)


ORDER = ((0, 1), (1, 1), (2, 1), (3, 1), (0, 2), (1, 2), (0, 3), (1, 3), (2, 2), (0, 4), (1, 4), (3, 2), (2, 3), (3, 3), (2, 4), (3, 4))
SLOTS = len(ORDER)
EARLY = 2
EARLY_CLOSE = 10
EARLY_OUT = 11
THIRD_CLOSE = 14
DEFERRED = ((5, 2), (7, 3))
NEAR, REST, WHOLE = 0, 1, 2


def slot_table(values):
    return tuple(sum(v << (2 * s) for s, v in enumerate(values[h:h + 8])) for h in (0, 8))


HEAD_TABLE = slot_table([j for j, _ in ORDER])
HOP_TABLE = slot_table([d - 1 for _, d in ORDER])


def lookup(table, s):
    return lax.shift_right_logical(jnp.where(s < 8, table[0], table[1]), 2 * (s % 8)) % 4


def kernel(group_size, x_hbm, wq, wk, wv, wo, ln_hbm, q_gain_hbm, k_gain_hbm, angle_hbm, out_ref,
           x_buf, h_buf, w_buf, wo_buf, kv, stage, q_t, o_t, m_buf, l_buf, o_all, o_send, acc,
           ln_buf, gain_buf, angle_t, gain_t, cos_k, sin_k,
           x_sem, small_sem, w_sem, wo_sem, h_ssem, h_rsem, d2d_ssem, d2d_rsem, first_ssem, first_rsem, ring_ssem, ring_rsem, o_ssem, o_rsem):
    chips = group_size // CORES
    me = lax.axis_index('sp')
    chip = me // CORES
    core = me % CORES
    partner = chip * CORES + (1 - core)
    rows, dim = x_buf.shape
    head = gain_buf.shape[2]
    half_head = head // 2
    width = w_buf.shape[2]
    local_heads = kv.shape[1]
    group = width // head
    chip_rows = rows * CORES
    far = chips // 2
    mixed_dim = local_heads * width
    lanes = ln_buf.shape[1]

    def device(c, k):
        return {'sp': c * CORES + k}

    def neighbour(dirn):
        return (chip + chips + 1 - 2 * dirn) % chips

    x_parts = x_sem.shape[0]
    part_rows = rows // x_parts

    def x_copy(r):
        sl = pl.ds(r * part_rows, part_rows)
        return pltpu.make_async_copy(x_hbm.at[sl, :], x_buf.at[sl, :], x_sem.at[r])

    chip_cols = pl.ds(pl.multiple_of(chip * chip_rows, chip_rows), chip_rows)
    small = (pltpu.make_async_copy(ln_hbm, ln_buf, small_sem.at[0]),
             pltpu.make_async_copy(q_gain_hbm, gain_buf.at[0], small_sem.at[1]),
             pltpu.make_async_copy(k_gain_hbm, gain_buf.at[1], small_sem.at[2]),
             pltpu.make_async_copy(angle_hbm.at[:, :, chip_cols], angle_t, small_sem.at[3]))

    def kv_copies(idx):
        pair = (idx % 2) * 2 + idx // 2
        cols = pl.ds(pl.multiple_of(pair * (width // 2), width // 2), width // 2)
        slot = idx % 3
        return (pltpu.make_async_copy(wk.at[:, cols], w_buf.at[slot, :, pl.ds(0, width // 2)], w_sem.at[slot, 0]),
                pltpu.make_async_copy(wv.at[:, cols], w_buf.at[slot, :, pl.ds(width // 2, width // 2)], w_sem.at[slot, 1]))

    def q_copies(idx):
        cols = pl.ds(pl.multiple_of((core * local_heads + idx) * width, width), width)
        slot = (idx + 4) % 3
        return tuple(pltpu.make_async_copy(wq.at[pl.ds(r * (dim // 2), dim // 2), cols],
                                           w_buf.at[slot, pl.ds(r * (dim // 2), dim // 2), :], w_sem.at[slot, r]) for r in range(2))

    stages = ((0, EARLY), (EARLY, EARLY + 1), (EARLY + 1, local_heads))

    def span_of(k, c):
        first, last = stages[k]
        return (CORES * first + c * (last - first)) * width, (last - first) * width

    def wo_copies(k):
        copies = []
        for c in range(CORES):
            at, size = span_of(k, c)
            source = pl.ds(c * mixed_dim + stages[k][0] * width, size)
            copies.append(pltpu.make_async_copy(wo.at[source, :], wo_buf.at[pl.ds(at, size), :], wo_sem.at[k]))
        return copies

    def wo_wait(k):
        at, size = span_of(k, 0)
        span = pl.ds(at, CORES * size)
        pltpu.make_async_copy(wo.at[span, :], wo_buf.at[span, :], wo_sem.at[k]).wait()

    for copy in small[:1]:
        copy.start()
    for r in range(x_parts):
        x_copy(r).start()
    for copy in small[1:]:
        copy.start()
    kv_copies(0)[0].start()

    barrier = pltpu.get_barrier_semaphore()
    pl.semaphore_signal(barrier, inc=1, device_id={'sp': partner})
    for dirn in range(2):
        for k in range(CORES):
            pl.semaphore_signal(barrier, inc=1, device_id=device(neighbour(dirn), k))

    small[0].wait()
    for r in range(x_parts):
        x_copy(r).wait()
        if r == 0:
            kv_copies(0)[1].start()
        if r == x_parts - 1:
            for idx in range(1, 3):
                for copy in kv_copies(idx):
                    copy.start()
        step_rows = 16
        for t in range(part_rows // step_rows):
            sl = slice(r * part_rows + t * step_rows, r * part_rows + (t + 1) * step_rows)
            xf = x_buf[sl, :].astype(F32)
            scale = lax.rsqrt(jnp.mean(xf * xf, axis=-1, keepdims=True) + EPS)
            for b in range(dim // lanes):
                cols = slice(b * lanes, (b + 1) * lanes)
                h_buf[core, sl, cols] = (xf[:, cols] * scale * ln_buf[b:b + 1, :].astype(F32)).astype(BF16)

    for copy in small[1:]:
        copy.wait()
    own_cols = pl.ds(pl.multiple_of(core * rows, rows), rows)
    cos_own = angle_t[0, :, own_cols].T
    sin_own = angle_t[1, :, own_cols].T
    cos_k[...] = jnp.concatenate([cos_own, cos_own], axis=1)
    sin_k[...] = jnp.concatenate([-sin_own, sin_own], axis=1)

    pl.semaphore_wait(barrier, 1 + 2 * CORES)
    h_copy = pltpu.make_async_remote_copy(h_buf.at[core], h_buf.at[core], h_ssem, h_rsem, device_id={'sp': partner})

    def first_copies(idx):
        owner = idx % 2
        pair = idx // 2
        src = stage.at[idx]
        dst = kv.at[chip, pl.ds(pair * 2, 2), core]
        up = pltpu.make_async_remote_copy(src, dst, first_ssem.at[0, idx], first_rsem.at[0, pair, core], device_id=device(neighbour(0), owner))
        down = pltpu.make_async_remote_copy(src, dst, first_ssem.at[1, idx], first_rsem.at[1, pair, core], device_id=device(neighbour(1), owner))
        across = pltpu.make_async_remote_copy(src, dst, d2d_ssem.at[pair], d2d_rsem.at[pair], device_id={'sp': partner})
        return ((up, chip < chips - 1), (down, chip < far), (across, owner != core))

    def project_kv(idx, carry):
        slot = idx % 3
        for copy in kv_copies(idx):
            copy.wait()
        raw = dot(h_buf[core], w_buf[slot])

        @pl.when(idx == 0)
        def _():
            for copy in kv_copies(3):
                copy.start()

        @pl.when(idx > 0)
        def _():
            for copy in q_copies(idx - 1):
                copy.start()

        for e in range(2):
            t = raw[:, e * head:(e + 1) * head]
            t = t * lax.rsqrt(jnp.mean(t * t, axis=-1, keepdims=True) + EPS) * gain_buf[1].astype(F32)
            k_val = (t * cos_k[...] + pltpu.roll(t, half_head, 1) * sin_k[...]).astype(BF16)
            v_val = raw[:, width // 2 + e * head:width // 2 + (e + 1) * head].T.astype(BF16)
            stage[idx, e, 0] = k_val
            stage[idx, e, 1] = v_val

            @pl.when(idx % 2 == core)
            def _():
                kv[chip, (idx // 2) * 2 + e, core, 0] = k_val
                kv[chip, (idx // 2) * 2 + e, core, 1] = v_val

        for copy, cond in first_copies(idx):
            pl.when(cond)(copy.start)

        @pl.when(idx == 0)
        def _():
            h_copy.start()

        return carry

    lax.fori_loop(0, 4, project_kv, 0)
    gain_t[...] = jnp.broadcast_to(gain_buf[0].astype(F32), (chip_rows, head)).T
    h_copy.wait_recv()

    def item_of(dirn, d):
        return (chip + chips + (2 * dirn - 1) * d) % chips

    def arrives(dirn, d):
        return chip >= d if dirn == 0 else item_of(1, d) < far

    def goes_on(dirn, d):
        return arrives(dirn, d) & (chip < chips - 1) if dirn == 0 else arrives(dirn, d)

    def ring_copy(dirn, j, d, item, part):
        half = (dirn, 1 - dirn, None)[part]
        sem = (d - 2) * local_heads + j + (2 * local_heads if part == REST else 0)
        ref = kv.at[item, j] if half is None else kv.at[item, j, half]
        return pltpu.make_async_remote_copy(ref, ref, ring_ssem.at[dirn, sem], ring_rsem.at[dirn, sem], device_id=device(neighbour(dirn), core))

    def outgoing(dirn, j, d, part):
        return ring_copy(dirn, j, d, item_of(dirn, d - 1), part)

    def landed(dirn, j, d, part):
        return ring_copy(dirn, j, d, item_of(dirn, d), part)

    def forward_first(j):
        for dirn in range(2):
            pl.when(goes_on(dirn, 1))(outgoing(dirn, j, 2, WHOLE).start)

    def poll_first(pair):
        for dirn in range(2):
            @pl.when(arrives(dirn, 1))
            def _():
                for k in range(CORES):
                    pltpu.make_async_remote_copy(stage.at[0], kv.at[item_of(dirn, 1), pl.ds(pair * 2, 2), k], first_ssem.at[0, 0],
                                                 first_rsem.at[dirn, pair, k], device_id={'sp': partner}).wait_recv()

    def poll_near(s):
        j = lookup(HEAD_TABLE, s)
        d = lookup(HOP_TABLE, s) + 1
        for dirn in range(2):
            @pl.when(arrives(dirn, 2) & (d == 2))
            def _():
                landed(dirn, j, 2, WHOLE).wait_recv()

            @pl.when(goes_on(dirn, 2) & (d == 2))
            def _():
                outgoing(dirn, j, 3, NEAR).start()
                outgoing(dirn, j, 3, REST).start()

            @pl.when(arrives(dirn, 3) & (d == 3))
            def _():
                landed(dirn, j, 3, NEAR).wait_recv()

            @pl.when(goes_on(dirn, 3) & (d == 3))
            def _():
                outgoing(dirn, j, 4, NEAR).start()

    def poll_rest(s):
        j = lookup(HEAD_TABLE, s)
        d = lookup(HOP_TABLE, s) + 1
        for dirn in range(2):
            @pl.when(arrives(dirn, 3) & (d == 3))
            def _():
                landed(dirn, j, 3, REST).wait_recv()

            @pl.when(arrives(dirn, 4) & (d == 4))
            def _():
                landed(dirn, j, 4, NEAR).wait_recv()

    def drain(j, carry):
        for dirn in range(2):
            pl.when(goes_on(dirn, 1))(outgoing(dirn, j, 2, WHOLE).wait_send)
            pl.when(goes_on(dirn, 2))(outgoing(dirn, j, 3, NEAR).wait_send)
            pl.when(goes_on(dirn, 2))(outgoing(dirn, j, 3, REST).wait_send)
            pl.when(goes_on(dirn, 3))(outgoing(dirn, j, 4, NEAR).wait_send)
        return carry

    def project_q(idx, carry):
        slot = (idx + 4) % 3
        for copy in q_copies(idx):
            copy.wait()
        raw = dot(h_buf[...].reshape(chip_rows, dim), w_buf[slot])

        @pl.when(idx == 0)
        def _():
            for copy in q_copies(3):
                copy.start()

        @pl.when(idx == local_heads - 1)
        def _():
            poll_first(0)
            forward_first(0)
            forward_first(1)

        for g in range(group):
            t = raw[:, g * head:(g + 1) * head].T
            t = t * lax.rsqrt(jnp.mean(t * t, axis=0, keepdims=True) + EPS) * gain_t[...]
            t1 = t[:half_head]
            t2 = t[half_head:]
            c = angle_t[0]
            s = angle_t[1]
            q_t[idx, :, g * chip_rows:(g + 1) * chip_rows] = jnp.concatenate([t1 * c - t2 * s, t2 * c + t1 * s], axis=0).astype(BF16)
        return carry

    lax.fori_loop(0, local_heads, project_q, 0)
    for k in range(len(stages)):
        for copy in wo_copies(k):
            copy.start()

    score_scale = (head ** -0.5) * LOG2E

    def attend(items, j, first=False, ahead=2):
        keys = [kv[item, j, :, 0].reshape(chip_rows, head) for item in items]
        vals = jnp.concatenate([kv[item, j, c, 1] for item in items for c in range(CORES)], axis=1)

        def scores_of(g):
            return [dot(k, q_t[j, :, g * chip_rows:(g + 1) * chip_rows]) for k in keys]

        pending = [scores_of(g) for g in range(ahead)]
        for g in range(group):
            cols = slice(g * chip_rows, (g + 1) * chip_rows)
            scores = pending[g]
            if first:
                key_pos = lax.broadcasted_iota(jnp.int32, scores[0].shape, 0)
                q_pos = lax.broadcasted_iota(jnp.int32, scores[0].shape, 1)
                scores = [jnp.where(key_pos <= q_pos, scores[0], -jnp.inf)]
            top = functools.reduce(jnp.maximum, [jnp.max(x.reshape(chip_rows // 8, 8, chip_rows), axis=0) for x in scores])
            top = jnp.max(top, axis=0, keepdims=True)
            if first:
                m_new = jnp.broadcast_to(top, (8, chip_rows))
            else:
                m_old = m_buf[j, :, cols]
                m_new = jnp.maximum(m_old, top)
            probs = [jnp.exp2((x.reshape(chip_rows // 8, 8, chip_rows) - m_new[None]) * score_scale) for x in scores]
            total = functools.reduce(jnp.add, [jnp.sum(p, axis=0) for p in probs])
            if g + ahead < group:
                pending.append(scores_of(g + ahead))
            mixed = dot(vals, jnp.concatenate([p.reshape(chip_rows, chip_rows).astype(BF16) for p in probs], axis=0))
            m_buf[j, :, cols] = m_new
            if first:
                l_buf[j, :, cols] = total
                o_t[j, :, cols] = mixed
            else:
                alpha = jnp.exp2((m_old - m_new) * score_scale)
                l_buf[j, :, cols] = l_buf[j, :, cols] * alpha + total
                old = o_t[j, :, cols].reshape(head // 8, 8, chip_rows)
                o_t[j, :, cols] = (old * alpha[None]).reshape(head, chip_rows) + mixed

    def diagonal(j, carry):
        @pl.when(j % 2 == 0)
        def _():
            pltpu.make_async_remote_copy(stage.at[0], kv.at[chip, pl.ds(j, 2), 1 - core], d2d_ssem.at[j // 2], d2d_rsem.at[j // 2],
                                         device_id={'sp': partner}).wait_recv()

        attend((chip,), j, first=True, ahead=group)
        return carry

    lax.fori_loop(0, local_heads, diagonal, 0)
    poll_first(1)

    def o_copy(k):
        at, size = span_of(k, core)
        target = pl.ds(pl.multiple_of(at, head), size)
        return pltpu.make_async_remote_copy(o_send.at[:, pl.ds(stages[k][0] * width, size)], o_all.at[:, target], o_ssem.at[k], o_rsem.at[k],
                                            device_id={'sp': partner})

    def close_head(j):
        k = min(j // EARLY, 1) + max(0, j - EARLY)
        at = span_of(k, core)[0] + (j - stages[k][0]) * width
        inv = 1.0 / jnp.sum(l_buf[j], axis=0, keepdims=True)
        for g in range(group):
            cols = slice(g * chip_rows, (g + 1) * chip_rows)
            o_val = (o_t[j, :, cols] * inv[:, cols]).T.astype(BF16)
            o_all[:, pl.ds(pl.multiple_of(at + g * head, head), head)] = jnp.where(core == 0, o_val[:rows], o_val[rows:])
            o_send[:, j * width + g * head:j * width + (g + 1) * head] = jnp.where(core == 0, o_val[rows:], o_val[:rows])

    def project_out(k, start, end, half=None):
        if half in (None, 0):
            wo_wait(k)
            o_copy(k).wait_recv()
        at, size = span_of(k, 0)
        depth = slice(at, at + CORES * size)

        def block(n, carry):
            for w in range(wide // width):
                cols = pl.ds(n * wide + w * width, width) if isinstance(n, int) else pl.ds(pl.multiple_of(n * wide + w * width, width), width)
                total = x_buf[:, cols].astype(F32) if start else acc[:, cols]
                total = total + dot(o_all[:, depth], wo_buf[depth, cols])
                if end:
                    out_ref[:, cols] = total.astype(BF16)
                else:
                    acc[:, cols] = total
            return carry

        wide = dim // 2
        if half is None:
            lax.fori_loop(0, dim // wide, block, 0)
        else:
            block(half, 0)

    def ring_step(s, carry):
        @pl.when(s >= local_heads)
        def _():
            poll_rest(s)

        j = lookup(HEAD_TABLE, s)
        d = lookup(HOP_TABLE, s) + 1
        both = (d < far) & (chip + d >= chips)

        @pl.when(both)
        def _():
            attend((item_of(0, d), item_of(1, d)), j)

        @pl.when((chip >= d) & jnp.logical_not(both))
        def _():
            attend((item_of(0, d),), j, ahead=group)

        @pl.when((s + 1 >= local_heads) & (s + 1 < SLOTS))
        def _():
            poll_near(s + 1)

        for at, late in DEFERRED:
            @pl.when(s + 1 == at)
            def _():
                forward_first(late)

        @pl.when(s == EARLY_CLOSE)
        def _():
            for early in range(EARLY):
                close_head(early)
            o_copy(0).start()

        for half in range(2):
            @pl.when(s == EARLY_OUT + half)
            def _():
                project_out(0, True, False, half)

        @pl.when(s == THIRD_CLOSE)
        def _():
            close_head(EARLY)
            o_copy(1).start()

        return carry

    lax.fori_loop(0, SLOTS, ring_step, 0)
    close_head(local_heads - 1)
    o_copy(2).start()
    project_out(1, False, False)
    project_out(2, False, True)

    h_copy.wait_send()
    for k in range(len(stages)):
        o_copy(k).wait_send()

    def drain_first(idx, carry):
        for copy, cond in first_copies(idx):
            pl.when(cond)(copy.wait_send)
        return carry

    lax.fori_loop(0, 4, drain_first, 0)
    lax.fori_loop(0, local_heads, drain, 0)


def solution(mesh):
    group_size = mesh.shape['sp']

    def device_step(hidden, ln_gain, w_q, w_k, w_v, w_o, q_gain, k_gain):
        rows, dim = hidden.shape
        head = q_gain.shape[0]
        half = head // 2
        chips = group_size // CORES
        local_heads = w_k.shape[1] // head // CORES
        width = w_q.shape[1] // CORES // local_heads
        chip_rows = rows * CORES
        inv_freq = THETA ** -(np.arange(half, dtype=np.float64) * (2.0 / head))
        angles = inv_freq[:, None] * np.arange(rows * group_size)[None, :]
        angle_all = jnp.asarray(np.stack([np.cos(angles), np.sin(angles)]).astype(np.float32))
        hbm = pl.BlockSpec(memory_space=pl.ANY)
        dma = pltpu.SemaphoreType.DMA
        wide = width // head * chip_rows
        return pl.pallas_call(
            functools.partial(kernel, group_size),
            out_shape=pltpu.VMEM((rows, dim), BF16),
            in_specs=[hbm] * 9,
            out_specs=pl.BlockSpec(memory_space=pltpu.VMEM),
            scratch_shapes=[
                pltpu.VMEM((rows, dim), BF16),
                pltpu.VMEM((CORES, rows, dim), BF16),
                pltpu.VMEM((3, dim, width), BF16),
                pltpu.VMEM(w_o.shape, BF16),
                pltpu.VMEM((chips, local_heads, CORES, 2, rows, head), BF16),
                pltpu.VMEM((4, 2, 2, rows, head), BF16),
                pltpu.VMEM((local_heads, head, wide), BF16),
                pltpu.VMEM((local_heads, head, wide), F32),
                pltpu.VMEM((local_heads, 8, wide), F32),
                pltpu.VMEM((local_heads, 8, wide), F32),
                pltpu.VMEM((rows, w_o.shape[0]), BF16),
                pltpu.VMEM((rows, local_heads * width), BF16),
                pltpu.VMEM((rows, dim), F32),
                pltpu.VMEM((dim // LANES, LANES), BF16),
                pltpu.VMEM((2, 1, head), BF16),
                pltpu.VMEM((2, half, chip_rows), F32),
                pltpu.VMEM((head, chip_rows), F32),
                pltpu.VMEM((rows, head), F32),
                pltpu.VMEM((rows, head), F32),
                dma((2,)), dma((4,)), dma((3, 2)), dma((3,)), dma, dma,
                dma((2,)), dma((2,)),
                dma((2, 4)), dma((2, 2, CORES)),
                dma((2, 4 * local_heads)), dma((2, 4 * local_heads)),
                dma((3,)), dma((3,)),
            ],
            compiler_params=pltpu.CompilerParams(collective_id=0, has_side_effects=True, vmem_limit_bytes=VMEM_LIMIT),
        )(hidden, w_q, w_k, w_v, w_o, ln_gain.reshape(-1, LANES), q_gain[None, :], k_gain[None, :], angle_all)

    row_spec = P(('dp', 'sp'), None)
    return jax.shard_map(device_step, mesh=mesh, in_specs=(row_spec, P(), P(), P(), P(), P(), P(), P()), out_specs=row_spec, check_vma=False)
```

```python
import functools
import jax
import jax.numpy as jnp
import numpy as np
from jax import lax
from jax.experimental import pallas as pl
from jax.experimental.pallas import tpu as pltpu
from jax.sharding import PartitionSpec as P

EPS = 1e-6
THETA = 1000000.0
LOG2E = 1.4426950408889634
CORES = 2
LANES = 128
VMEM_LIMIT = 62 * 2 ** 20
BF16 = jnp.bfloat16
F32 = jnp.float32


def dot(a, b):
    return jnp.dot(a, b, preferred_element_type=F32)


ORDER = ((0, 1), (1, 1), (2, 1), (3, 1), (0, 2), (1, 2), (0, 3), (1, 3), (2, 2), (0, 4), (1, 4), (3, 2), (2, 3), (3, 3), (2, 4), (3, 4))
SLOTS = len(ORDER)
EARLY = 2
EARLY_CLOSE = 10
EARLY_OUT = 11
THIRD_CLOSE = 14
DEFERRED = ((5, 2), (7, 3))
NEAR, REST, WHOLE = 0, 1, 2


def slot_table(values):
    return tuple(sum(v << (2 * s) for s, v in enumerate(values[h:h + 8])) for h in (0, 8))


HEAD_TABLE = slot_table([j for j, _ in ORDER])
HOP_TABLE = slot_table([d - 1 for _, d in ORDER])


def lookup(table, s):
    return lax.shift_right_logical(jnp.where(s < 8, table[0], table[1]), 2 * (s % 8)) % 4


def kernel(group_size, x_hbm, wq, wk, wv, wo, ln_hbm, q_gain_hbm, k_gain_hbm, angle_hbm, out_ref,
           x_buf, h_buf, w_buf, wo_buf, kv, stage, q_t, o_t, m_buf, l_buf, o_all, o_send, acc,
           ln_buf, gain_buf, angle_t, gain_t, cos_k, sin_k,
           x_sem, small_sem, w_sem, wo_sem, h_ssem, h_rsem, d2d_ssem, d2d_rsem, first_ssem, first_rsem, ring_ssem, ring_rsem, o_ssem, o_rsem):
    chips = group_size // CORES
    me = lax.axis_index('sp')
    chip = me // CORES
    core = me % CORES
    partner = chip * CORES + (1 - core)
    rows, dim = x_buf.shape
    head = gain_buf.shape[2]
    half_head = head // 2
    width = w_buf.shape[2]
    local_heads = kv.shape[1]
    group = width // head
    chip_rows = rows * CORES
    far = chips // 2
    mixed_dim = local_heads * width
    lanes = ln_buf.shape[1]

    def device(c, k):
        return {'sp': c * CORES + k}

    def neighbour(dirn):
        return (chip + chips + 1 - 2 * dirn) % chips

    x_parts = x_sem.shape[0]
    part_rows = rows // x_parts

    def x_copy(r):
        sl = pl.ds(r * part_rows, part_rows)
        return pltpu.make_async_copy(x_hbm.at[sl, :], x_buf.at[sl, :], x_sem.at[r])

    chip_cols = pl.ds(pl.multiple_of(chip * chip_rows, chip_rows), chip_rows)
    small = (pltpu.make_async_copy(ln_hbm, ln_buf, small_sem.at[0]),
             pltpu.make_async_copy(q_gain_hbm, gain_buf.at[0], small_sem.at[1]),
             pltpu.make_async_copy(k_gain_hbm, gain_buf.at[1], small_sem.at[2]),
             pltpu.make_async_copy(angle_hbm.at[:, :, chip_cols], angle_t, small_sem.at[3]))

    def kv_copies(idx):
        pair = (idx % 2) * 2 + idx // 2
        cols = pl.ds(pl.multiple_of(pair * (width // 2), width // 2), width // 2)
        slot = idx % 3
        return (pltpu.make_async_copy(wk.at[:, cols], w_buf.at[slot, :, pl.ds(0, width // 2)], w_sem.at[slot, 0]),
                pltpu.make_async_copy(wv.at[:, cols], w_buf.at[slot, :, pl.ds(width // 2, width // 2)], w_sem.at[slot, 1]))

    def lead_copies(e):
        cols = pl.ds(e * head, head)
        return tuple(pltpu.make_async_copy(w.at[:, cols], w_buf.at[0, :, pl.ds((2 * e + part) * head, head)], w_sem.at[0, e])
                     for part, w in enumerate((wk, wv)))

    def lead_wait(e):
        pltpu.make_async_copy(wk.at[:, pl.ds(0, 2 * head)], w_buf.at[0, :, pl.ds(2 * e * head, 2 * head)], w_sem.at[0, e]).wait()

    def q_copies(idx):
        cols = pl.ds(pl.multiple_of((core * local_heads + idx) * width, width), width)
        slot = (idx + 4) % 3
        return tuple(pltpu.make_async_copy(wq.at[pl.ds(r * (dim // 2), dim // 2), cols],
                                           w_buf.at[slot, pl.ds(r * (dim // 2), dim // 2), :], w_sem.at[slot, r]) for r in range(2))

    stages = ((0, EARLY), (EARLY, EARLY + 1), (EARLY + 1, local_heads))

    def span_of(k, c):
        first, last = stages[k]
        return (CORES * first + c * (last - first)) * width, (last - first) * width

    def wo_copies(k):
        copies = []
        for c in range(CORES):
            at, size = span_of(k, c)
            source = pl.ds(c * mixed_dim + stages[k][0] * width, size)
            copies.append(pltpu.make_async_copy(wo.at[source, :], wo_buf.at[pl.ds(at, size), :], wo_sem.at[k]))
        return copies

    def wo_wait(k):
        at, size = span_of(k, 0)
        span = pl.ds(at, CORES * size)
        pltpu.make_async_copy(wo.at[span, :], wo_buf.at[span, :], wo_sem.at[k]).wait()

    for copy in small[:1]:
        copy.start()
    for r in range(x_parts):
        x_copy(r).start()
    for copy in small[1:]:
        copy.start()
    for copy in lead_copies(0):
        copy.start()

    barrier = pltpu.get_barrier_semaphore()
    pl.semaphore_signal(barrier, inc=1, device_id={'sp': partner})
    for dirn in range(2):
        for k in range(CORES):
            pl.semaphore_signal(barrier, inc=1, device_id=device(neighbour(dirn), k))

    small[0].wait()
    for r in range(x_parts):
        x_copy(r).wait()
        if r == 0:
            for copy in lead_copies(1):
                copy.start()
        if r == x_parts - 1:
            for copy in kv_copies(1):
                copy.start()
        step_rows = 16
        for t in range(part_rows // step_rows):
            sl = slice(r * part_rows + t * step_rows, r * part_rows + (t + 1) * step_rows)
            xf = x_buf[sl, :].astype(F32)
            scale = lax.rsqrt(jnp.mean(xf * xf, axis=-1, keepdims=True) + EPS)
            for b in range(dim // lanes):
                cols = slice(b * lanes, (b + 1) * lanes)
                h_buf[core, sl, cols] = (xf[:, cols] * scale * ln_buf[b:b + 1, :].astype(F32)).astype(BF16)

    for copy in small[1:]:
        copy.wait()
    own_cols = pl.ds(pl.multiple_of(core * rows, rows), rows)
    cos_own = angle_t[0, :, own_cols].T
    sin_own = angle_t[1, :, own_cols].T
    cos_k[...] = jnp.concatenate([cos_own, cos_own], axis=1)
    sin_k[...] = jnp.concatenate([-sin_own, sin_own], axis=1)

    pl.semaphore_wait(barrier, 1 + 2 * CORES)
    h_copy = pltpu.make_async_remote_copy(h_buf.at[core], h_buf.at[core], h_ssem, h_rsem, device_id={'sp': partner})

    def first_copies(idx, e=None):
        owner = idx % 2
        pair = idx // 2
        src = stage.at[idx] if e is None else stage.at[idx, e]
        dst = kv.at[chip, pl.ds(pair * 2, 2), core] if e is None else kv.at[chip, e, core]
        up = pltpu.make_async_remote_copy(src, dst, first_ssem.at[0, idx], first_rsem.at[0, pair, core], device_id=device(neighbour(0), owner))
        down = pltpu.make_async_remote_copy(src, dst, first_ssem.at[1, idx], first_rsem.at[1, pair, core], device_id=device(neighbour(1), owner))
        across = pltpu.make_async_remote_copy(src, dst, d2d_ssem.at[pair], d2d_rsem.at[pair], device_id={'sp': partner})
        return ((up, chip < chips - 1), (down, chip < far), (across, owner != core))

    def keep_kv(idx, e, k_raw, v_raw):
        t = k_raw * lax.rsqrt(jnp.mean(k_raw * k_raw, axis=-1, keepdims=True) + EPS) * gain_buf[1].astype(F32)
        k_val = (t * cos_k[...] + pltpu.roll(t, half_head, 1) * sin_k[...]).astype(BF16)
        v_val = v_raw.T.astype(BF16)
        stage[idx, e, 0] = k_val
        stage[idx, e, 1] = v_val

        @pl.when(idx % 2 == core)
        def _():
            kv[chip, (idx // 2) * 2 + e, core, 0] = k_val
            kv[chip, (idx // 2) * 2 + e, core, 1] = v_val

    for e in range(2):
        lead_wait(e)
        raw = dot(h_buf[core], w_buf[0, :, 2 * e * head:2 * (e + 1) * head])
        if e == 0:
            for copy in kv_copies(2):
                copy.start()
        keep_kv(0, e, raw[:, :head], raw[:, head:])
        for copy, cond in first_copies(0, e):
            pl.when(cond)(copy.start)
    for copy in kv_copies(3):
        copy.start()
    h_copy.start()

    def project_kv(idx, carry):
        slot = idx % 3
        for copy in kv_copies(idx):
            copy.wait()
        raw = dot(h_buf[core], w_buf[slot])
        for copy in q_copies(idx - 1):
            copy.start()
        for e in range(2):
            keep_kv(idx, e, raw[:, e * head:(e + 1) * head], raw[:, width // 2 + e * head:width // 2 + (e + 1) * head])
        for copy, cond in first_copies(idx):
            pl.when(cond)(copy.start)
        return carry

    lax.fori_loop(1, 4, project_kv, 0)
    gain_t[...] = jnp.broadcast_to(gain_buf[0].astype(F32), (chip_rows, head)).T
    h_copy.wait_recv()

    def item_of(dirn, d):
        return (chip + chips + (2 * dirn - 1) * d) % chips

    def arrives(dirn, d):
        return chip >= d if dirn == 0 else item_of(1, d) < far

    def goes_on(dirn, d):
        return arrives(dirn, d) & (chip < chips - 1) if dirn == 0 else arrives(dirn, d)

    def ring_copy(dirn, j, d, item, part):
        half = (dirn, 1 - dirn, None)[part]
        sem = (d - 2) * local_heads + j + (2 * local_heads if part == REST else 0)
        ref = kv.at[item, j] if half is None else kv.at[item, j, half]
        return pltpu.make_async_remote_copy(ref, ref, ring_ssem.at[dirn, sem], ring_rsem.at[dirn, sem], device_id=device(neighbour(dirn), core))

    def outgoing(dirn, j, d, part):
        return ring_copy(dirn, j, d, item_of(dirn, d - 1), part)

    def landed(dirn, j, d, part):
        return ring_copy(dirn, j, d, item_of(dirn, d), part)

    def forward_first(j):
        for dirn in range(2):
            pl.when(goes_on(dirn, 1))(outgoing(dirn, j, 2, WHOLE).start)

    def poll_first(pair):
        for dirn in range(2):
            @pl.when(arrives(dirn, 1))
            def _():
                for k in range(CORES):
                    pltpu.make_async_remote_copy(stage.at[0], kv.at[item_of(dirn, 1), pl.ds(pair * 2, 2), k], first_ssem.at[0, 0],
                                                 first_rsem.at[dirn, pair, k], device_id={'sp': partner}).wait_recv()

    def poll_near(s):
        j = lookup(HEAD_TABLE, s)
        d = lookup(HOP_TABLE, s) + 1
        for dirn in range(2):
            @pl.when(arrives(dirn, 2) & (d == 2))
            def _():
                landed(dirn, j, 2, WHOLE).wait_recv()

            @pl.when(goes_on(dirn, 2) & (d == 2))
            def _():
                outgoing(dirn, j, 3, NEAR).start()
                outgoing(dirn, j, 3, REST).start()

            @pl.when(arrives(dirn, 3) & (d == 3))
            def _():
                landed(dirn, j, 3, NEAR).wait_recv()

            @pl.when(goes_on(dirn, 3) & (d == 3))
            def _():
                outgoing(dirn, j, 4, NEAR).start()

    def poll_rest(s):
        j = lookup(HEAD_TABLE, s)
        d = lookup(HOP_TABLE, s) + 1
        for dirn in range(2):
            @pl.when(arrives(dirn, 3) & (d == 3))
            def _():
                landed(dirn, j, 3, REST).wait_recv()

            @pl.when(arrives(dirn, 4) & (d == 4))
            def _():
                landed(dirn, j, 4, NEAR).wait_recv()

    def drain(j, carry):
        for dirn in range(2):
            pl.when(goes_on(dirn, 1))(outgoing(dirn, j, 2, WHOLE).wait_send)
            pl.when(goes_on(dirn, 2))(outgoing(dirn, j, 3, NEAR).wait_send)
            pl.when(goes_on(dirn, 2))(outgoing(dirn, j, 3, REST).wait_send)
            pl.when(goes_on(dirn, 3))(outgoing(dirn, j, 4, NEAR).wait_send)
        return carry

    def project_q(idx, carry):
        slot = (idx + 4) % 3
        for copy in q_copies(idx):
            copy.wait()
        raw = dot(h_buf[...].reshape(chip_rows, dim), w_buf[slot])

        @pl.when(idx == 0)
        def _():
            for copy in q_copies(3):
                copy.start()

        @pl.when(idx == local_heads - 1)
        def _():
            poll_first(0)
            forward_first(0)
            forward_first(1)

        for g in range(group):
            t = raw[:, g * head:(g + 1) * head].T
            t = t * lax.rsqrt(jnp.mean(t * t, axis=0, keepdims=True) + EPS) * gain_t[...]
            t1 = t[:half_head]
            t2 = t[half_head:]
            c = angle_t[0]
            s = angle_t[1]
            q_t[idx, :, g * chip_rows:(g + 1) * chip_rows] = jnp.concatenate([t1 * c - t2 * s, t2 * c + t1 * s], axis=0).astype(BF16)
        return carry

    lax.fori_loop(0, local_heads, project_q, 0)
    for k in range(len(stages)):
        for copy in wo_copies(k):
            copy.start()

    score_scale = (head ** -0.5) * LOG2E

    def attend(items, j, first=False, ahead=2):
        keys = [kv[item, j, :, 0].reshape(chip_rows, head) for item in items]
        vals = jnp.concatenate([kv[item, j, c, 1] for item in items for c in range(CORES)], axis=1)

        def scores_of(g):
            return [dot(k, q_t[j, :, g * chip_rows:(g + 1) * chip_rows]) for k in keys]

        pending = [scores_of(g) for g in range(ahead)]
        for g in range(group):
            cols = slice(g * chip_rows, (g + 1) * chip_rows)
            scores = pending[g]
            if first:
                key_pos = lax.broadcasted_iota(jnp.int32, scores[0].shape, 0)
                q_pos = lax.broadcasted_iota(jnp.int32, scores[0].shape, 1)
                scores = [jnp.where(key_pos <= q_pos, scores[0], -jnp.inf)]
            top = functools.reduce(jnp.maximum, [jnp.max(x.reshape(chip_rows // 8, 8, chip_rows), axis=0) for x in scores])
            top = jnp.max(top, axis=0, keepdims=True)
            if first:
                m_new = jnp.broadcast_to(top, (8, chip_rows))
            else:
                m_old = m_buf[j, :, cols]
                m_new = jnp.maximum(m_old, top)
            probs = [jnp.exp2((x.reshape(chip_rows // 8, 8, chip_rows) - m_new[None]) * score_scale) for x in scores]
            total = functools.reduce(jnp.add, [jnp.sum(p, axis=0) for p in probs])
            if g + ahead < group:
                pending.append(scores_of(g + ahead))
            mixed = dot(vals, jnp.concatenate([p.reshape(chip_rows, chip_rows).astype(BF16) for p in probs], axis=0))
            m_buf[j, :, cols] = m_new
            if first:
                l_buf[j, :, cols] = total
                o_t[j, :, cols] = mixed
            else:
                alpha = jnp.exp2((m_old - m_new) * score_scale)
                l_buf[j, :, cols] = l_buf[j, :, cols] * alpha + total
                old = o_t[j, :, cols].reshape(head // 8, 8, chip_rows)
                o_t[j, :, cols] = (old * alpha[None]).reshape(head, chip_rows) + mixed

    def diagonal(j, carry):
        @pl.when(j % 2 == 0)
        def _():
            pltpu.make_async_remote_copy(stage.at[0], kv.at[chip, pl.ds(j, 2), 1 - core], d2d_ssem.at[j // 2], d2d_rsem.at[j // 2],
                                         device_id={'sp': partner}).wait_recv()

        attend((chip,), j, first=True, ahead=group)
        return carry

    lax.fori_loop(0, local_heads, diagonal, 0)
    poll_first(1)

    def o_copy(k):
        at, size = span_of(k, core)
        target = pl.ds(pl.multiple_of(at, head), size)
        return pltpu.make_async_remote_copy(o_send.at[:, pl.ds(stages[k][0] * width, size)], o_all.at[:, target], o_ssem.at[k], o_rsem.at[k],
                                            device_id={'sp': partner})

    def close_head(j):
        k = min(j // EARLY, 1) + max(0, j - EARLY)
        at = span_of(k, core)[0] + (j - stages[k][0]) * width
        inv = 1.0 / jnp.sum(l_buf[j], axis=0, keepdims=True)
        for g in range(group):
            cols = slice(g * chip_rows, (g + 1) * chip_rows)
            o_val = (o_t[j, :, cols] * inv[:, cols]).T.astype(BF16)
            o_all[:, pl.ds(pl.multiple_of(at + g * head, head), head)] = jnp.where(core == 0, o_val[:rows], o_val[rows:])
            o_send[:, j * width + g * head:j * width + (g + 1) * head] = jnp.where(core == 0, o_val[rows:], o_val[:rows])

    def project_out(k, start, end, half=None):
        if half in (None, 0):
            wo_wait(k)
            o_copy(k).wait_recv()
        at, size = span_of(k, 0)
        depth = slice(at, at + CORES * size)

        def block(n, carry):
            for w in range(wide // width):
                cols = pl.ds(n * wide + w * width, width) if isinstance(n, int) else pl.ds(pl.multiple_of(n * wide + w * width, width), width)
                total = x_buf[:, cols].astype(F32) if start else acc[:, cols]
                total = total + dot(o_all[:, depth], wo_buf[depth, cols])
                if end:
                    out_ref[:, cols] = total.astype(BF16)
                else:
                    acc[:, cols] = total
            return carry

        wide = dim // 2
        if half is None:
            lax.fori_loop(0, dim // wide, block, 0)
        else:
            block(half, 0)

    def ring_step(s, carry):
        @pl.when(s >= local_heads)
        def _():
            poll_rest(s)

        j = lookup(HEAD_TABLE, s)
        d = lookup(HOP_TABLE, s) + 1
        both = (d < far) & (chip + d >= chips)

        @pl.when(both)
        def _():
            attend((item_of(0, d), item_of(1, d)), j)

        @pl.when((chip >= d) & jnp.logical_not(both))
        def _():
            attend((item_of(0, d),), j, ahead=group)

        @pl.when((s + 1 >= local_heads) & (s + 1 < SLOTS))
        def _():
            poll_near(s + 1)

        for at, late in DEFERRED:
            @pl.when(s + 1 == at)
            def _():
                forward_first(late)

        @pl.when(s == EARLY_CLOSE)
        def _():
            for early in range(EARLY):
                close_head(early)
            o_copy(0).start()

        for half in range(2):
            @pl.when(s == EARLY_OUT + half)
            def _():
                project_out(0, True, False, half)

        @pl.when(s == THIRD_CLOSE)
        def _():
            close_head(EARLY)
            o_copy(1).start()

        return carry

    lax.fori_loop(0, SLOTS, ring_step, 0)
    close_head(local_heads - 1)
    o_copy(2).start()
    project_out(1, False, False)
    project_out(2, False, True)

    h_copy.wait_send()
    for k in range(len(stages)):
        o_copy(k).wait_send()

    def drain_first(idx, carry):
        for copy, cond in first_copies(idx):
            pl.when(cond)(copy.wait_send)
        return carry

    lax.fori_loop(0, 4, drain_first, 0)
    lax.fori_loop(0, local_heads, drain, 0)


def solution(mesh):
    group_size = mesh.shape['sp']

    def device_step(hidden, ln_gain, w_q, w_k, w_v, w_o, q_gain, k_gain):
        rows, dim = hidden.shape
        head = q_gain.shape[0]
        half = head // 2
        chips = group_size // CORES
        local_heads = w_k.shape[1] // head // CORES
        width = w_q.shape[1] // CORES // local_heads
        chip_rows = rows * CORES
        inv_freq = THETA ** -(np.arange(half, dtype=np.float64) * (2.0 / head))
        angles = inv_freq[:, None] * np.arange(rows * group_size)[None, :]
        angle_all = jnp.asarray(np.stack([np.cos(angles), np.sin(angles)]).astype(np.float32))
        hbm = pl.BlockSpec(memory_space=pl.ANY)
        dma = pltpu.SemaphoreType.DMA
        wide = width // head * chip_rows
        return pl.pallas_call(
            functools.partial(kernel, group_size),
            out_shape=pltpu.VMEM((rows, dim), BF16),
            in_specs=[hbm] * 9,
            out_specs=pl.BlockSpec(memory_space=pltpu.VMEM),
            scratch_shapes=[
                pltpu.VMEM((rows, dim), BF16),
                pltpu.VMEM((CORES, rows, dim), BF16),
                pltpu.VMEM((3, dim, width), BF16),
                pltpu.VMEM(w_o.shape, BF16),
                pltpu.VMEM((chips, local_heads, CORES, 2, rows, head), BF16),
                pltpu.VMEM((4, 2, 2, rows, head), BF16),
                pltpu.VMEM((local_heads, head, wide), BF16),
                pltpu.VMEM((local_heads, head, wide), F32),
                pltpu.VMEM((local_heads, 8, wide), F32),
                pltpu.VMEM((local_heads, 8, wide), F32),
                pltpu.VMEM((rows, w_o.shape[0]), BF16),
                pltpu.VMEM((rows, local_heads * width), BF16),
                pltpu.VMEM((rows, dim), F32),
                pltpu.VMEM((dim // LANES, LANES), BF16),
                pltpu.VMEM((2, 1, head), BF16),
                pltpu.VMEM((2, half, chip_rows), F32),
                pltpu.VMEM((head, chip_rows), F32),
                pltpu.VMEM((rows, head), F32),
                pltpu.VMEM((rows, head), F32),
                dma((2,)), dma((4,)), dma((3, 2)), dma((3,)), dma, dma,
                dma((2,)), dma((2,)),
                dma((2, 4)), dma((2, 2, CORES)),
                dma((2, 4 * local_heads)), dma((2, 4 * local_heads)),
                dma((3,)), dma((3,)),
            ],
            compiler_params=pltpu.CompilerParams(collective_id=0, has_side_effects=True, vmem_limit_bytes=VMEM_LIMIT),
        )(hidden, w_q, w_k, w_v, w_o, ln_gain.reshape(-1, LANES), q_gain[None, :], k_gain[None, :], angle_all)

    row_spec = P(('dp', 'sp'), None)
    return jax.shard_map(device_step, mesh=mesh, in_specs=(row_spec, P(), P(), P(), P(), P(), P(), P()), out_specs=row_spec, check_vma=False)
```

```python
import functools
import jax
import jax.numpy as jnp
import numpy as np
from jax import lax
from jax.experimental import pallas as pl
from jax.experimental.pallas import tpu as pltpu
from jax.sharding import PartitionSpec as P

EPS = 1e-6
THETA = 1000000.0
LOG2E = 1.4426950408889634
CORES = 2
LANES = 128
VMEM_LIMIT = 62 * 2 ** 20
BF16 = jnp.bfloat16
F32 = jnp.float32


def dot(a, b):
    return jnp.dot(a, b, preferred_element_type=F32)


ORDER = ((0, 1), (1, 1), (2, 1), (3, 1), (0, 2), (1, 2), (0, 3), (1, 3), (2, 2), (0, 4), (1, 4), (3, 2), (2, 3), (3, 3), (2, 4), (3, 4))
SLOTS = len(ORDER)
EARLY = 2
FIRST_POLL = 1
EARLY_CLOSE = 10
EARLY_OUT = 11
THIRD_CLOSE = 14
DEFERRED = ((5, 2), (7, 3))
NEAR, REST, WHOLE = 0, 1, 2


def slot_table(values):
    return tuple(sum(v << (2 * s) for s, v in enumerate(values[h:h + 8])) for h in (0, 8))


HEAD_TABLE = slot_table([j for j, _ in ORDER])
HOP_TABLE = slot_table([d - 1 for _, d in ORDER])


def lookup(table, s):
    return lax.shift_right_logical(jnp.where(s < 8, table[0], table[1]), 2 * (s % 8)) % 4


def kernel(group_size, x_hbm, wq, wk, wv, wo, ln_hbm, q_gain_hbm, k_gain_hbm, angle_hbm, out_ref,
           x_buf, h_buf, w_buf, wo_buf, kv, stage, q_t, o_t, m_buf, l_buf, o_all, o_send, acc,
           ln_buf, gain_buf, angle_t, gain_t, cos_k, sin_k,
           x_sem, small_sem, w_sem, wo_sem, h_ssem, h_rsem, d2d_ssem, d2d_rsem, first_ssem, first_rsem, ring_ssem, ring_rsem, o_ssem, o_rsem):
    chips = group_size // CORES
    me = lax.axis_index('sp')
    chip = me // CORES
    core = me % CORES
    partner = chip * CORES + (1 - core)
    rows, dim = x_buf.shape
    head = gain_buf.shape[2]
    half_head = head // 2
    width = w_buf.shape[2]
    local_heads = kv.shape[1]
    group = width // head
    chip_rows = rows * CORES
    far = chips // 2
    mixed_dim = local_heads * width
    lanes = ln_buf.shape[1]

    def device(c, k):
        return {'sp': c * CORES + k}

    def neighbour(dirn):
        return (chip + chips + 1 - 2 * dirn) % chips

    x_parts = x_sem.shape[0]
    part_rows = rows // x_parts

    def x_copy(r):
        sl = pl.ds(r * part_rows, part_rows)
        return pltpu.make_async_copy(x_hbm.at[sl, :], x_buf.at[sl, :], x_sem.at[r])

    chip_cols = pl.ds(pl.multiple_of(chip * chip_rows, chip_rows), chip_rows)
    small = (pltpu.make_async_copy(ln_hbm, ln_buf, small_sem.at[0]),
             pltpu.make_async_copy(q_gain_hbm, gain_buf.at[0], small_sem.at[1]),
             pltpu.make_async_copy(k_gain_hbm, gain_buf.at[1], small_sem.at[2]),
             pltpu.make_async_copy(angle_hbm.at[:, :, chip_cols], angle_t, small_sem.at[3]))

    def kv_copies(idx):
        pair = (idx % 2) * 2 + idx // 2
        cols = pl.ds(pl.multiple_of(pair * (width // 2), width // 2), width // 2)
        slot = idx % 3
        return (pltpu.make_async_copy(wk.at[:, cols], w_buf.at[slot, :, pl.ds(0, width // 2)], w_sem.at[slot, 0]),
                pltpu.make_async_copy(wv.at[:, cols], w_buf.at[slot, :, pl.ds(width // 2, width // 2)], w_sem.at[slot, 1]))

    def lead_copies(e):
        cols = pl.ds(e * head, head)
        return tuple(pltpu.make_async_copy(w.at[:, cols], w_buf.at[0, :, pl.ds((2 * e + part) * head, head)], w_sem.at[0, e])
                     for part, w in enumerate((wk, wv)))

    def lead_wait(e):
        pltpu.make_async_copy(wk.at[:, pl.ds(0, 2 * head)], w_buf.at[0, :, pl.ds(2 * e * head, 2 * head)], w_sem.at[0, e]).wait()

    def q_copies(idx):
        cols = pl.ds(pl.multiple_of((core * local_heads + idx) * width, width), width)
        slot = (idx + 4) % 3
        return tuple(pltpu.make_async_copy(wq.at[pl.ds(r * (dim // 2), dim // 2), cols],
                                           w_buf.at[slot, pl.ds(r * (dim // 2), dim // 2), :], w_sem.at[slot, r]) for r in range(2))

    stages = ((0, EARLY), (EARLY, EARLY + 1), (EARLY + 1, local_heads))

    def span_of(k, c):
        first, last = stages[k]
        return (CORES * first + c * (last - first)) * width, (last - first) * width

    def wo_copies(k):
        copies = []
        for c in range(CORES):
            at, size = span_of(k, c)
            source = pl.ds(c * mixed_dim + stages[k][0] * width, size)
            copies.append(pltpu.make_async_copy(wo.at[source, :], wo_buf.at[pl.ds(at, size), :], wo_sem.at[k]))
        return copies

    def wo_wait(k):
        at, size = span_of(k, 0)
        span = pl.ds(at, CORES * size)
        pltpu.make_async_copy(wo.at[span, :], wo_buf.at[span, :], wo_sem.at[k]).wait()

    for copy in small[:1]:
        copy.start()
    for r in range(x_parts):
        x_copy(r).start()
    for copy in small[1:]:
        copy.start()
    for copy in lead_copies(0):
        copy.start()

    barrier = pltpu.get_barrier_semaphore()
    pl.semaphore_signal(barrier, inc=1, device_id={'sp': partner})
    for dirn in range(2):
        for k in range(CORES):
            pl.semaphore_signal(barrier, inc=1, device_id=device(neighbour(dirn), k))

    small[0].wait()
    for r in range(x_parts):
        x_copy(r).wait()
        if r == 0:
            for copy in lead_copies(1):
                copy.start()
        if r == x_parts - 1:
            for copy in kv_copies(1):
                copy.start()
        step_rows = 16
        for t in range(part_rows // step_rows):
            sl = slice(r * part_rows + t * step_rows, r * part_rows + (t + 1) * step_rows)
            xf = x_buf[sl, :].astype(F32)
            scale = lax.rsqrt(jnp.mean(xf * xf, axis=-1, keepdims=True) + EPS)
            for b in range(dim // lanes):
                cols = slice(b * lanes, (b + 1) * lanes)
                h_buf[core, sl, cols] = (xf[:, cols] * scale * ln_buf[b:b + 1, :].astype(F32)).astype(BF16)

    for copy in small[1:]:
        copy.wait()
    own_cols = pl.ds(pl.multiple_of(core * rows, rows), rows)
    cos_own = angle_t[0, :, own_cols].T
    sin_own = angle_t[1, :, own_cols].T
    cos_k[...] = jnp.concatenate([cos_own, cos_own], axis=1)
    sin_k[...] = jnp.concatenate([-sin_own, sin_own], axis=1)

    pl.semaphore_wait(barrier, 1 + 2 * CORES)
    h_copy = pltpu.make_async_remote_copy(h_buf.at[core], h_buf.at[core], h_ssem, h_rsem, device_id={'sp': partner})

    def first_copies(idx, e=None):
        owner = idx % 2
        pair = idx // 2
        src = stage.at[idx] if e is None else stage.at[idx, e]
        dst = kv.at[chip, pl.ds(pair * 2, 2), core] if e is None else kv.at[chip, e, core]
        up = pltpu.make_async_remote_copy(src, dst, first_ssem.at[0, idx], first_rsem.at[0, pair], device_id=device(neighbour(0), owner))
        down = pltpu.make_async_remote_copy(src, dst, first_ssem.at[1, idx], first_rsem.at[1, pair], device_id=device(neighbour(1), owner))
        across = pltpu.make_async_remote_copy(src, dst, d2d_ssem.at[pair], d2d_rsem.at[pair], device_id={'sp': partner})
        return ((up, chip < chips - 1), (down, chip < far), (across, owner != core))

    def keep_kv(idx, e, k_raw, v_raw):
        t = k_raw * lax.rsqrt(jnp.mean(k_raw * k_raw, axis=-1, keepdims=True) + EPS) * gain_buf[1].astype(F32)
        k_val = (t * cos_k[...] + pltpu.roll(t, half_head, 1) * sin_k[...]).astype(BF16)
        v_val = v_raw.T.astype(BF16)
        stage[idx, e, 0] = k_val
        stage[idx, e, 1] = v_val

        @pl.when(idx % 2 == core)
        def _():
            kv[chip, (idx // 2) * 2 + e, core, 0] = k_val
            kv[chip, (idx // 2) * 2 + e, core, 1] = v_val

    for e in range(2):
        lead_wait(e)
        raw = dot(h_buf[core], w_buf[0, :, 2 * e * head:2 * (e + 1) * head])
        if e == 0:
            for copy in kv_copies(2):
                copy.start()
        keep_kv(0, e, raw[:, :head], raw[:, head:])
        for copy, cond in first_copies(0, e):
            pl.when(cond)(copy.start)
    for copy in kv_copies(3):
        copy.start()
    h_copy.start()

    def project_kv(idx, carry):
        slot = idx % 3
        for copy in kv_copies(idx):
            copy.wait()
        raw = dot(h_buf[core], w_buf[slot])
        for copy in q_copies(idx - 1):
            copy.start()
        for e in range(2):
            keep_kv(idx, e, raw[:, e * head:(e + 1) * head], raw[:, width // 2 + e * head:width // 2 + (e + 1) * head])
        for copy, cond in first_copies(idx):
            pl.when(cond)(copy.start)
        return carry

    lax.fori_loop(1, 4, project_kv, 0)
    gain_t[...] = jnp.broadcast_to(gain_buf[0].astype(F32), (chip_rows, head)).T
    h_copy.wait_recv()

    def item_of(dirn, d):
        return (chip + chips + (2 * dirn - 1) * d) % chips

    def arrives(dirn, d):
        return chip >= d if dirn == 0 else item_of(1, d) < far

    def goes_on(dirn, d):
        return arrives(dirn, d) & (chip < chips - 1) if dirn == 0 else arrives(dirn, d)

    def ring_copy(dirn, j, d, item, part):
        half = (dirn, 1 - dirn, None)[part]
        sem = (d - 2) * local_heads + j + (2 * local_heads if part == REST else 0)
        ref = kv.at[item, j] if half is None else kv.at[item, j, half]
        return pltpu.make_async_remote_copy(ref, ref, ring_ssem.at[dirn, j + (local_heads if part == REST else 0)], ring_rsem.at[dirn, sem], device_id=device(neighbour(dirn), core))

    def outgoing(dirn, j, d, part):
        return ring_copy(dirn, j, d, item_of(dirn, d - 1), part)

    def landed(dirn, j, d, part):
        return ring_copy(dirn, j, d, item_of(dirn, d), part)

    def forward_first(j):
        for dirn in range(2):
            pl.when(goes_on(dirn, 1))(outgoing(dirn, j, 2, WHOLE).start)

    def poll_first(pair):
        for dirn in range(2):
            @pl.when(arrives(dirn, 1))
            def _():
                both = kv.at[item_of(dirn, 1), pl.ds(pair * 2, 2)]
                pltpu.make_async_remote_copy(both, both, first_ssem.at[0, 0], first_rsem.at[dirn, pair], device_id={'sp': partner}).wait_recv()

    def poll_near(s):
        j = lookup(HEAD_TABLE, s)
        d = lookup(HOP_TABLE, s) + 1
        for dirn in range(2):
            @pl.when(arrives(dirn, 2) & (d == 2))
            def _():
                landed(dirn, j, 2, WHOLE).wait_recv()

            @pl.when(goes_on(dirn, 2) & (d == 2))
            def _():
                pl.when(goes_on(dirn, 1))(outgoing(dirn, j, 2, WHOLE).wait_send)
                outgoing(dirn, j, 3, NEAR).start()
                outgoing(dirn, j, 3, REST).start()

            @pl.when(arrives(dirn, 3) & (d == 3))
            def _():
                landed(dirn, j, 3, NEAR).wait_recv()

            @pl.when(goes_on(dirn, 3) & (d == 3))
            def _():
                pl.when(goes_on(dirn, 2))(outgoing(dirn, j, 3, NEAR).wait_send)
                outgoing(dirn, j, 4, NEAR).start()

    def poll_rest(s):
        j = lookup(HEAD_TABLE, s)
        d = lookup(HOP_TABLE, s) + 1
        for dirn in range(2):
            @pl.when(arrives(dirn, 3) & (d == 3))
            def _():
                landed(dirn, j, 3, REST).wait_recv()

            @pl.when(arrives(dirn, 4) & (d == 4))
            def _():
                landed(dirn, j, 4, NEAR).wait_recv()

    def drain(j, carry):
        for dirn in range(2):
            on = [goes_on(dirn, d) for d in range(4)]
            pl.when(on[1] & jnp.logical_not(on[2]))(outgoing(dirn, j, 2, WHOLE).wait_send)
            pl.when(on[2] & jnp.logical_not(on[3]))(outgoing(dirn, j, 3, NEAR).wait_send)
            pl.when(on[2])(outgoing(dirn, j, 3, REST).wait_send)
            pl.when(on[3])(outgoing(dirn, j, 4, NEAR).wait_send)
        return carry

    def project_q(idx, carry):
        slot = (idx + 4) % 3
        for copy in q_copies(idx):
            copy.wait()
        raw = dot(h_buf[...].reshape(chip_rows, dim), w_buf[slot])

        @pl.when(idx == 0)
        def _():
            for copy in q_copies(3):
                copy.start()

        @pl.when(idx == local_heads - 1)
        def _():
            poll_first(0)
            forward_first(0)
            forward_first(1)

        for g in range(group):
            t = raw[:, g * head:(g + 1) * head].T
            t = t * lax.rsqrt(jnp.mean(t * t, axis=0, keepdims=True) + EPS) * gain_t[...]
            t1 = t[:half_head]
            t2 = t[half_head:]
            c = angle_t[0]
            s = angle_t[1]
            q_t[idx, :, g * chip_rows:(g + 1) * chip_rows] = jnp.concatenate([t1 * c - t2 * s, t2 * c + t1 * s], axis=0).astype(BF16)
        return carry

    lax.fori_loop(0, local_heads, project_q, 0)
    for k in range(len(stages)):
        for copy in wo_copies(k):
            copy.start()

    score_scale = (head ** -0.5) * LOG2E

    def attend(items, j, first=False, ahead=2):
        keys = [kv[item, j, :, 0].reshape(chip_rows, head) for item in items]
        vals = jnp.concatenate([kv[item, j, c, 1] for item in items for c in range(CORES)], axis=1)

        def scores_of(g):
            return [dot(k, q_t[j, :, g * chip_rows:(g + 1) * chip_rows]) for k in keys]

        pending = [scores_of(g) for g in range(ahead)]
        for g in range(group):
            cols = slice(g * chip_rows, (g + 1) * chip_rows)
            scores = pending[g]
            if first:
                key_pos = lax.broadcasted_iota(jnp.int32, scores[0].shape, 0)
                q_pos = lax.broadcasted_iota(jnp.int32, scores[0].shape, 1)
                scores = [jnp.where(key_pos <= q_pos, scores[0], -jnp.inf)]
            top = functools.reduce(jnp.maximum, [jnp.max(x.reshape(chip_rows // 8, 8, chip_rows), axis=0) for x in scores])
            top = jnp.max(top, axis=0, keepdims=True)
            if first:
                m_new = jnp.broadcast_to(top, (8, chip_rows))
            else:
                m_old = m_buf[j, :, cols]
                m_new = jnp.maximum(m_old, top)
            probs = [jnp.exp2((x.reshape(chip_rows // 8, 8, chip_rows) - m_new[None]) * score_scale) for x in scores]
            total = functools.reduce(jnp.add, [jnp.sum(p, axis=0) for p in probs])
            if g + ahead < group:
                pending.append(scores_of(g + ahead))
            mixed = dot(vals, jnp.concatenate([p.reshape(chip_rows, chip_rows).astype(BF16) for p in probs], axis=0))
            m_buf[j, :, cols] = m_new
            if first:
                l_buf[j, :, cols] = total
                o_t[j, :, cols] = mixed
            else:
                alpha = jnp.exp2((m_old - m_new) * score_scale)
                l_buf[j, :, cols] = l_buf[j, :, cols] * alpha + total
                old = o_t[j, :, cols].reshape(head // 8, 8, chip_rows)
                o_t[j, :, cols] = (old * alpha[None]).reshape(head, chip_rows) + mixed

    def diagonal(j, carry):
        @pl.when(j % 2 == 0)
        def _():
            pltpu.make_async_remote_copy(stage.at[0], kv.at[chip, pl.ds(j, 2), 1 - core], d2d_ssem.at[j // 2], d2d_rsem.at[j // 2],
                                         device_id={'sp': partner}).wait_recv()

        attend((chip,), j, first=True, ahead=group)
        return carry

    lax.fori_loop(0, local_heads, diagonal, 0)
    poll_first(1)

    def o_copy(k):
        at, size = span_of(k, core)
        target = pl.ds(pl.multiple_of(at, head), size)
        return pltpu.make_async_remote_copy(o_send.at[:, pl.ds(stages[k][0] * width, size)], o_all.at[:, target], o_ssem.at[k], o_rsem.at[k],
                                            device_id={'sp': partner})

    def close_head(j):
        k = min(j // EARLY, 1) + max(0, j - EARLY)
        at = span_of(k, core)[0] + (j - stages[k][0]) * width
        inv = 1.0 / jnp.sum(l_buf[j], axis=0, keepdims=True)
        for g in range(group):
            cols = slice(g * chip_rows, (g + 1) * chip_rows)
            o_val = (o_t[j, :, cols] * inv[:, cols]).T.astype(BF16)
            o_all[:, pl.ds(pl.multiple_of(at + g * head, head), head)] = jnp.where(core == 0, o_val[:rows], o_val[rows:])
            o_send[:, j * width + g * head:j * width + (g + 1) * head] = jnp.where(core == 0, o_val[rows:], o_val[:rows])

    def project_out(k, start, end, half=None):
        if half in (None, 0):
            wo_wait(k)
            o_copy(k).wait_recv()
        at, size = span_of(k, 0)
        depth = slice(at, at + CORES * size)

        def block(n):
            for w in range(wide // width):
                cols = pl.ds(n * wide + w * width, width)
                total = x_buf[:, cols].astype(F32) if start else acc[:, cols]
                total = total + dot(o_all[:, depth], wo_buf[depth, cols])
                if end:
                    out_ref[:, cols] = total.astype(BF16)
                else:
                    acc[:, cols] = total

        wide = dim // 2
        for n in range(dim // wide) if half is None else (half,):
            block(n)

    def ring_step(s, carry):
        @pl.when(s >= local_heads)
        def _():
            poll_rest(s)

        j = lookup(HEAD_TABLE, s)
        d = lookup(HOP_TABLE, s) + 1
        both = (d < far) & (chip + d >= chips)

        @pl.when(both)
        def _():
            attend((item_of(0, d), item_of(1, d)), j)

        @pl.when((chip >= d) & jnp.logical_not(both))
        def _():
            attend((item_of(0, d),), j, ahead=group)

        @pl.when(s == EARLY_CLOSE)
        def _():
            for early in range(EARLY):
                close_head(early)
            o_copy(0).start()

        @pl.when((s == FIRST_POLL) | ((s + 1 > local_heads) & (s + 1 < SLOTS)))
        def _():
            poll_near(jnp.where(s == FIRST_POLL, local_heads, s + 1))

        for at, late in DEFERRED:
            @pl.when(s + 1 == at)
            def _():
                forward_first(late)

        for half in range(2):
            @pl.when(s == EARLY_OUT + half)
            def _():
                project_out(0, True, False, half)

        @pl.when(s == THIRD_CLOSE)
        def _():
            close_head(EARLY)
            o_copy(1).start()

        return carry

    lax.fori_loop(0, SLOTS, ring_step, 0)
    close_head(local_heads - 1)
    o_copy(2).start()
    project_out(1, False, False)
    project_out(2, False, True)

    h_copy.wait_send()
    for k in range(len(stages)):
        o_copy(k).wait_send()

    def drain_first(idx, carry):
        for copy, cond in first_copies(idx):
            pl.when(cond)(copy.wait_send)
        return carry

    lax.fori_loop(0, 4, drain_first, 0)
    lax.fori_loop(0, local_heads, drain, 0)


def solution(mesh):
    group_size = mesh.shape['sp']

    def device_step(hidden, ln_gain, w_q, w_k, w_v, w_o, q_gain, k_gain):
        rows, dim = hidden.shape
        head = q_gain.shape[0]
        half = head // 2
        chips = group_size // CORES
        local_heads = w_k.shape[1] // head // CORES
        width = w_q.shape[1] // CORES // local_heads
        chip_rows = rows * CORES
        inv_freq = THETA ** -(np.arange(half, dtype=np.float64) * (2.0 / head))
        angles = inv_freq[:, None] * np.arange(rows * group_size)[None, :]
        angle_all = jnp.asarray(np.stack([np.cos(angles), np.sin(angles)]).astype(np.float32))
        hbm = pl.BlockSpec(memory_space=pl.ANY)
        dma = pltpu.SemaphoreType.DMA
        wide = width // head * chip_rows
        return pl.pallas_call(
            functools.partial(kernel, group_size),
            out_shape=pltpu.VMEM((rows, dim), BF16),
            in_specs=[hbm] * 9,
            out_specs=pl.BlockSpec(memory_space=pltpu.VMEM),
            scratch_shapes=[
                pltpu.VMEM((rows, dim), BF16),
                pltpu.VMEM((CORES, rows, dim), BF16),
                pltpu.VMEM((3, dim, width), BF16),
                pltpu.VMEM(w_o.shape, BF16),
                pltpu.VMEM((chips, local_heads, CORES, 2, rows, head), BF16),
                pltpu.VMEM((4, 2, 2, rows, head), BF16),
                pltpu.VMEM((local_heads, head, wide), BF16),
                pltpu.VMEM((local_heads, head, wide), F32),
                pltpu.VMEM((local_heads, 8, wide), F32),
                pltpu.VMEM((local_heads, 8, wide), F32),
                pltpu.VMEM((rows, w_o.shape[0]), BF16),
                pltpu.VMEM((rows, local_heads * width), BF16),
                pltpu.VMEM((rows, dim), F32),
                pltpu.VMEM((dim // LANES, LANES), BF16),
                pltpu.VMEM((2, 1, head), BF16),
                pltpu.VMEM((2, half, chip_rows), F32),
                pltpu.VMEM((head, chip_rows), F32),
                pltpu.VMEM((rows, head), F32),
                pltpu.VMEM((rows, head), F32),
                dma((2,)), dma((4,)), dma((3, 2)), dma((3,)), dma, dma,
                dma((2,)), dma((2,)),
                dma((2, 4)), dma((2, 2)),
                dma((2, 2 * local_heads)), dma((2, 4 * local_heads)),
                dma((3,)), dma((3,)),
            ],
            compiler_params=pltpu.CompilerParams(collective_id=0, has_side_effects=True, vmem_limit_bytes=VMEM_LIMIT),
        )(hidden, w_q, w_k, w_v, w_o, ln_gain.reshape(-1, LANES), q_gain[None, :], k_gain[None, :], angle_all)

    row_spec = P(('dp', 'sp'), None)
    return jax.shard_map(device_step, mesh=mesh, in_specs=(row_spec, P(), P(), P(), P(), P(), P(), P()), out_specs=row_spec, check_vma=False)
```

```python
import functools
import jax
import jax.numpy as jnp
import numpy as np
from jax import lax
from jax.experimental import pallas as pl
from jax.experimental.pallas import tpu as pltpu
from jax.sharding import PartitionSpec as P

EPS = 1e-6
THETA = 1000000.0
LOG2E = 1.4426950408889634
CORES = 2
LANES = 128
VMEM_LIMIT = 62 * 2 ** 20
BF16 = jnp.bfloat16
F32 = jnp.float32


def dot(a, b):
    return jnp.dot(a, b, preferred_element_type=F32)


ORDER = ((0, 1), (1, 1), (2, 1), (3, 1), (0, 2), (1, 2), (0, 3), (1, 3), (2, 2), (0, 4), (1, 4), (3, 2), (2, 3), (3, 3), (2, 4), (3, 4))
SLOTS = len(ORDER)
EARLY = 2
FIRST_POLL = 1
LOW_CHIPS = 2
LOW_CLOSE = 7
LOW_OUT = 9
EARLY_CLOSE = 10
EARLY_OUT = 11
THIRD_CLOSE = 14
DEFERRED = ((5, 2), (7, 3))
NEAR, REST, WHOLE = 0, 1, 2


def slot_table(values):
    return tuple(sum(v << (2 * s) for s, v in enumerate(values[h:h + 8])) for h in (0, 8))


HEAD_TABLE = slot_table([j for j, _ in ORDER])
HOP_TABLE = slot_table([d - 1 for _, d in ORDER])


def lookup(table, s):
    return lax.shift_right_logical(jnp.where(s < 8, table[0], table[1]), 2 * (s % 8)) % 4


def kernel(group_size, x_hbm, wq, wk, wv, wo, ln_hbm, q_gain_hbm, k_gain_hbm, angle_hbm, out_ref,
           x_buf, h_buf, w_buf, wo_buf, kv, stage, q_t, o_t, m_buf, l_buf, o_all, o_send, acc,
           ln_buf, gain_buf, angle_t, gain_t, cos_k, sin_k,
           x_sem, small_sem, w_sem, wo_sem, h_ssem, h_rsem, d2d_ssem, d2d_rsem, first_ssem, first_rsem, ring_ssem, ring_rsem, o_ssem, o_rsem):
    chips = group_size // CORES
    me = lax.axis_index('sp')
    chip = me // CORES
    core = me % CORES
    partner = chip * CORES + (1 - core)
    rows, dim = x_buf.shape
    head = gain_buf.shape[2]
    half_head = head // 2
    width = w_buf.shape[2]
    local_heads = kv.shape[1]
    group = width // head
    chip_rows = rows * CORES
    far = chips // 2
    mixed_dim = local_heads * width
    lanes = ln_buf.shape[1]

    def device(c, k):
        return {'sp': c * CORES + k}

    def neighbour(dirn):
        return (chip + chips + 1 - 2 * dirn) % chips

    x_parts = x_sem.shape[0]
    part_rows = rows // x_parts

    def x_copy(r):
        sl = pl.ds(r * part_rows, part_rows)
        return pltpu.make_async_copy(x_hbm.at[sl, :], x_buf.at[sl, :], x_sem.at[r])

    chip_cols = pl.ds(pl.multiple_of(chip * chip_rows, chip_rows), chip_rows)
    small = (pltpu.make_async_copy(ln_hbm, ln_buf, small_sem.at[0]),
             pltpu.make_async_copy(q_gain_hbm, gain_buf.at[0], small_sem.at[1]),
             pltpu.make_async_copy(k_gain_hbm, gain_buf.at[1], small_sem.at[2]),
             pltpu.make_async_copy(angle_hbm.at[:, :, chip_cols], angle_t, small_sem.at[3]))

    def kv_copies(idx):
        pair = (idx % 2) * 2 + idx // 2
        cols = pl.ds(pl.multiple_of(pair * (width // 2), width // 2), width // 2)
        slot = idx % 3
        return (pltpu.make_async_copy(wk.at[:, cols], w_buf.at[slot, :, pl.ds(0, width // 2)], w_sem.at[slot, 0]),
                pltpu.make_async_copy(wv.at[:, cols], w_buf.at[slot, :, pl.ds(width // 2, width // 2)], w_sem.at[slot, 1]))

    def lead_copies(e):
        cols = pl.ds(e * head, head)
        return tuple(pltpu.make_async_copy(w.at[:, cols], w_buf.at[0, :, pl.ds((2 * e + part) * head, head)], w_sem.at[0, e])
                     for part, w in enumerate((wk, wv)))

    def lead_wait(e):
        pltpu.make_async_copy(wk.at[:, pl.ds(0, 2 * head)], w_buf.at[0, :, pl.ds(2 * e * head, 2 * head)], w_sem.at[0, e]).wait()

    def q_copies(idx):
        cols = pl.ds(pl.multiple_of((core * local_heads + idx) * width, width), width)
        slot = (idx + 4) % 3
        return tuple(pltpu.make_async_copy(wq.at[pl.ds(r * (dim // 2), dim // 2), cols],
                                           w_buf.at[slot, pl.ds(r * (dim // 2), dim // 2), :], w_sem.at[slot, r]) for r in range(2))

    stages = ((0, EARLY), (EARLY, EARLY + 1), (EARLY + 1, local_heads))

    def span_of(k, c):
        first, last = stages[k]
        return (CORES * first + c * (last - first)) * width, (last - first) * width

    def wo_copies(k):
        copies = []
        for c in range(CORES):
            at, size = span_of(k, c)
            source = pl.ds(c * mixed_dim + stages[k][0] * width, size)
            copies.append(pltpu.make_async_copy(wo.at[source, :], wo_buf.at[pl.ds(at, size), :], wo_sem.at[k]))
        return copies

    def wo_wait(k):
        at, size = span_of(k, 0)
        span = pl.ds(at, CORES * size)
        pltpu.make_async_copy(wo.at[span, :], wo_buf.at[span, :], wo_sem.at[k]).wait()

    for copy in small[:1]:
        copy.start()
    for r in range(x_parts):
        x_copy(r).start()
    for copy in small[1:]:
        copy.start()
    for copy in lead_copies(0):
        copy.start()

    barrier = pltpu.get_barrier_semaphore()
    pl.semaphore_signal(barrier, inc=1, device_id={'sp': partner})
    for dirn in range(2):
        for k in range(CORES):
            pl.semaphore_signal(barrier, inc=1, device_id=device(neighbour(dirn), k))

    small[0].wait()
    for r in range(x_parts):
        x_copy(r).wait()
        if r == 0:
            for copy in lead_copies(1):
                copy.start()
        if r == x_parts - 1:
            for copy in kv_copies(1):
                copy.start()
        step_rows = 16
        for t in range(part_rows // step_rows):
            sl = slice(r * part_rows + t * step_rows, r * part_rows + (t + 1) * step_rows)
            xf = x_buf[sl, :].astype(F32)
            scale = lax.rsqrt(jnp.mean(xf * xf, axis=-1, keepdims=True) + EPS)
            for b in range(dim // lanes):
                cols = slice(b * lanes, (b + 1) * lanes)
                h_buf[core, sl, cols] = (xf[:, cols] * scale * ln_buf[b:b + 1, :].astype(F32)).astype(BF16)

    for copy in small[1:]:
        copy.wait()
    own_cols = pl.ds(pl.multiple_of(core * rows, rows), rows)
    cos_own = angle_t[0, :, own_cols].T
    sin_own = angle_t[1, :, own_cols].T
    cos_k[...] = jnp.concatenate([cos_own, cos_own], axis=1)
    sin_k[...] = jnp.concatenate([-sin_own, sin_own], axis=1)

    pl.semaphore_wait(barrier, 1 + 2 * CORES)
    h_copy = pltpu.make_async_remote_copy(h_buf.at[core], h_buf.at[core], h_ssem, h_rsem, device_id={'sp': partner})

    def first_copies(idx, e=None):
        owner = idx % 2
        pair = idx // 2
        src = stage.at[idx] if e is None else stage.at[idx, e]
        dst = kv.at[chip, pl.ds(pair * 2, 2), core] if e is None else kv.at[chip, e, core]
        up = pltpu.make_async_remote_copy(src, dst, first_ssem.at[0, idx], first_rsem.at[0, pair], device_id=device(neighbour(0), owner))
        down = pltpu.make_async_remote_copy(src, dst, first_ssem.at[1, idx], first_rsem.at[1, pair], device_id=device(neighbour(1), owner))
        across = pltpu.make_async_remote_copy(src, dst, d2d_ssem.at[pair], d2d_rsem.at[pair], device_id={'sp': partner})
        return ((up, chip < chips - 1), (down, chip < far), (across, owner != core))

    def keep_kv(idx, e, k_raw, v_raw):
        t = k_raw * lax.rsqrt(jnp.mean(k_raw * k_raw, axis=-1, keepdims=True) + EPS) * gain_buf[1].astype(F32)
        k_val = (t * cos_k[...] + pltpu.roll(t, half_head, 1) * sin_k[...]).astype(BF16)
        v_val = v_raw.T.astype(BF16)
        stage[idx, e, 0] = k_val
        stage[idx, e, 1] = v_val

        @pl.when(idx % 2 == core)
        def _():
            kv[chip, (idx // 2) * 2 + e, core, 0] = k_val
            kv[chip, (idx // 2) * 2 + e, core, 1] = v_val

    for e in range(2):
        lead_wait(e)
        raw = dot(h_buf[core], w_buf[0, :, 2 * e * head:2 * (e + 1) * head])
        if e == 0:
            for copy in kv_copies(2):
                copy.start()
        keep_kv(0, e, raw[:, :head], raw[:, head:])
        for copy, cond in first_copies(0, e):
            pl.when(cond)(copy.start)
    for copy in kv_copies(3):
        copy.start()
    h_copy.start()

    def project_kv(idx, carry):
        slot = idx % 3
        for copy in kv_copies(idx):
            copy.wait()
        raw = dot(h_buf[core], w_buf[slot])
        for copy in q_copies(idx - 1):
            copy.start()
        for e in range(2):
            keep_kv(idx, e, raw[:, e * head:(e + 1) * head], raw[:, width // 2 + e * head:width // 2 + (e + 1) * head])
        for copy, cond in first_copies(idx):
            pl.when(cond)(copy.start)
        return carry

    lax.fori_loop(1, 4, project_kv, 0)
    gain_t[...] = jnp.broadcast_to(gain_buf[0].astype(F32), (chip_rows, head)).T
    h_copy.wait_recv()

    def item_of(dirn, d):
        return (chip + chips + (2 * dirn - 1) * d) % chips

    def arrives(dirn, d):
        return chip >= d if dirn == 0 else item_of(1, d) < far

    def goes_on(dirn, d):
        return arrives(dirn, d) & (chip < chips - 1) if dirn == 0 else arrives(dirn, d)

    def ring_copy(dirn, j, d, item, part):
        half = (dirn, 1 - dirn, None)[part]
        sem = (d - 2) * local_heads + j + (2 * local_heads if part == REST else 0)
        ref = kv.at[item, j] if half is None else kv.at[item, j, half]
        return pltpu.make_async_remote_copy(ref, ref, ring_ssem.at[dirn, j + (local_heads if part == REST else 0)], ring_rsem.at[dirn, sem], device_id=device(neighbour(dirn), core))

    def outgoing(dirn, j, d, part):
        return ring_copy(dirn, j, d, item_of(dirn, d - 1), part)

    def landed(dirn, j, d, part):
        return ring_copy(dirn, j, d, item_of(dirn, d), part)

    def forward_first(j):
        for dirn in range(2):
            pl.when(goes_on(dirn, 1))(outgoing(dirn, j, 2, WHOLE).start)

    def poll_first(pair):
        for dirn in range(2):
            @pl.when(arrives(dirn, 1))
            def _():
                both = kv.at[item_of(dirn, 1), pl.ds(pair * 2, 2)]
                pltpu.make_async_remote_copy(both, both, first_ssem.at[0, 0], first_rsem.at[dirn, pair], device_id={'sp': partner}).wait_recv()

    def poll_near(s):
        j = lookup(HEAD_TABLE, s)
        d = lookup(HOP_TABLE, s) + 1
        for dirn in range(2):
            @pl.when(arrives(dirn, 2) & (d == 2))
            def _():
                landed(dirn, j, 2, WHOLE).wait_recv()

            @pl.when(goes_on(dirn, 2) & (d == 2))
            def _():
                pl.when(goes_on(dirn, 1))(outgoing(dirn, j, 2, WHOLE).wait_send)
                outgoing(dirn, j, 3, NEAR).start()
                outgoing(dirn, j, 3, REST).start()

            @pl.when(arrives(dirn, 3) & (d == 3))
            def _():
                landed(dirn, j, 3, NEAR).wait_recv()

            @pl.when(goes_on(dirn, 3) & (d == 3))
            def _():
                pl.when(goes_on(dirn, 2))(outgoing(dirn, j, 3, NEAR).wait_send)
                outgoing(dirn, j, 4, NEAR).start()

    def poll_rest(s):
        j = lookup(HEAD_TABLE, s)
        d = lookup(HOP_TABLE, s) + 1
        for dirn in range(2):
            @pl.when(arrives(dirn, 3) & (d == 3))
            def _():
                landed(dirn, j, 3, REST).wait_recv()

            @pl.when(arrives(dirn, 4) & (d == 4))
            def _():
                landed(dirn, j, 4, NEAR).wait_recv()

    def drain(j, carry):
        for dirn in range(2):
            on = [goes_on(dirn, d) for d in range(4)]
            pl.when(on[1] & jnp.logical_not(on[2]))(outgoing(dirn, j, 2, WHOLE).wait_send)
            pl.when(on[2] & jnp.logical_not(on[3]))(outgoing(dirn, j, 3, NEAR).wait_send)
            pl.when(on[2])(outgoing(dirn, j, 3, REST).wait_send)
            pl.when(on[3])(outgoing(dirn, j, 4, NEAR).wait_send)
        return carry

    def project_q(idx, carry):
        slot = (idx + 4) % 3
        for copy in q_copies(idx):
            copy.wait()
        raw = dot(h_buf[...].reshape(chip_rows, dim), w_buf[slot])

        @pl.when(idx == 0)
        def _():
            for copy in q_copies(3):
                copy.start()

        @pl.when(idx == local_heads - 1)
        def _():
            poll_first(0)
            forward_first(0)
            forward_first(1)

        for g in range(group):
            t = raw[:, g * head:(g + 1) * head].T
            t = t * lax.rsqrt(jnp.mean(t * t, axis=0, keepdims=True) + EPS) * gain_t[...]
            t1 = t[:half_head]
            t2 = t[half_head:]
            c = angle_t[0]
            s = angle_t[1]
            q_t[idx, :, g * chip_rows:(g + 1) * chip_rows] = jnp.concatenate([t1 * c - t2 * s, t2 * c + t1 * s], axis=0).astype(BF16)
        return carry

    lax.fori_loop(0, local_heads, project_q, 0)
    for k in range(len(stages)):
        for copy in wo_copies(k):
            copy.start()

    score_scale = (head ** -0.5) * LOG2E

    def attend(items, j, first=False, ahead=2):
        keys = [kv[item, j, :, 0].reshape(chip_rows, head) for item in items]
        vals = jnp.concatenate([kv[item, j, c, 1] for item in items for c in range(CORES)], axis=1)

        def scores_of(g):
            return [dot(k, q_t[j, :, g * chip_rows:(g + 1) * chip_rows]) for k in keys]

        pending = [scores_of(g) for g in range(ahead)]
        for g in range(group):
            cols = slice(g * chip_rows, (g + 1) * chip_rows)
            scores = pending[g]
            if first:
                key_pos = lax.broadcasted_iota(jnp.int32, scores[0].shape, 0)
                q_pos = lax.broadcasted_iota(jnp.int32, scores[0].shape, 1)
                scores = [jnp.where(key_pos <= q_pos, scores[0], -jnp.inf)]
            top = functools.reduce(jnp.maximum, [jnp.max(x.reshape(chip_rows // 8, 8, chip_rows), axis=0) for x in scores])
            top = jnp.max(top, axis=0, keepdims=True)
            if first:
                m_new = jnp.broadcast_to(top, (8, chip_rows))
            else:
                m_old = m_buf[j, :, cols]
                m_new = jnp.maximum(m_old, top)
            probs = [jnp.exp2((x.reshape(chip_rows // 8, 8, chip_rows) - m_new[None]) * score_scale) for x in scores]
            total = functools.reduce(jnp.add, [jnp.sum(p, axis=0) for p in probs])
            if g + ahead < group:
                pending.append(scores_of(g + ahead))
            mixed = dot(vals, jnp.concatenate([p.reshape(chip_rows, chip_rows).astype(BF16) for p in probs], axis=0))
            m_buf[j, :, cols] = m_new
            if first:
                l_buf[j, :, cols] = total
                o_t[j, :, cols] = mixed
            else:
                alpha = jnp.exp2((m_old - m_new) * score_scale)
                l_buf[j, :, cols] = l_buf[j, :, cols] * alpha + total
                old = o_t[j, :, cols].reshape(head // 8, 8, chip_rows)
                o_t[j, :, cols] = (old * alpha[None]).reshape(head, chip_rows) + mixed

    def diagonal(j, carry):
        @pl.when(j % 2 == 0)
        def _():
            pltpu.make_async_remote_copy(stage.at[0], kv.at[chip, pl.ds(j, 2), 1 - core], d2d_ssem.at[j // 2], d2d_rsem.at[j // 2],
                                         device_id={'sp': partner}).wait_recv()

        attend((chip,), j, first=True, ahead=group)
        return carry

    lax.fori_loop(0, local_heads, diagonal, 0)
    poll_first(1)

    def o_copy(k):
        at, size = span_of(k, core)
        target = pl.ds(pl.multiple_of(at, head), size)
        return pltpu.make_async_remote_copy(o_send.at[:, pl.ds(stages[k][0] * width, size)], o_all.at[:, target], o_ssem.at[k], o_rsem.at[k],
                                            device_id={'sp': partner})

    def close_head(j):
        k = min(j // EARLY, 1) + max(0, j - EARLY)
        at = span_of(k, core)[0] + (j - stages[k][0]) * width
        inv = 1.0 / jnp.sum(l_buf[j], axis=0, keepdims=True)
        for g in range(group):
            cols = slice(g * chip_rows, (g + 1) * chip_rows)
            o_val = (o_t[j, :, cols] * inv[:, cols]).T.astype(BF16)
            o_all[:, pl.ds(pl.multiple_of(at + g * head, head), head)] = jnp.where(core == 0, o_val[:rows], o_val[rows:])
            o_send[:, j * width + g * head:j * width + (g + 1) * head] = jnp.where(core == 0, o_val[rows:], o_val[:rows])

    def project_out(k, start, end, half=None):
        if half in (None, 0):
            wo_wait(k)
            o_copy(k).wait_recv()
        at, size = span_of(k, 0)
        depth = slice(at, at + CORES * size)

        def block(n):
            for w in range(wide // width):
                cols = pl.ds(n * wide + w * width, width)
                total = x_buf[:, cols].astype(F32) if start else acc[:, cols]
                total = total + dot(o_all[:, depth], wo_buf[depth, cols])
                if end:
                    out_ref[:, cols] = total.astype(BF16)
                else:
                    acc[:, cols] = total

        wide = dim // 2
        for n in range(dim // wide) if half is None else (half,):
            block(n)

    def ring_step(s, carry):
        @pl.when(s >= local_heads)
        def _():
            poll_rest(s)

        j = lookup(HEAD_TABLE, s)
        d = lookup(HOP_TABLE, s) + 1
        both = (d < far) & (chip + d >= chips)

        @pl.when(both)
        def _():
            attend((item_of(0, d), item_of(1, d)), j)

        @pl.when((chip >= d) & jnp.logical_not(both))
        def _():
            attend((item_of(0, d),), j, ahead=group)

        low = chip < LOW_CHIPS

        @pl.when(s == jnp.where(low, LOW_CLOSE, EARLY_CLOSE))
        def _():
            for early in range(EARLY):
                close_head(early)
            o_copy(0).start()

        @pl.when(s == jnp.where(low, LOW_CLOSE, THIRD_CLOSE))
        def _():
            close_head(EARLY)
            o_copy(1).start()

        @pl.when(s == jnp.where(low, LOW_CLOSE, SLOTS - 1))
        def _():
            close_head(local_heads - 1)
            o_copy(2).start()

        @pl.when((s == FIRST_POLL) | ((s + 1 > local_heads) & (s + 1 < SLOTS)))
        def _():
            poll_near(jnp.where(s == FIRST_POLL, local_heads, s + 1))

        for at, late in DEFERRED:
            @pl.when(s + 1 == at)
            def _():
                forward_first(late)

        for half in range(2):
            @pl.when(s == jnp.where(low, LOW_OUT, EARLY_OUT + half))
            def _():
                project_out(0, True, False, half)

        @pl.when(s == jnp.where(low, LOW_OUT, SLOTS - 1))
        def _():
            project_out(1, False, False)

        @pl.when(s == jnp.where(low, LOW_OUT, SLOTS - 1))
        def _():
            project_out(2, False, True)

        return carry

    lax.fori_loop(0, SLOTS, ring_step, 0)

    h_copy.wait_send()
    for k in range(len(stages)):
        o_copy(k).wait_send()

    def drain_first(idx, carry):
        for copy, cond in first_copies(idx):
            pl.when(cond)(copy.wait_send)
        return carry

    lax.fori_loop(0, 4, drain_first, 0)
    lax.fori_loop(0, local_heads, drain, 0)


def solution(mesh):
    group_size = mesh.shape['sp']

    def device_step(hidden, ln_gain, w_q, w_k, w_v, w_o, q_gain, k_gain):
        rows, dim = hidden.shape
        head = q_gain.shape[0]
        half = head // 2
        chips = group_size // CORES
        local_heads = w_k.shape[1] // head // CORES
        width = w_q.shape[1] // CORES // local_heads
        chip_rows = rows * CORES
        inv_freq = THETA ** -(np.arange(half, dtype=np.float64) * (2.0 / head))
        angles = inv_freq[:, None] * np.arange(rows * group_size)[None, :]
        angle_all = jnp.asarray(np.stack([np.cos(angles), np.sin(angles)]).astype(np.float32))
        hbm = pl.BlockSpec(memory_space=pl.ANY)
        dma = pltpu.SemaphoreType.DMA
        wide = width // head * chip_rows
        return pl.pallas_call(
            functools.partial(kernel, group_size),
            out_shape=pltpu.VMEM((rows, dim), BF16),
            in_specs=[hbm] * 9,
            out_specs=pl.BlockSpec(memory_space=pltpu.VMEM),
            scratch_shapes=[
                pltpu.VMEM((rows, dim), BF16),
                pltpu.VMEM((CORES, rows, dim), BF16),
                pltpu.VMEM((3, dim, width), BF16),
                pltpu.VMEM(w_o.shape, BF16),
                pltpu.VMEM((chips, local_heads, CORES, 2, rows, head), BF16),
                pltpu.VMEM((4, 2, 2, rows, head), BF16),
                pltpu.VMEM((local_heads, head, wide), BF16),
                pltpu.VMEM((local_heads, head, wide), F32),
                pltpu.VMEM((local_heads, 8, wide), F32),
                pltpu.VMEM((local_heads, 8, wide), F32),
                pltpu.VMEM((rows, w_o.shape[0]), BF16),
                pltpu.VMEM((rows, local_heads * width), BF16),
                pltpu.VMEM((rows, dim), F32),
                pltpu.VMEM((dim // LANES, LANES), BF16),
                pltpu.VMEM((2, 1, head), BF16),
                pltpu.VMEM((2, half, chip_rows), F32),
                pltpu.VMEM((head, chip_rows), F32),
                pltpu.VMEM((rows, head), F32),
                pltpu.VMEM((rows, head), F32),
                dma((2,)), dma((4,)), dma((3, 2)), dma((3,)), dma, dma,
                dma((2,)), dma((2,)),
                dma((2, 4)), dma((2, 2)),
                dma((2, 2 * local_heads)), dma((2, 4 * local_heads)),
                dma((3,)), dma((3,)),
            ],
            compiler_params=pltpu.CompilerParams(collective_id=0, has_side_effects=True, vmem_limit_bytes=VMEM_LIMIT),
        )(hidden, w_q, w_k, w_v, w_o, ln_gain.reshape(-1, LANES), q_gain[None, :], k_gain[None, :], angle_all)

    row_spec = P(('dp', 'sp'), None)
    return jax.shard_map(device_step, mesh=mesh, in_specs=(row_spec, P(), P(), P(), P(), P(), P(), P()), out_specs=row_spec, check_vma=False)
```

```python
import functools
import jax
import jax.numpy as jnp
import numpy as np
from jax import lax
from jax.experimental import pallas as pl
from jax.experimental.pallas import tpu as pltpu
from jax.sharding import PartitionSpec as P

EPS = 1e-6
THETA = 1000000.0
LOG2E = 1.4426950408889634
CORES = 2
LANES = 128
VMEM_LIMIT = 62 * 2 ** 20
BF16 = jnp.bfloat16
F32 = jnp.float32


def dot(a, b):
    return jnp.dot(a, b, preferred_element_type=F32)


ORDER = ((0, 1), (1, 1), (2, 1), (3, 1), (0, 2), (1, 2), (0, 3), (1, 3), (2, 2), (0, 4), (1, 4), (3, 2), (2, 3), (3, 3), (2, 4), (3, 4))
SLOTS = len(ORDER)
EARLY = 2
FIRST_POLL = 1
LOW_CHIPS = 2
LOW_CLOSE = 7
LOW_OUT = 9
EARLY_CLOSE = 10
EARLY_OUT = 11
THIRD_CLOSE = 14
DEFERRED = ((5, 2), (7, 3))
NEAR, REST, WHOLE = 0, 1, 2


def slot_table(values):
    return tuple(sum(v << (2 * s) for s, v in enumerate(values[h:h + 8])) for h in (0, 8))


HEAD_TABLE = slot_table([j for j, _ in ORDER])
HOP_TABLE = slot_table([d - 1 for _, d in ORDER])


def lookup(table, s):
    return lax.shift_right_logical(jnp.where(s < 8, table[0], table[1]), 2 * (s % 8)) % 4


def kernel(group_size, x_hbm, wq, wk, wv, wo, ln_hbm, q_gain_hbm, k_gain_hbm, angle_hbm, out_ref,
           x_buf, h_buf, w_buf, wo_buf, kv, stage, q_t, o_t, m_buf, l_buf, o_all, o_send, acc,
           ln_buf, gain_buf, angle_t, gain_t, cos_k, sin_k,
           x_sem, small_sem, w_sem, wo_sem, h_ssem, h_rsem, d2d_ssem, d2d_rsem, first_ssem, first_rsem, ring_ssem, ring_rsem, o_ssem, o_rsem):
    chips = group_size // CORES
    me = lax.axis_index('sp')
    chip = me // CORES
    core = me % CORES
    partner = chip * CORES + (1 - core)
    rows, dim = x_buf.shape
    head = gain_buf.shape[2]
    half_head = head // 2
    width = w_buf.shape[2]
    local_heads = kv.shape[1]
    group = width // head
    chip_rows = rows * CORES
    far = chips // 2
    mixed_dim = local_heads * width
    lanes = ln_buf.shape[1]

    def device(c, k):
        return {'sp': c * CORES + k}

    def neighbour(dirn):
        return (chip + chips + 1 - 2 * dirn) % chips

    x_parts = x_sem.shape[0]
    part_rows = rows // x_parts

    def x_copy(r):
        sl = pl.ds(r * part_rows, part_rows)
        return pltpu.make_async_copy(x_hbm.at[sl, :], x_buf.at[sl, :], x_sem.at[r])

    chip_cols = pl.ds(pl.multiple_of(chip * chip_rows, chip_rows), chip_rows)
    small = (pltpu.make_async_copy(ln_hbm, ln_buf, small_sem.at[0]),
             pltpu.make_async_copy(q_gain_hbm, gain_buf.at[0], small_sem.at[1]),
             pltpu.make_async_copy(k_gain_hbm, gain_buf.at[1], small_sem.at[2]),
             pltpu.make_async_copy(angle_hbm.at[:, :, chip_cols], angle_t, small_sem.at[3]))

    def kv_copies(idx):
        pair = (idx % 2) * 2 + idx // 2
        cols = pl.ds(pl.multiple_of(pair * (width // 2), width // 2), width // 2)
        slot = idx % 3
        return (pltpu.make_async_copy(wk.at[:, cols], w_buf.at[slot, :, pl.ds(0, width // 2)], w_sem.at[slot, 0]),
                pltpu.make_async_copy(wv.at[:, cols], w_buf.at[slot, :, pl.ds(width // 2, width // 2)], w_sem.at[slot, 1]))

    def lead_copies(e):
        cols = pl.ds(e * head, head)
        return tuple(pltpu.make_async_copy(w.at[:, cols], w_buf.at[0, :, pl.ds((2 * e + part) * head, head)], w_sem.at[0, e])
                     for part, w in enumerate((wk, wv)))

    def lead_wait(e):
        pltpu.make_async_copy(wk.at[:, pl.ds(0, 2 * head)], w_buf.at[0, :, pl.ds(2 * e * head, 2 * head)], w_sem.at[0, e]).wait()

    def q_copies(idx):
        cols = pl.ds(pl.multiple_of((core * local_heads + idx) * width, width), width)
        slot = (idx + 4) % 3
        return tuple(pltpu.make_async_copy(wq.at[pl.ds(r * (dim // 2), dim // 2), cols],
                                           w_buf.at[slot, pl.ds(r * (dim // 2), dim // 2), :], w_sem.at[slot, r]) for r in range(2))

    stages = ((0, EARLY), (EARLY, EARLY + 1), (EARLY + 1, local_heads))

    def span_of(k, c):
        first, last = stages[k]
        return (CORES * first + c * (last - first)) * width, (last - first) * width

    def wo_copies(k):
        copies = []
        for c in range(CORES):
            at, size = span_of(k, c)
            source = pl.ds(c * mixed_dim + stages[k][0] * width, size)
            copies.append(pltpu.make_async_copy(wo.at[source, :], wo_buf.at[pl.ds(at, size), :], wo_sem.at[k]))
        return copies

    def wo_wait(k):
        at, size = span_of(k, 0)
        span = pl.ds(at, CORES * size)
        pltpu.make_async_copy(wo.at[span, :], wo_buf.at[span, :], wo_sem.at[k]).wait()

    for copy in small[:1]:
        copy.start()
    for r in range(x_parts):
        x_copy(r).start()
    for copy in small[1:]:
        copy.start()
    for copy in lead_copies(0):
        copy.start()

    barrier = pltpu.get_barrier_semaphore()
    pl.semaphore_signal(barrier, inc=1, device_id={'sp': partner})
    for dirn in range(2):
        for k in range(CORES):
            pl.semaphore_signal(barrier, inc=1, device_id=device(neighbour(dirn), k))

    small[0].wait()
    for r in range(x_parts):
        if r == x_parts - 1:
            for copy in small[1:]:
                copy.wait()
            own_cols = pl.ds(pl.multiple_of(core * rows, rows), rows)
            cos_own = angle_t[0, :, own_cols].T
            sin_own = angle_t[1, :, own_cols].T
            cos_k[...] = jnp.concatenate([cos_own, cos_own], axis=1)
            sin_k[...] = jnp.concatenate([-sin_own, sin_own], axis=1)
        x_copy(r).wait()
        if r == 1:
            for copy in lead_copies(1):
                copy.start()
        if r == x_parts - 1:
            for copy in kv_copies(1):
                copy.start()
        step_rows = 16
        for t in range(part_rows // step_rows):
            sl = slice(r * part_rows + t * step_rows, r * part_rows + (t + 1) * step_rows)
            xf = x_buf[sl, :].astype(F32)
            scale = lax.rsqrt(jnp.mean(xf * xf, axis=-1, keepdims=True) + EPS)
            for b in range(dim // lanes):
                cols = slice(b * lanes, (b + 1) * lanes)
                h_buf[core, sl, cols] = (xf[:, cols] * scale * ln_buf[b:b + 1, :].astype(F32)).astype(BF16)

    pl.semaphore_wait(barrier, 1 + 2 * CORES)
    h_copy = pltpu.make_async_remote_copy(h_buf.at[core], h_buf.at[core], h_ssem, h_rsem, device_id={'sp': partner})

    def first_copies(idx, e=None):
        owner = idx % 2
        pair = idx // 2
        src = stage.at[idx] if e is None else stage.at[idx, e]
        dst = kv.at[chip, pl.ds(pair * 2, 2), core] if e is None else kv.at[chip, e, core]
        up = pltpu.make_async_remote_copy(src, dst, first_ssem.at[0, idx], first_rsem.at[0, pair], device_id=device(neighbour(0), owner))
        down = pltpu.make_async_remote_copy(src, dst, first_ssem.at[1, idx], first_rsem.at[1, pair], device_id=device(neighbour(1), owner))
        across = pltpu.make_async_remote_copy(src, dst, d2d_ssem.at[pair], d2d_rsem.at[pair], device_id={'sp': partner})
        return ((up, chip < chips - 1), (down, chip < far), (across, owner != core))

    def keep_kv(idx, e, k_raw, v_raw):
        t = k_raw * lax.rsqrt(jnp.mean(k_raw * k_raw, axis=-1, keepdims=True) + EPS) * gain_buf[1].astype(F32)
        k_val = (t * cos_k[...] + pltpu.roll(t, half_head, 1) * sin_k[...]).astype(BF16)
        v_val = v_raw.T.astype(BF16)
        stage[idx, e, 0] = k_val
        stage[idx, e, 1] = v_val

        @pl.when(idx % 2 == core)
        def _():
            kv[chip, (idx // 2) * 2 + e, core, 0] = k_val
            kv[chip, (idx // 2) * 2 + e, core, 1] = v_val

    for e in range(2):
        lead_wait(e)
        both = slice(2 * e * head, 2 * (e + 1) * head)
        o_t[e, :rows, :2 * head] = dot(h_buf[core, :, :dim // 2], w_buf[0, :dim // 2, both])
        raw = dot(h_buf[core, :, dim // 2:], w_buf[0, dim // 2:, both]) + o_t[e, :rows, :2 * head]
        if e == 0:
            for copy in kv_copies(2):
                copy.start()
        keep_kv(0, e, raw[:, :head], raw[:, head:])
        for copy, cond in first_copies(0, e):
            pl.when(cond)(copy.start)
    for copy in kv_copies(3):
        copy.start()
    h_copy.start()

    def project_kv(idx, carry):
        slot = idx % 3
        for copy in kv_copies(idx):
            copy.wait()
        raw = dot(h_buf[core], w_buf[slot])
        for copy in q_copies(idx - 1):
            copy.start()
        for e in range(2):
            keep_kv(idx, e, raw[:, e * head:(e + 1) * head], raw[:, width // 2 + e * head:width // 2 + (e + 1) * head])
        for copy, cond in first_copies(idx):
            pl.when(cond)(copy.start)
        return carry

    lax.fori_loop(1, 4, project_kv, 0)
    gain_t[...] = jnp.broadcast_to(gain_buf[0].astype(F32), (chip_rows, head)).T
    h_copy.wait_recv()

    def item_of(dirn, d):
        return (chip + chips + (2 * dirn - 1) * d) % chips

    def arrives(dirn, d):
        return chip >= d if dirn == 0 else item_of(1, d) < far

    def goes_on(dirn, d):
        return arrives(dirn, d) & (chip < chips - 1) if dirn == 0 else arrives(dirn, d)

    def ring_copy(dirn, j, d, item, part):
        half = (dirn, 1 - dirn, None)[part]
        sem = (d - 2) * local_heads + j + (2 * local_heads if part == REST else 0)
        ref = kv.at[item, j] if half is None else kv.at[item, j, half]
        return pltpu.make_async_remote_copy(ref, ref, ring_ssem.at[dirn, local_heads if part == REST else j], ring_rsem.at[dirn, sem], device_id=device(neighbour(dirn), core))

    def outgoing(dirn, j, d, part):
        return ring_copy(dirn, j, d, item_of(dirn, d - 1), part)

    def landed(dirn, j, d, part):
        return ring_copy(dirn, j, d, item_of(dirn, d), part)

    def forward_first(j):
        for dirn in range(2):
            pl.when(goes_on(dirn, 1))(outgoing(dirn, j, 2, WHOLE).start)

    def poll_first(pair):
        for dirn in range(2):
            @pl.when(arrives(dirn, 1))
            def _():
                both = kv.at[item_of(dirn, 1), pl.ds(pair * 2, 2)]
                pltpu.make_async_remote_copy(both, both, first_ssem.at[0, 0], first_rsem.at[dirn, pair], device_id={'sp': partner}).wait_recv()

    def poll_near(s):
        j = lookup(HEAD_TABLE, s)
        d = lookup(HOP_TABLE, s) + 1
        for dirn in range(2):
            @pl.when(arrives(dirn, 2) & (d == 2))
            def _():
                landed(dirn, j, 2, WHOLE).wait_recv()

            @pl.when(goes_on(dirn, 2) & (d == 2))
            def _():
                pl.when(goes_on(dirn, 1))(outgoing(dirn, j, 2, WHOLE).wait_send)
                outgoing(dirn, j, 3, NEAR).start()
                outgoing(dirn, j, 3, REST).start()

            @pl.when(arrives(dirn, 3) & (d == 3))
            def _():
                landed(dirn, j, 3, NEAR).wait_recv()

            @pl.when(goes_on(dirn, 3) & (d == 3))
            def _():
                pl.when(goes_on(dirn, 2))(outgoing(dirn, j, 3, NEAR).wait_send)
                outgoing(dirn, j, 4, NEAR).start()

    def poll_rest(s):
        j = lookup(HEAD_TABLE, s)
        d = lookup(HOP_TABLE, s) + 1
        for dirn in range(2):
            @pl.when(arrives(dirn, 3) & (d == 3))
            def _():
                landed(dirn, j, 3, REST).wait_recv()

            @pl.when(arrives(dirn, 4) & (d == 4))
            def _():
                landed(dirn, j, 4, NEAR).wait_recv()

    def drain(j, carry):
        for dirn in range(2):
            on = [goes_on(dirn, d) for d in range(4)]
            pl.when(on[1] & jnp.logical_not(on[2]))(outgoing(dirn, j, 2, WHOLE).wait_send)
            pl.when(on[2] & jnp.logical_not(on[3]))(outgoing(dirn, j, 3, NEAR).wait_send)
            pl.when(on[3])(outgoing(dirn, j, 4, NEAR).wait_send)
        return carry

    def project_q(idx, carry):
        slot = (idx + 4) % 3
        for copy in q_copies(idx):
            copy.wait()
        raw = dot(h_buf[...].reshape(chip_rows, dim), w_buf[slot])

        @pl.when(idx == 0)
        def _():
            for copy in q_copies(3):
                copy.start()

        @pl.when(idx == local_heads - 1)
        def _():
            poll_first(0)
            forward_first(0)
            forward_first(1)

        for g in range(group):
            t = raw[:, g * head:(g + 1) * head].T
            t = t * lax.rsqrt(jnp.mean(t * t, axis=0, keepdims=True) + EPS) * gain_t[...]
            t1 = t[:half_head]
            t2 = t[half_head:]
            c = angle_t[0]
            s = angle_t[1]
            q_t[idx, :, g * chip_rows:(g + 1) * chip_rows] = jnp.concatenate([t1 * c - t2 * s, t2 * c + t1 * s], axis=0).astype(BF16)
        return carry

    lax.fori_loop(0, local_heads, project_q, 0)
    for k in range(len(stages)):
        for copy in wo_copies(k):
            copy.start()

    score_scale = (head ** -0.5) * LOG2E

    def attend(items, j, first=False, ahead=2):
        keys = [kv[item, j, :, 0].reshape(chip_rows, head) for item in items]
        vals = jnp.concatenate([kv[item, j, c, 1] for item in items for c in range(CORES)], axis=1)

        def scores_of(g):
            return [dot(k, q_t[j, :, g * chip_rows:(g + 1) * chip_rows]) for k in keys]

        pending = [scores_of(g) for g in range(ahead)]
        for g in range(group):
            cols = slice(g * chip_rows, (g + 1) * chip_rows)
            scores = pending[g]
            if first:
                key_pos = lax.broadcasted_iota(jnp.int32, scores[0].shape, 0)
                q_pos = lax.broadcasted_iota(jnp.int32, scores[0].shape, 1)
                scores = [jnp.where(key_pos <= q_pos, scores[0], -jnp.inf)]
            top = functools.reduce(jnp.maximum, [jnp.max(x.reshape(chip_rows // 8, 8, chip_rows), axis=0) for x in scores])
            top = jnp.max(top, axis=0, keepdims=True)
            if first:
                m_new = jnp.broadcast_to(top, (8, chip_rows))
            else:
                m_old = m_buf[j, :, cols]
                m_new = jnp.maximum(m_old, top)
            probs = [jnp.exp2((x.reshape(chip_rows // 8, 8, chip_rows) - m_new[None]) * score_scale) for x in scores]
            total = functools.reduce(jnp.add, [jnp.sum(p, axis=0) for p in probs])
            if g + ahead < group:
                pending.append(scores_of(g + ahead))
            mixed = dot(vals, jnp.concatenate([p.reshape(chip_rows, chip_rows).astype(BF16) for p in probs], axis=0))
            m_buf[j, :, cols] = m_new
            if first:
                l_buf[j, :, cols] = total
                o_t[j, :, cols] = mixed
            else:
                alpha = jnp.exp2((m_old - m_new) * score_scale)
                l_buf[j, :, cols] = l_buf[j, :, cols] * alpha + total
                old = o_t[j, :, cols].reshape(head // 8, 8, chip_rows)
                o_t[j, :, cols] = (old * alpha[None]).reshape(head, chip_rows) + mixed

    def diagonal(j, carry):
        @pl.when(j % 2 == 0)
        def _():
            pltpu.make_async_remote_copy(stage.at[0], kv.at[chip, pl.ds(j, 2), 1 - core], d2d_ssem.at[j // 2], d2d_rsem.at[j // 2],
                                         device_id={'sp': partner}).wait_recv()

        attend((chip,), j, first=True, ahead=group)
        return carry

    lax.fori_loop(0, local_heads, diagonal, 0)
    poll_first(1)

    def o_copy(k):
        at, size = span_of(k, core)
        target = pl.ds(pl.multiple_of(at, head), size)
        return pltpu.make_async_remote_copy(o_send.at[:, pl.ds(stages[k][0] * width, size)], o_all.at[:, target], o_ssem, o_rsem.at[k],
                                            device_id={'sp': partner})

    def close_head(j):
        k = min(j // EARLY, 1) + max(0, j - EARLY)
        at = span_of(k, core)[0] + (j - stages[k][0]) * width
        inv = 1.0 / jnp.sum(l_buf[j], axis=0, keepdims=True)
        for g in range(group):
            cols = slice(g * chip_rows, (g + 1) * chip_rows)
            o_val = (o_t[j, :, cols] * inv[:, cols]).T.astype(BF16)
            o_all[:, pl.ds(pl.multiple_of(at + g * head, head), head)] = jnp.where(core == 0, o_val[:rows], o_val[rows:])
            o_send[:, j * width + g * head:j * width + (g + 1) * head] = jnp.where(core == 0, o_val[rows:], o_val[:rows])

    def project_out(k, start, end, half=None):
        if half in (None, 0):
            wo_wait(k)
            o_copy(k).wait_recv()
        at, size = span_of(k, 0)
        depth = slice(at, at + CORES * size)

        def block(n):
            for w in range(wide // width):
                cols = pl.ds(n * wide + w * width, width)
                total = x_buf[:, cols].astype(F32) if start else acc[:, cols]
                total = total + dot(o_all[:, depth], wo_buf[depth, cols])
                if end:
                    out_ref[:, cols] = total.astype(BF16)
                else:
                    acc[:, cols] = total

        wide = dim // 2
        for n in range(dim // wide) if half is None else (half,):
            block(n)

    def ring_step(s, carry):
        @pl.when(s >= local_heads)
        def _():
            poll_rest(s)

        j = lookup(HEAD_TABLE, s)
        d = lookup(HOP_TABLE, s) + 1
        both = (d < far) & (chip + d >= chips)

        @pl.when(both)
        def _():
            attend((item_of(0, d), item_of(1, d)), j)

        @pl.when((chip >= d) & jnp.logical_not(both))
        def _():
            attend((item_of(0, d),), j, ahead=group)

        low = chip < LOW_CHIPS

        @pl.when(s == jnp.where(low, LOW_CLOSE, EARLY_CLOSE))
        def _():
            for early in range(EARLY):
                close_head(early)
            o_copy(0).start()

        @pl.when(s == jnp.where(low, LOW_CLOSE, THIRD_CLOSE))
        def _():
            close_head(EARLY)
            o_copy(1).start()

        @pl.when(s == jnp.where(low, LOW_CLOSE, SLOTS - 1))
        def _():
            close_head(local_heads - 1)
            o_copy(2).start()

        @pl.when((s == FIRST_POLL) | ((s + 1 > local_heads) & (s + 1 < SLOTS)))
        def _():
            poll_near(jnp.where(s == FIRST_POLL, local_heads, s + 1))

        for at, late in DEFERRED:
            @pl.when(s + 1 == at)
            def _():
                forward_first(late)

        for half in range(2):
            @pl.when(s == jnp.where(low, LOW_OUT, EARLY_OUT + half))
            def _():
                project_out(0, True, False, half)

        @pl.when(s == jnp.where(low, LOW_OUT, SLOTS - 1))
        def _():
            project_out(1, False, False)

        @pl.when(s == jnp.where(low, LOW_OUT, SLOTS - 1))
        def _():
            project_out(2, False, True)

        return carry

    lax.fori_loop(0, SLOTS, ring_step, 0)

    h_copy.wait_send()
    pltpu.make_async_remote_copy(o_send, o_all.at[:, pl.ds(0, mixed_dim)], o_ssem, o_rsem.at[0], device_id={'sp': partner}).wait_send()

    def drain_first(idx, carry):
        for copy, cond in first_copies(idx):
            pl.when(cond)(copy.wait_send)
        return carry

    lax.fori_loop(0, 4, drain_first, 0)
    lax.fori_loop(0, local_heads, drain, 0)
    for dirn in range(2):
        @pl.when(goes_on(dirn, 2))
        def _():
            rest = kv.at[item_of(dirn, 2), :, 1 - dirn]
            pltpu.make_async_remote_copy(rest, rest, ring_ssem.at[dirn, local_heads], ring_rsem.at[dirn, 0], device_id=device(neighbour(dirn), core)).wait_send()


def solution(mesh):
    group_size = mesh.shape['sp']

    def device_step(hidden, ln_gain, w_q, w_k, w_v, w_o, q_gain, k_gain):
        rows, dim = hidden.shape
        head = q_gain.shape[0]
        half = head // 2
        chips = group_size // CORES
        local_heads = w_k.shape[1] // head // CORES
        width = w_q.shape[1] // CORES // local_heads
        chip_rows = rows * CORES
        inv_freq = THETA ** -(np.arange(half, dtype=np.float64) * (2.0 / head))
        angles = inv_freq[:, None] * np.arange(rows * group_size)[None, :]
        angle_all = jnp.asarray(np.stack([np.cos(angles), np.sin(angles)]).astype(np.float32))
        hbm = pl.BlockSpec(memory_space=pl.ANY)
        dma = pltpu.SemaphoreType.DMA
        wide = width // head * chip_rows
        return pl.pallas_call(
            functools.partial(kernel, group_size),
            out_shape=pltpu.VMEM((rows, dim), BF16),
            in_specs=[hbm] * 9,
            out_specs=pl.BlockSpec(memory_space=pltpu.VMEM),
            scratch_shapes=[
                pltpu.VMEM((rows, dim), BF16),
                pltpu.VMEM((CORES, rows, dim), BF16),
                pltpu.VMEM((3, dim, width), BF16),
                pltpu.VMEM(w_o.shape, BF16),
                pltpu.VMEM((chips, local_heads, CORES, 2, rows, head), BF16),
                pltpu.VMEM((4, 2, 2, rows, head), BF16),
                pltpu.VMEM((local_heads, head, wide), BF16),
                pltpu.VMEM((local_heads, head, wide), F32),
                pltpu.VMEM((local_heads, 8, wide), F32),
                pltpu.VMEM((local_heads, 8, wide), F32),
                pltpu.VMEM((rows, w_o.shape[0]), BF16),
                pltpu.VMEM((rows, local_heads * width), BF16),
                pltpu.VMEM((rows, dim), F32),
                pltpu.VMEM((dim // LANES, LANES), BF16),
                pltpu.VMEM((2, 1, head), BF16),
                pltpu.VMEM((2, half, chip_rows), F32),
                pltpu.VMEM((head, chip_rows), F32),
                pltpu.VMEM((rows, head), F32),
                pltpu.VMEM((rows, head), F32),
                dma((4,)), dma((4,)), dma((3, 2)), dma((3,)), dma, dma,
                dma((2,)), dma((2,)),
                dma((2, 4)), dma((2, 2)),
                dma((2, local_heads + 1)), dma((2, 4 * local_heads)),
                dma, dma((3,)),
            ],
            compiler_params=pltpu.CompilerParams(collective_id=0, has_side_effects=True, vmem_limit_bytes=VMEM_LIMIT),
        )(hidden, w_q, w_k, w_v, w_o, ln_gain.reshape(-1, LANES), q_gain[None, :], k_gain[None, :], angle_all)

    row_spec = P(('dp', 'sp'), None)
    return jax.shard_map(device_step, mesh=mesh, in_specs=(row_spec, P(), P(), P(), P(), P(), P(), P()), out_specs=row_spec, check_vma=False)
```

```python
import functools
import jax
import jax.numpy as jnp
import numpy as np
from jax import lax
from jax.experimental import pallas as pl
from jax.experimental.pallas import tpu as pltpu
from jax.sharding import PartitionSpec as P

EPS = 1e-6
THETA = 1000000.0
LOG2E = 1.4426950408889634
CORES = 2
LANES = 128
VMEM_LIMIT = 62 * 2 ** 20
BF16 = jnp.bfloat16
F32 = jnp.float32


def dot(a, b):
    return jnp.dot(a, b, preferred_element_type=F32)


ORDER = ((0, 1), (1, 1), (2, 1), (3, 1), (0, 2), (1, 2), (0, 3), (1, 3), (2, 2), (0, 4), (1, 4), (3, 2), (2, 3), (3, 3), (2, 4), (3, 4))
SLOTS = len(ORDER)
EARLY = 2
FIRST_POLL = 1
LOW_CHIPS = 2
LOW_CLOSE = 7
LOW_OUT = 9
EARLY_CLOSE = 10
EARLY_OUT = 11
THIRD_CLOSE = 14
DEFERRED = ((5, 2), (7, 3))
NEAR, REST, WHOLE = 0, 1, 2


def slot_table(values):
    return tuple(sum(v << (2 * s) for s, v in enumerate(values[h:h + 8])) for h in (0, 8))


HEAD_TABLE = slot_table([j for j, _ in ORDER])
HOP_TABLE = slot_table([d - 1 for _, d in ORDER])


def lookup(table, s):
    return lax.shift_right_logical(jnp.where(s < 8, table[0], table[1]), 2 * (s % 8)) % 4


def kernel(group_size, x_hbm, wq, wk, wv, wo, ln_hbm, q_gain_hbm, k_gain_hbm, angle_hbm, out_ref,
           x_buf, h_buf, w_buf, wo_buf, kv, stage, q_t, o_t, m_buf, l_buf, o_all, o_send, acc,
           ln_buf, gain_buf, angle_t, gain_t, cos_k, sin_k,
           x_sem, small_sem, w_sem, wo_sem, h_ssem, h_rsem, d2d_ssem, d2d_rsem, first_ssem, first_rsem, ring_ssem, ring_rsem, o_ssem, o_rsem):
    chips = group_size // CORES
    me = lax.axis_index('sp')
    chip = me // CORES
    core = me % CORES
    partner = chip * CORES + (1 - core)
    rows, dim = x_buf.shape
    head = gain_buf.shape[2]
    half_head = head // 2
    width = w_buf.shape[2]
    local_heads = kv.shape[1]
    group = width // head
    chip_rows = rows * CORES
    far = chips // 2
    mixed_dim = local_heads * width
    lanes = ln_buf.shape[1]

    def device(c, k):
        return {'sp': c * CORES + k}

    def neighbour(dirn):
        return (chip + chips + 1 - 2 * dirn) % chips

    x_parts = x_sem.shape[0]
    part_rows = rows // x_parts

    def x_copy(r):
        sl = pl.ds(r * part_rows, part_rows)
        return pltpu.make_async_copy(x_hbm.at[sl, :], x_buf.at[sl, :], x_sem.at[r])

    chip_cols = pl.ds(pl.multiple_of(chip * chip_rows, chip_rows), chip_rows)
    small = (pltpu.make_async_copy(ln_hbm, ln_buf, small_sem.at[0]),
             pltpu.make_async_copy(q_gain_hbm, gain_buf.at[0], small_sem.at[1]),
             pltpu.make_async_copy(k_gain_hbm, gain_buf.at[1], small_sem.at[2]),
             pltpu.make_async_copy(angle_hbm.at[:, :, chip_cols], angle_t, small_sem.at[3]))

    def kv_copies(idx):
        pair = (idx % 2) * 2 + idx // 2
        cols = pl.ds(pl.multiple_of(pair * (width // 2), width // 2), width // 2)
        slot = idx % 3
        return (pltpu.make_async_copy(wk.at[:, cols], w_buf.at[slot, :, pl.ds(0, width // 2)], w_sem.at[slot, 0]),
                pltpu.make_async_copy(wv.at[:, cols], w_buf.at[slot, :, pl.ds(width // 2, width // 2)], w_sem.at[slot, 1]))

    def lead_copies(e):
        cols = pl.ds(e * head, head)
        return tuple(pltpu.make_async_copy(w.at[:, cols], w_buf.at[0, :, pl.ds((2 * e + part) * head, head)], w_sem.at[0, e])
                     for part, w in enumerate((wk, wv)))

    def lead_wait(e):
        pltpu.make_async_copy(wk.at[:, pl.ds(0, 2 * head)], w_buf.at[0, :, pl.ds(2 * e * head, 2 * head)], w_sem.at[0, e]).wait()

    def q_copies(idx):
        cols = pl.ds(pl.multiple_of((core * local_heads + idx) * width, width), width)
        slot = (idx + 4) % 3
        return tuple(pltpu.make_async_copy(wq.at[pl.ds(r * (dim // 2), dim // 2), cols],
                                           w_buf.at[slot, pl.ds(r * (dim // 2), dim // 2), :], w_sem.at[slot, r]) for r in range(2))

    stages = ((0, EARLY), (EARLY, EARLY + 1), (EARLY + 1, local_heads))

    def span_of(k, c):
        first, last = stages[k]
        return (CORES * first + c * (last - first)) * width, (last - first) * width

    def wo_copies(k):
        copies = []
        for c in range(CORES):
            at, size = span_of(k, c)
            source = pl.ds(c * mixed_dim + stages[k][0] * width, size)
            copies.append(pltpu.make_async_copy(wo.at[source, :], wo_buf.at[pl.ds(at, size), :], wo_sem.at[k]))
        return copies

    def wo_wait(k):
        at, size = span_of(k, 0)
        span = pl.ds(at, CORES * size)
        pltpu.make_async_copy(wo.at[span, :], wo_buf.at[span, :], wo_sem.at[k]).wait()

    for copy in small[:1]:
        copy.start()
    for r in range(x_parts):
        x_copy(r).start()
    for copy in small[1:]:
        copy.start()
    for copy in lead_copies(0):
        copy.start()

    barrier = pltpu.get_barrier_semaphore()
    pl.semaphore_signal(barrier, inc=1, device_id={'sp': partner})
    for dirn in range(2):
        for k in range(CORES):
            pl.semaphore_signal(barrier, inc=1, device_id=device(neighbour(dirn), k))

    small[0].wait()
    for r in range(x_parts):
        if r == x_parts - 1:
            for copy in small[1:]:
                copy.wait()
            own_cols = pl.ds(pl.multiple_of(core * rows, rows), rows)
            cos_own = angle_t[0, :, own_cols].T
            sin_own = angle_t[1, :, own_cols].T
            cos_k[...] = jnp.concatenate([cos_own, cos_own], axis=1)
            sin_k[...] = jnp.concatenate([-sin_own, sin_own], axis=1)
        x_copy(r).wait()
        if r == 1:
            for copy in lead_copies(1):
                copy.start()
        if r == x_parts - 1:
            for copy in kv_copies(1):
                copy.start()
        step_rows = 16
        for t in range(part_rows // step_rows):
            sl = slice(r * part_rows + t * step_rows, r * part_rows + (t + 1) * step_rows)
            xf = x_buf[sl, :].astype(F32)
            scale = lax.rsqrt(jnp.mean(xf * xf, axis=-1, keepdims=True) + EPS)
            for b in range(dim // lanes):
                cols = slice(b * lanes, (b + 1) * lanes)
                h_buf[core, sl, cols] = (xf[:, cols] * scale * ln_buf[b:b + 1, :].astype(F32)).astype(BF16)

    pl.semaphore_wait(barrier, 1 + 2 * CORES)
    h_copy = pltpu.make_async_remote_copy(h_buf.at[core], h_buf.at[core], h_ssem, h_rsem, device_id={'sp': partner})

    def first_copies(idx, e=None):
        owner = idx % 2
        pair = idx // 2
        src = stage.at[idx] if e is None else stage.at[idx, e]
        dst = kv.at[chip, pl.ds(pair * 2, 2), core] if e is None else kv.at[chip, e, core]
        up = pltpu.make_async_remote_copy(src, dst, first_ssem.at[0, idx], first_rsem.at[0, pair], device_id=device(neighbour(0), owner))
        down = pltpu.make_async_remote_copy(src, dst, first_ssem.at[1, idx], first_rsem.at[1, pair], device_id=device(neighbour(1), owner))
        across = pltpu.make_async_remote_copy(src, dst, d2d_ssem.at[pair], d2d_rsem.at[pair], device_id={'sp': partner})
        return ((up, chip < chips - 1), (down, chip < far), (across, owner != core))

    def keep_kv(idx, e, k_raw, v_raw):
        t = k_raw * lax.rsqrt(jnp.mean(k_raw * k_raw, axis=-1, keepdims=True) + EPS) * gain_buf[1].astype(F32)
        k_val = (t * cos_k[...] + pltpu.roll(t, half_head, 1) * sin_k[...]).astype(BF16)
        v_val = v_raw.T.astype(BF16)
        stage[idx, e, 0] = k_val
        stage[idx, e, 1] = v_val

        @pl.when(idx % 2 == core)
        def _():
            kv[chip, (idx // 2) * 2 + e, core, 0] = k_val
            kv[chip, (idx // 2) * 2 + e, core, 1] = v_val

    for e in range(2):
        lead_wait(e)
        both = slice(2 * e * head, 2 * (e + 1) * head)
        o_t[e, :rows, :2 * head] = dot(h_buf[core, :, :dim // 2], w_buf[0, :dim // 2, both])
        raw = dot(h_buf[core, :, dim // 2:], w_buf[0, dim // 2:, both]) + o_t[e, :rows, :2 * head]
        if e == 0:
            for copy in kv_copies(2):
                copy.start()
        keep_kv(0, e, raw[:, :head], raw[:, head:])
        for copy, cond in first_copies(0, e):
            pl.when(cond)(copy.start)
    for copy in kv_copies(3):
        copy.start()
    h_copy.start()

    def project_kv(idx, carry):
        slot = idx % 3
        for copy in kv_copies(idx):
            copy.wait()
        raw = dot(h_buf[core], w_buf[slot])
        for copy in q_copies(idx - 1):
            copy.start()
        for e in range(2):
            keep_kv(idx, e, raw[:, e * head:(e + 1) * head], raw[:, width // 2 + e * head:width // 2 + (e + 1) * head])
        for copy, cond in first_copies(idx):
            pl.when(cond)(copy.start)
        return carry

    lax.fori_loop(1, 4, project_kv, 0)
    gain_t[...] = jnp.broadcast_to(gain_buf[0].astype(F32), (chip_rows, head)).T
    h_copy.wait_recv()

    def item_of(dirn, d):
        return (chip + chips + (2 * dirn - 1) * d) % chips

    def arrives(dirn, d):
        return chip >= d if dirn == 0 else item_of(1, d) < far

    def goes_on(dirn, d):
        return arrives(dirn, d) & (chip < chips - 1) if dirn == 0 else arrives(dirn, d)

    def ring_copy(dirn, j, d, item, part):
        half = (dirn, 1 - dirn, None)[part]
        sem = (d - 2) * local_heads + j + (2 * local_heads if part == REST else 0)
        ref = kv.at[item, j] if half is None else kv.at[item, j, half]
        return pltpu.make_async_remote_copy(ref, ref, ring_ssem.at[dirn, local_heads if part == REST else j], ring_rsem.at[dirn, sem], device_id=device(neighbour(dirn), core))

    def outgoing(dirn, j, d, part):
        return ring_copy(dirn, j, d, item_of(dirn, d - 1), part)

    def landed(dirn, j, d, part):
        return ring_copy(dirn, j, d, item_of(dirn, d), part)

    def forward_first(j):
        for dirn in range(2):
            pl.when(goes_on(dirn, 1))(outgoing(dirn, j, 2, WHOLE).start)

    def poll_first(pair):
        for dirn in range(2):
            @pl.when(arrives(dirn, 1))
            def _():
                both = kv.at[item_of(dirn, 1), pl.ds(pair * 2, 2)]
                pltpu.make_async_remote_copy(both, both, first_ssem.at[0, 0], first_rsem.at[dirn, pair], device_id={'sp': partner}).wait_recv()

    def poll_near(s):
        j = lookup(HEAD_TABLE, s)
        d = lookup(HOP_TABLE, s) + 1
        for dirn in range(2):
            @pl.when(arrives(dirn, 2) & (d == 2))
            def _():
                landed(dirn, j, 2, WHOLE).wait_recv()

            @pl.when(goes_on(dirn, 2) & (d == 2))
            def _():
                pl.when(goes_on(dirn, 1))(outgoing(dirn, j, 2, WHOLE).wait_send)
                outgoing(dirn, j, 3, NEAR).start()
                outgoing(dirn, j, 3, REST).start()

            @pl.when(arrives(dirn, 3) & (d == 3))
            def _():
                landed(dirn, j, 3, NEAR).wait_recv()

            @pl.when(goes_on(dirn, 3) & (d == 3))
            def _():
                pl.when(goes_on(dirn, 2))(outgoing(dirn, j, 3, NEAR).wait_send)
                outgoing(dirn, j, 4, NEAR).start()

    def poll_rest(s):
        j = lookup(HEAD_TABLE, s)
        d = lookup(HOP_TABLE, s) + 1
        for dirn in range(2):
            @pl.when(arrives(dirn, 3) & (d == 3))
            def _():
                landed(dirn, j, 3, REST).wait_recv()

            @pl.when(arrives(dirn, 4) & (d == 4))
            def _():
                landed(dirn, j, 4, NEAR).wait_recv()

    def drain(j, carry):
        for dirn in range(2):
            on = [goes_on(dirn, d) for d in range(4)]
            pl.when(on[1] & jnp.logical_not(on[2]))(outgoing(dirn, j, 2, WHOLE).wait_send)
            pl.when(on[2] & jnp.logical_not(on[3]))(outgoing(dirn, j, 3, NEAR).wait_send)
            pl.when(on[3])(outgoing(dirn, j, 4, NEAR).wait_send)
        return carry

    def project_q(idx, carry):
        slot = (idx + 4) % 3
        for copy in q_copies(idx):
            copy.wait()
        raw = dot(h_buf[...].reshape(chip_rows, dim), w_buf[slot])

        @pl.when(idx == 0)
        def _():
            for copy in q_copies(3):
                copy.start()

        @pl.when(idx == local_heads - 1)
        def _():
            poll_first(0)
            forward_first(0)
            forward_first(1)

        for g in range(group):
            t = raw[:, g * head:(g + 1) * head].T
            t = t * lax.rsqrt(jnp.mean(t * t, axis=0, keepdims=True) + EPS) * gain_t[...]
            t1 = t[:half_head]
            t2 = t[half_head:]
            c = angle_t[0]
            s = angle_t[1]
            q_t[idx, :, g * chip_rows:(g + 1) * chip_rows] = jnp.concatenate([t1 * c - t2 * s, t2 * c + t1 * s], axis=0).astype(BF16)
        return carry

    lax.fori_loop(0, local_heads, project_q, 0)
    for k in range(len(stages)):
        for copy in wo_copies(k):
            copy.start()

    score_scale = (head ** -0.5) * LOG2E

    def attend(items, j, first=False, ahead=2):
        keys = [kv[item, j, :, 0].reshape(chip_rows, head) for item in items]
        vals = jnp.concatenate([kv[item, j, c, 1] for item in items for c in range(CORES)], axis=1)

        def scores_of(g):
            return [dot(k, q_t[j, :, g * chip_rows:(g + 1) * chip_rows]) for k in keys]

        pending = [scores_of(g) for g in range(ahead)]
        for g in range(group):
            cols = slice(g * chip_rows, (g + 1) * chip_rows)
            scores = pending[g]
            if first:
                key_pos = lax.broadcasted_iota(jnp.int32, scores[0].shape, 0)
                q_pos = lax.broadcasted_iota(jnp.int32, scores[0].shape, 1)
                scores = [jnp.where(key_pos <= q_pos, scores[0], -jnp.inf)]
            top = functools.reduce(jnp.maximum, [jnp.max(x.reshape(chip_rows // 8, 8, chip_rows), axis=0) for x in scores])
            top = jnp.max(top, axis=0, keepdims=True)
            if first:
                m_new = jnp.broadcast_to(top, (8, chip_rows))
            else:
                m_old = m_buf[j, :, cols]
                m_new = jnp.maximum(m_old, top)
            probs = [jnp.exp2((x.reshape(chip_rows // 8, 8, chip_rows) - m_new[None]) * score_scale) for x in scores]
            total = functools.reduce(jnp.add, [jnp.sum(p, axis=0) for p in probs])
            if g + ahead < group:
                pending.append(scores_of(g + ahead))
            mixed = dot(vals, jnp.concatenate([p.reshape(chip_rows, chip_rows).astype(BF16) for p in probs], axis=0))
            m_buf[j, :, cols] = m_new
            if first:
                l_buf[j, :, cols] = total
                o_t[j, :, cols] = mixed
            else:
                alpha = jnp.exp2((m_old - m_new) * score_scale)
                l_buf[j, :, cols] = l_buf[j, :, cols] * alpha + total
                old = o_t[j, :, cols].reshape(head // 8, 8, chip_rows)
                o_t[j, :, cols] = (old * alpha[None]).reshape(head, chip_rows) + mixed

    def diagonal(j, carry):
        @pl.when(j % 2 == 0)
        def _():
            pltpu.make_async_remote_copy(stage.at[0], kv.at[chip, pl.ds(j, 2), 1 - core], d2d_ssem.at[j // 2], d2d_rsem.at[j // 2],
                                         device_id={'sp': partner}).wait_recv()

        attend((chip,), j, first=True, ahead=group)
        return carry

    lax.fori_loop(0, local_heads, diagonal, 0)
    poll_first(1)

    def o_copy(k):
        at, size = span_of(k, core)
        target = pl.ds(pl.multiple_of(at, head), size)
        return pltpu.make_async_remote_copy(o_send.at[:, pl.ds(stages[k][0] * width, size)], o_all.at[:, target], o_ssem, o_rsem.at[k],
                                            device_id={'sp': partner})

    def close_head(j):
        k = min(j // EARLY, 1) + max(0, j - EARLY)
        at = span_of(k, core)[0] + (j - stages[k][0]) * width
        inv = 1.0 / jnp.sum(l_buf[j], axis=0, keepdims=True)
        for g in range(group):
            cols = slice(g * chip_rows, (g + 1) * chip_rows)
            o_val = (o_t[j, :, cols] * inv[:, cols]).T.astype(BF16)
            o_all[:, pl.ds(pl.multiple_of(at + g * head, head), head)] = jnp.where(core == 0, o_val[:rows], o_val[rows:])
            o_send[:, j * width + g * head:j * width + (g + 1) * head] = jnp.where(core == 0, o_val[rows:], o_val[:rows])

    def project_early(half):
        if half == 0:
            wo_wait(0)
            o_copy(0).wait_recv()
        at, size = span_of(0, 0)
        depth = slice(at, at + CORES * size)
        for n in range(dim // 2 // width):
            cols = pl.ds(half * (dim // 2) + n * width, width)
            acc[:, cols] = x_buf[:, cols].astype(F32) + dot(o_all[:, depth], wo_buf[depth, cols])

    def project_late(parts, end):
        for n in range(dim // width):
            cols = pl.ds(n * width, width)
            total = acc[:, cols]
            for k, c in parts:
                at, size = span_of(k, c)
                total = total + dot(o_all[:, pl.ds(pl.multiple_of(at, size), size)], wo_buf[pl.ds(pl.multiple_of(at, size), size), cols])
            if end:
                out_ref[:, cols] = total.astype(BF16)
            else:
                acc[:, cols] = total

    def ring_step(s, carry):
        @pl.when(s >= local_heads)
        def _():
            poll_rest(s)

        j = lookup(HEAD_TABLE, s)
        d = lookup(HOP_TABLE, s) + 1
        both = (d < far) & (chip + d >= chips)

        @pl.when(both)
        def _():
            attend((item_of(0, d), item_of(1, d)), j)

        @pl.when((chip >= d) & jnp.logical_not(both))
        def _():
            attend((item_of(0, d),), j, ahead=group)

        low = chip < LOW_CHIPS

        @pl.when(s == jnp.where(low, LOW_CLOSE, EARLY_CLOSE))
        def _():
            for early in range(EARLY):
                close_head(early)
            o_copy(0).start()

        @pl.when(s == jnp.where(low, LOW_CLOSE, THIRD_CLOSE))
        def _():
            close_head(EARLY)
            o_copy(1).start()

        @pl.when(s == jnp.where(low, LOW_CLOSE, SLOTS - 1))
        def _():
            close_head(local_heads - 1)
            o_copy(2).start()

        @pl.when((s == FIRST_POLL) | ((s + 1 > local_heads) & (s + 1 < SLOTS)))
        def _():
            poll_near(jnp.where(s == FIRST_POLL, local_heads, s + 1))

        for at, late in DEFERRED:
            @pl.when(s + 1 == at)
            def _():
                forward_first(late)

        for half in range(2):
            @pl.when(s == jnp.where(low, LOW_OUT, EARLY_OUT + half))
            def _():
                project_early(half)

        @pl.when(s == jnp.where(low, LOW_OUT, SLOTS - 1))
        def _():
            for k in (1, 2):
                wo_wait(k)
            project_late(((1, core), (2, core)), False)
            o_copy(1).wait_recv()
            project_late(((1, 1 - core),), False)
            o_copy(2).wait_recv()
            project_late(((2, 1 - core),), True)

        return carry

    lax.fori_loop(0, SLOTS, ring_step, 0)

    h_copy.wait_send()
    pltpu.make_async_remote_copy(o_send, o_all.at[:, pl.ds(0, mixed_dim)], o_ssem, o_rsem.at[0], device_id={'sp': partner}).wait_send()

    def drain_first(idx, carry):
        for copy, cond in first_copies(idx):
            pl.when(cond)(copy.wait_send)
        return carry

    lax.fori_loop(0, 4, drain_first, 0)
    lax.fori_loop(0, local_heads, drain, 0)
    for dirn in range(2):
        @pl.when(goes_on(dirn, 2))
        def _():
            rest = kv.at[item_of(dirn, 2), :, 1 - dirn]
            pltpu.make_async_remote_copy(rest, rest, ring_ssem.at[dirn, local_heads], ring_rsem.at[dirn, 0], device_id=device(neighbour(dirn), core)).wait_send()


def solution(mesh):
    group_size = mesh.shape['sp']

    def device_step(hidden, ln_gain, w_q, w_k, w_v, w_o, q_gain, k_gain):
        rows, dim = hidden.shape
        head = q_gain.shape[0]
        half = head // 2
        chips = group_size // CORES
        local_heads = w_k.shape[1] // head // CORES
        width = w_q.shape[1] // CORES // local_heads
        chip_rows = rows * CORES
        inv_freq = THETA ** -(np.arange(half, dtype=np.float64) * (2.0 / head))
        angles = inv_freq[:, None] * np.arange(rows * group_size)[None, :]
        angle_all = jnp.asarray(np.stack([np.cos(angles), np.sin(angles)]).astype(np.float32))
        hbm = pl.BlockSpec(memory_space=pl.ANY)
        dma = pltpu.SemaphoreType.DMA
        wide = width // head * chip_rows
        return pl.pallas_call(
            functools.partial(kernel, group_size),
            out_shape=pltpu.VMEM((rows, dim), BF16),
            in_specs=[hbm] * 9,
            out_specs=pl.BlockSpec(memory_space=pltpu.VMEM),
            scratch_shapes=[
                pltpu.VMEM((rows, dim), BF16),
                pltpu.VMEM((CORES, rows, dim), BF16),
                pltpu.VMEM((3, dim, width), BF16),
                pltpu.VMEM(w_o.shape, BF16),
                pltpu.VMEM((chips, local_heads, CORES, 2, rows, head), BF16),
                pltpu.VMEM((4, 2, 2, rows, head), BF16),
                pltpu.VMEM((local_heads, head, wide), BF16),
                pltpu.VMEM((local_heads, head, wide), F32),
                pltpu.VMEM((local_heads, 8, wide), F32),
                pltpu.VMEM((local_heads, 8, wide), F32),
                pltpu.VMEM((rows, w_o.shape[0]), BF16),
                pltpu.VMEM((rows, local_heads * width), BF16),
                pltpu.VMEM((rows, dim), F32),
                pltpu.VMEM((dim // LANES, LANES), BF16),
                pltpu.VMEM((2, 1, head), BF16),
                pltpu.VMEM((2, half, chip_rows), F32),
                pltpu.VMEM((head, chip_rows), F32),
                pltpu.VMEM((rows, head), F32),
                pltpu.VMEM((rows, head), F32),
                dma((4,)), dma((4,)), dma((3, 2)), dma((3,)), dma, dma,
                dma((2,)), dma((2,)),
                dma((2, 4)), dma((2, 2)),
                dma((2, local_heads + 1)), dma((2, 4 * local_heads)),
                dma, dma((3,)),
            ],
            compiler_params=pltpu.CompilerParams(collective_id=0, has_side_effects=True, vmem_limit_bytes=VMEM_LIMIT),
        )(hidden, w_q, w_k, w_v, w_o, ln_gain.reshape(-1, LANES), q_gain[None, :], k_gain[None, :], angle_all)

    row_spec = P(('dp', 'sp'), None)
    return jax.shard_map(device_step, mesh=mesh, in_specs=(row_spec, P(), P(), P(), P(), P(), P(), P()), out_specs=row_spec, check_vma=False)
```

```python
import functools
import jax
import jax.numpy as jnp
import numpy as np
from jax import lax
from jax.experimental import pallas as pl
from jax.experimental.pallas import tpu as pltpu
from jax.sharding import PartitionSpec as P

EPS = 1e-6
THETA = 1000000.0
LOG2E = 1.4426950408889634
CORES = 2
LANES = 128
VMEM_LIMIT = 62 * 2 ** 20
BF16 = jnp.bfloat16
F32 = jnp.float32


def dot(a, b):
    return jnp.dot(a, b, preferred_element_type=F32)


ORDER = ((0, 1), (1, 1), (2, 1), (3, 1), (0, 2), (1, 2), (0, 3), (1, 3), (2, 2), (0, 4), (1, 4), (3, 2), (2, 3), (3, 3), (2, 4), (3, 4))
SLOTS = len(ORDER)
EARLY = 2
FIRST_POLL = 1
FIRST_DRAIN = 8
LOW_CHIPS = 2
LOW_CLOSE = 7
LOW_OUT = 9
EARLY_CLOSE = 10
EARLY_OUT = 11
THIRD_CLOSE = 14
DEFERRED = ((5, 2), (7, 3))
NEAR, REST, WHOLE = 0, 1, 2


def slot_table(values):
    return tuple(sum(v << (2 * s) for s, v in enumerate(values[h:h + 8])) for h in (0, 8))


HEAD_TABLE = slot_table([j for j, _ in ORDER])
HOP_TABLE = slot_table([d - 1 for _, d in ORDER])


def lookup(table, s):
    return lax.shift_right_logical(jnp.where(s < 8, table[0], table[1]), 2 * (s % 8)) % 4


def kernel(group_size, x_hbm, wq, wk, wv, wo, ln_hbm, q_gain_hbm, k_gain_hbm, angle_hbm, out_ref,
           x_buf, h_buf, w_buf, wo_buf, kv, stage, q_t, o_t, m_buf, l_buf, o_all, o_send, acc,
           ln_buf, gain_buf, angle_t, gain_t, cos_k, sin_k,
           x_sem, small_sem, w_sem, wo_sem, h_ssem, h_rsem, d2d_ssem, d2d_rsem, first_ssem, first_rsem, ring_ssem, ring_rsem, o_ssem, o_rsem):
    chips = group_size // CORES
    me = lax.axis_index('sp')
    chip = me // CORES
    core = me % CORES
    partner = chip * CORES + (1 - core)
    rows, dim = x_buf.shape
    head = gain_buf.shape[2]
    half_head = head // 2
    width = w_buf.shape[2]
    local_heads = kv.shape[1]
    group = width // head
    chip_rows = rows * CORES
    far = chips // 2
    mixed_dim = local_heads * width
    lanes = ln_buf.shape[1]

    def device(c, k):
        return {'sp': c * CORES + k}

    def neighbour(dirn):
        return (chip + chips + 1 - 2 * dirn) % chips

    x_parts = x_sem.shape[0]
    part_rows = rows // x_parts

    def x_copy(r):
        sl = pl.ds(r * part_rows, part_rows)
        return pltpu.make_async_copy(x_hbm.at[sl, :], x_buf.at[sl, :], x_sem.at[r])

    chip_cols = pl.ds(pl.multiple_of(chip * chip_rows, chip_rows), chip_rows)
    small = (pltpu.make_async_copy(ln_hbm, ln_buf, small_sem.at[0]),
             pltpu.make_async_copy(q_gain_hbm, gain_buf.at[0], small_sem.at[1]),
             pltpu.make_async_copy(k_gain_hbm, gain_buf.at[1], small_sem.at[2]),
             pltpu.make_async_copy(angle_hbm.at[:, :, chip_cols], angle_t, small_sem.at[3]))

    def kv_copies(idx):
        pair = (idx % 2) * 2 + idx // 2
        cols = pl.ds(pl.multiple_of(pair * (width // 2), width // 2), width // 2)
        slot = idx % 3
        return (pltpu.make_async_copy(wk.at[:, cols], w_buf.at[slot, :, pl.ds(0, width // 2)], w_sem.at[slot, 0]),
                pltpu.make_async_copy(wv.at[:, cols], w_buf.at[slot, :, pl.ds(width // 2, width // 2)], w_sem.at[slot, 1]))

    def lead_copies(e):
        cols = pl.ds(e * head, head)
        return tuple(pltpu.make_async_copy(w.at[:, cols], w_buf.at[0, :, pl.ds((2 * e + part) * head, head)], w_sem.at[0, e])
                     for part, w in enumerate((wk, wv)))

    def lead_wait(e):
        pltpu.make_async_copy(wk.at[:, pl.ds(0, 2 * head)], w_buf.at[0, :, pl.ds(2 * e * head, 2 * head)], w_sem.at[0, e]).wait()

    def q_copies(idx):
        cols = pl.ds(pl.multiple_of((core * local_heads + idx) * width, width), width)
        slot = (idx + 4) % 3
        return tuple(pltpu.make_async_copy(wq.at[pl.ds(r * (dim // 2), dim // 2), cols],
                                           w_buf.at[slot, pl.ds(r * (dim // 2), dim // 2), :], w_sem.at[slot, r]) for r in range(2))

    stages = ((0, EARLY), (EARLY, EARLY + 1), (EARLY + 1, local_heads))

    def span_of(k, c):
        first, last = stages[k]
        return (CORES * first + c * (last - first)) * width, (last - first) * width

    def wo_copies(k):
        copies = []
        for c in range(CORES):
            at, size = span_of(k, c)
            source = pl.ds(c * mixed_dim + stages[k][0] * width, size)
            copies.append(pltpu.make_async_copy(wo.at[source, :], wo_buf.at[pl.ds(at, size), :], wo_sem))
        return copies

    def wo_wait():
        pltpu.make_async_copy(wo, wo_buf, wo_sem).wait()

    for copy in small[:1]:
        copy.start()
    for r in range(x_parts):
        x_copy(r).start()
    for copy in small[1:]:
        copy.start()
    for copy in lead_copies(0):
        copy.start()

    barrier = pltpu.get_barrier_semaphore()
    pl.semaphore_signal(barrier, inc=1, device_id={'sp': partner})
    for dirn in range(2):
        for k in range(CORES):
            pl.semaphore_signal(barrier, inc=1, device_id=device(neighbour(dirn), k))

    small[0].wait()
    for r in range(x_parts):
        if r == x_parts - 1:
            for copy in small[1:]:
                copy.wait()
            own_cols = pl.ds(pl.multiple_of(core * rows, rows), rows)
            cos_own = angle_t[0, :, own_cols].T
            sin_own = angle_t[1, :, own_cols].T
            cos_k[...] = jnp.concatenate([cos_own, cos_own], axis=1)
            sin_k[...] = jnp.concatenate([-sin_own, sin_own], axis=1)
        x_copy(r).wait()
        if r == 1:
            for copy in lead_copies(1):
                copy.start()
        if r == x_parts - 1:
            for copy in kv_copies(1):
                copy.start()
        step_rows = 16
        for t in range(part_rows // step_rows):
            sl = slice(r * part_rows + t * step_rows, r * part_rows + (t + 1) * step_rows)
            xf = x_buf[sl, :].astype(F32)
            scale = lax.rsqrt(jnp.mean(xf * xf, axis=-1, keepdims=True) + EPS)
            for b in range(dim // lanes):
                cols = slice(b * lanes, (b + 1) * lanes)
                h_buf[core, sl, cols] = (xf[:, cols] * scale * ln_buf[b:b + 1, :].astype(F32)).astype(BF16)

    h_copy = pltpu.make_async_remote_copy(h_buf.at[core], h_buf.at[core], h_ssem, h_rsem, device_id={'sp': partner})

    def first_copies(idx, e=None):
        owner = idx % 2
        pair = idx // 2
        src = stage.at[idx] if e is None else stage.at[idx, e]
        dst = kv.at[chip, pl.ds(pair * 2, 2), core] if e is None else kv.at[chip, e, core]
        up = pltpu.make_async_remote_copy(src, dst, first_ssem.at[0, idx], first_rsem.at[0, pair], device_id=device(neighbour(0), owner))
        down = pltpu.make_async_remote_copy(src, dst, first_ssem.at[1, idx], first_rsem.at[1, pair], device_id=device(neighbour(1), owner))
        across = pltpu.make_async_remote_copy(src, dst, d2d_ssem.at[pair], d2d_rsem.at[pair], device_id={'sp': partner})
        return ((up, chip < chips - 1), (down, chip < far), (across, owner != core))

    def keep_kv(idx, e, k_raw, v_raw):
        t = k_raw * lax.rsqrt(jnp.mean(k_raw * k_raw, axis=-1, keepdims=True) + EPS) * gain_buf[1].astype(F32)
        k_val = (t * cos_k[...] + pltpu.roll(t, half_head, 1) * sin_k[...]).astype(BF16)
        v_val = v_raw.T.astype(BF16)
        stage[idx, e, 0] = k_val
        stage[idx, e, 1] = v_val

        @pl.when(idx % 2 == core)
        def _():
            kv[chip, (idx // 2) * 2 + e, core, 0] = k_val
            kv[chip, (idx // 2) * 2 + e, core, 1] = v_val

    for e in range(2):
        lead_wait(e)
        both = slice(2 * e * head, 2 * (e + 1) * head)
        o_t[e, :rows, :2 * head] = dot(h_buf[core, :, :dim // 2], w_buf[0, :dim // 2, both])
        raw = dot(h_buf[core, :, dim // 2:], w_buf[0, dim // 2:, both]) + o_t[e, :rows, :2 * head]
        if e == 0:
            for copy in kv_copies(2):
                copy.start()
        keep_kv(0, e, raw[:, :head], raw[:, head:])
        if e == 0:
            pl.semaphore_wait(barrier, 1 + 2 * CORES)
        for copy, cond in first_copies(0, e):
            pl.when(cond)(copy.start)
    for copy in kv_copies(3):
        copy.start()
    h_copy.start()

    def project_kv(idx, carry):
        slot = idx % 3
        for copy in kv_copies(idx):
            copy.wait()
        raw = dot(h_buf[core], w_buf[slot])
        for copy in q_copies(idx - 1):
            copy.start()
        for e in range(2):
            keep_kv(idx, e, raw[:, e * head:(e + 1) * head], raw[:, width // 2 + e * head:width // 2 + (e + 1) * head])
        for copy, cond in first_copies(idx):
            pl.when(cond)(copy.start)
        return carry

    lax.fori_loop(1, 4, project_kv, 0)
    gain_t[...] = jnp.broadcast_to(gain_buf[0].astype(F32), (chip_rows, head)).T
    h_copy.wait_recv()

    def item_of(dirn, d):
        return (chip + chips + (2 * dirn - 1) * d) % chips

    def arrives(dirn, d):
        return chip >= d if dirn == 0 else item_of(1, d) < far

    def goes_on(dirn, d):
        return arrives(dirn, d) & (chip < chips - 1) if dirn == 0 else arrives(dirn, d)

    def ring_copy(dirn, j, d, item, part):
        half = (dirn, 1 - dirn, None)[part]
        sem = (d - 2) * local_heads + j + (2 * local_heads if part == REST else 0)
        ref = kv.at[item, j] if half is None else kv.at[item, j, half]
        return pltpu.make_async_remote_copy(ref, ref, ring_ssem.at[dirn, local_heads if part == REST else j], ring_rsem.at[dirn, sem], device_id=device(neighbour(dirn), core))

    def outgoing(dirn, j, d, part):
        return ring_copy(dirn, j, d, item_of(dirn, d - 1), part)

    def landed(dirn, j, d, part):
        return ring_copy(dirn, j, d, item_of(dirn, d), part)

    def forward_first(j):
        for dirn in range(2):
            pl.when(goes_on(dirn, 1))(outgoing(dirn, j, 2, WHOLE).start)

    def poll_first(pair):
        for dirn in range(2):
            @pl.when(arrives(dirn, 1))
            def _():
                both = kv.at[item_of(dirn, 1), pl.ds(pair * 2, 2)]
                pltpu.make_async_remote_copy(both, both, first_ssem.at[0, 0], first_rsem.at[dirn, pair], device_id={'sp': partner}).wait_recv()

    def poll_near(s):
        j = lookup(HEAD_TABLE, s)
        d = lookup(HOP_TABLE, s) + 1
        for dirn in range(2):
            @pl.when(arrives(dirn, 2) & (d == 2))
            def _():
                landed(dirn, j, 2, WHOLE).wait_recv()

            @pl.when(goes_on(dirn, 2) & (d == 2))
            def _():
                pl.when(goes_on(dirn, 1))(outgoing(dirn, j, 2, WHOLE).wait_send)
                outgoing(dirn, j, 3, NEAR).start()
                outgoing(dirn, j, 3, REST).start()

            @pl.when(arrives(dirn, 3) & (d == 3))
            def _():
                landed(dirn, j, 3, NEAR).wait_recv()

            @pl.when(goes_on(dirn, 3) & (d == 3))
            def _():
                pl.when(goes_on(dirn, 2))(outgoing(dirn, j, 3, NEAR).wait_send)
                outgoing(dirn, j, 4, NEAR).start()

    def poll_rest(s):
        j = lookup(HEAD_TABLE, s)
        d = lookup(HOP_TABLE, s) + 1
        for dirn in range(2):
            @pl.when(arrives(dirn, 3) & (d == 3))
            def _():
                landed(dirn, j, 3, REST).wait_recv()

            @pl.when(arrives(dirn, 4) & (d == 4))
            def _():
                landed(dirn, j, 4, NEAR).wait_recv()

    def drain(j, carry):
        for dirn in range(2):
            on = [goes_on(dirn, d) for d in range(4)]
            pl.when(on[1] & jnp.logical_not(on[2]))(outgoing(dirn, j, 2, WHOLE).wait_send)
            pl.when(on[2] & jnp.logical_not(on[3]))(outgoing(dirn, j, 3, NEAR).wait_send)
            pl.when(on[3])(outgoing(dirn, j, 4, NEAR).wait_send)
        return carry

    def project_q(idx, carry):
        slot = (idx + 4) % 3
        for copy in q_copies(idx):
            copy.wait()
        raw = dot(h_buf[...].reshape(chip_rows, dim), w_buf[slot])

        @pl.when(idx == 0)
        def _():
            for copy in q_copies(3):
                copy.start()

        @pl.when(idx == local_heads - 1)
        def _():
            poll_first(0)
            forward_first(0)
            forward_first(1)

        for g in range(group):
            t = raw[:, g * head:(g + 1) * head].T
            t = t * lax.rsqrt(jnp.mean(t * t, axis=0, keepdims=True) + EPS) * gain_t[...]
            t1 = t[:half_head]
            t2 = t[half_head:]
            c = angle_t[0]
            s = angle_t[1]
            q_t[idx, :, g * chip_rows:(g + 1) * chip_rows] = jnp.concatenate([t1 * c - t2 * s, t2 * c + t1 * s], axis=0).astype(BF16)
        return carry

    lax.fori_loop(0, local_heads, project_q, 0)
    for k in range(len(stages)):
        for copy in wo_copies(k):
            copy.start()

    score_scale = (head ** -0.5) * LOG2E

    def attend(items, j, first=False, ahead=2):
        keys = [kv[item, j, :, 0].reshape(chip_rows, head) for item in items]
        vals = jnp.concatenate([kv[item, j, c, 1] for item in items for c in range(CORES)], axis=1)

        def scores_of(g):
            return [dot(k, q_t[j, :, g * chip_rows:(g + 1) * chip_rows]) for k in keys]

        pending = [scores_of(g) for g in range(ahead)]
        for g in range(group):
            cols = slice(g * chip_rows, (g + 1) * chip_rows)
            scores = pending[g]
            if first:
                key_pos = lax.broadcasted_iota(jnp.int32, scores[0].shape, 0)
                q_pos = lax.broadcasted_iota(jnp.int32, scores[0].shape, 1)
                scores = [jnp.where(key_pos <= q_pos, scores[0], -jnp.inf)]
            top = functools.reduce(jnp.maximum, [jnp.max(x.reshape(chip_rows // 8, 8, chip_rows), axis=0) for x in scores])
            top = jnp.max(top, axis=0, keepdims=True)
            if first:
                m_new = jnp.broadcast_to(top, (8, chip_rows))
            else:
                m_old = m_buf[j, :, cols]
                m_new = jnp.maximum(m_old, top)
            probs = [jnp.exp2((x.reshape(chip_rows // 8, 8, chip_rows) - m_new[None]) * score_scale) for x in scores]
            total = functools.reduce(jnp.add, [jnp.sum(p, axis=0) for p in probs])
            if g + ahead < group:
                pending.append(scores_of(g + ahead))
            mixed = dot(vals, jnp.concatenate([p.reshape(chip_rows, chip_rows).astype(BF16) for p in probs], axis=0))
            m_buf[j, :, cols] = m_new
            if first:
                l_buf[j, :, cols] = total
                o_t[j, :, cols] = mixed
            else:
                alpha = jnp.exp2((m_old - m_new) * score_scale)
                l_buf[j, :, cols] = l_buf[j, :, cols] * alpha + total
                old = o_t[j, :, cols].reshape(head // 8, 8, chip_rows)
                o_t[j, :, cols] = (old * alpha[None]).reshape(head, chip_rows) + mixed

    def diagonal(j, carry):
        @pl.when(j % 2 == 0)
        def _():
            pltpu.make_async_remote_copy(stage.at[0], kv.at[chip, pl.ds(j, 2), 1 - core], d2d_ssem.at[j // 2], d2d_rsem.at[j // 2],
                                         device_id={'sp': partner}).wait_recv()

        attend((chip,), j, first=True, ahead=group)
        return carry

    lax.fori_loop(0, local_heads, diagonal, 0)
    poll_first(1)

    def o_copy(k):
        at, size = span_of(k, core)
        target = pl.ds(pl.multiple_of(at, head), size)
        return pltpu.make_async_remote_copy(o_send.at[:, pl.ds(stages[k][0] * width, size)], o_all.at[:, target], o_ssem, o_rsem.at[k],
                                            device_id={'sp': partner})

    def close_head(j):
        k = min(j // EARLY, 1) + max(0, j - EARLY)
        at = span_of(k, core)[0] + (j - stages[k][0]) * width
        inv = 1.0 / jnp.sum(l_buf[j], axis=0, keepdims=True)
        for g in range(group):
            cols = slice(g * chip_rows, (g + 1) * chip_rows)
            o_val = (o_t[j, :, cols] * inv[:, cols]).T.astype(BF16)
            o_all[:, pl.ds(pl.multiple_of(at + g * head, head), head)] = jnp.where(core == 0, o_val[:rows], o_val[rows:])
            o_send[:, j * width + g * head:j * width + (g + 1) * head] = jnp.where(core == 0, o_val[rows:], o_val[:rows])

    def project_early(half):
        if half == 0:
            wo_wait()
            o_copy(0).wait_recv()
        at, size = span_of(0, 0)
        depth = slice(at, at + CORES * size)
        for n in range(dim // 2 // width):
            cols = pl.ds(half * (dim // 2) + n * width, width)
            acc[:, cols] = x_buf[:, cols].astype(F32) + dot(o_all[:, depth], wo_buf[depth, cols])

    def project_late(parts, end):
        for n in range(dim // width):
            cols = pl.ds(n * width, width)
            total = acc[:, cols]
            for k, c in parts:
                at, size = span_of(k, c)
                total = total + dot(o_all[:, pl.ds(pl.multiple_of(at, size), size)], wo_buf[pl.ds(pl.multiple_of(at, size), size), cols])
            if end:
                out_ref[:, cols] = total.astype(BF16)
            else:
                acc[:, cols] = total

    def drain_first(idx, carry):
        for copy, cond in first_copies(idx):
            pl.when(cond)(copy.wait_send)
        return carry

    def ring_step(s, carry):
        @pl.when(s >= local_heads)
        def _():
            poll_rest(s)

        j = lookup(HEAD_TABLE, s)
        d = lookup(HOP_TABLE, s) + 1
        both = (d < far) & (chip + d >= chips)

        @pl.when(both)
        def _():
            attend((item_of(0, d), item_of(1, d)), j)

        @pl.when((chip >= d) & jnp.logical_not(both))
        def _():
            attend((item_of(0, d),), j, ahead=group)

        low = chip < LOW_CHIPS

        @pl.when(s == jnp.where(low, LOW_CLOSE, EARLY_CLOSE))
        def _():
            for early in range(EARLY):
                close_head(early)
            o_copy(0).start()

        @pl.when(s == jnp.where(low, LOW_CLOSE, THIRD_CLOSE))
        def _():
            close_head(EARLY)
            o_copy(1).start()

        @pl.when(s == jnp.where(low, LOW_CLOSE, SLOTS - 1))
        def _():
            close_head(local_heads - 1)
            o_copy(2).start()

        @pl.when((s == FIRST_POLL) | ((s + 1 > local_heads) & (s + 1 < SLOTS)))
        def _():
            poll_near(jnp.where(s == FIRST_POLL, local_heads, s + 1))

        pl.when(s == FIRST_DRAIN)(lambda: lax.fori_loop(0, 4, drain_first, None))

        for at, late in DEFERRED:
            @pl.when(s + 1 == at)
            def _():
                forward_first(late)

        for half in range(2):
            @pl.when(s == jnp.where(low, LOW_OUT, EARLY_OUT + half))
            def _():
                project_early(half)

        @pl.when(s == jnp.where(low, LOW_OUT, SLOTS - 1))
        def _():
            project_late(((1, core), (2, core)), False)
            o_copy(1).wait_recv()
            project_late(((1, 1 - core),), False)
            o_copy(2).wait_recv()
            project_late(((2, 1 - core),), True)

        return carry

    lax.fori_loop(0, SLOTS, ring_step, 0)

    h_copy.wait_send()
    pltpu.make_async_remote_copy(o_send, o_all.at[:, pl.ds(0, mixed_dim)], o_ssem, o_rsem.at[0], device_id={'sp': partner}).wait_send()

    lax.fori_loop(0, local_heads, drain, 0)
    for dirn in range(2):
        @pl.when(goes_on(dirn, 2))
        def _():
            rest = kv.at[item_of(dirn, 2), :, 1 - dirn]
            pltpu.make_async_remote_copy(rest, rest, ring_ssem.at[dirn, local_heads], ring_rsem.at[dirn, 0], device_id=device(neighbour(dirn), core)).wait_send()


def solution(mesh):
    group_size = mesh.shape['sp']

    def device_step(hidden, ln_gain, w_q, w_k, w_v, w_o, q_gain, k_gain):
        rows, dim = hidden.shape
        head = q_gain.shape[0]
        half = head // 2
        chips = group_size // CORES
        local_heads = w_k.shape[1] // head // CORES
        width = w_q.shape[1] // CORES // local_heads
        chip_rows = rows * CORES
        inv_freq = THETA ** -(np.arange(half, dtype=np.float64) * (2.0 / head))
        angles = inv_freq[:, None] * np.arange(rows * group_size)[None, :]
        angle_all = jnp.asarray(np.stack([np.cos(angles), np.sin(angles)]).astype(np.float32))
        hbm = pl.BlockSpec(memory_space=pl.ANY)
        dma = pltpu.SemaphoreType.DMA
        wide = width // head * chip_rows
        return pl.pallas_call(
            functools.partial(kernel, group_size),
            out_shape=pltpu.VMEM((rows, dim), BF16),
            in_specs=[hbm] * 9,
            out_specs=pl.BlockSpec(memory_space=pltpu.VMEM),
            scratch_shapes=[
                pltpu.VMEM((rows, dim), BF16),
                pltpu.VMEM((CORES, rows, dim), BF16),
                pltpu.VMEM((3, dim, width), BF16),
                pltpu.VMEM(w_o.shape, BF16),
                pltpu.VMEM((chips, local_heads, CORES, 2, rows, head), BF16),
                pltpu.VMEM((4, 2, 2, rows, head), BF16),
                pltpu.VMEM((local_heads, head, wide), BF16),
                pltpu.VMEM((local_heads, head, wide), F32),
                pltpu.VMEM((local_heads, 8, wide), F32),
                pltpu.VMEM((local_heads, 8, wide), F32),
                pltpu.VMEM((rows, w_o.shape[0]), BF16),
                pltpu.VMEM((rows, local_heads * width), BF16),
                pltpu.VMEM((rows, dim), F32),
                pltpu.VMEM((dim // LANES, LANES), BF16),
                pltpu.VMEM((2, 1, head), BF16),
                pltpu.VMEM((2, half, chip_rows), F32),
                pltpu.VMEM((head, chip_rows), F32),
                pltpu.VMEM((rows, head), F32),
                pltpu.VMEM((rows, head), F32),
                dma((4,)), dma((4,)), dma((3, 2)), dma, dma, dma,
                dma((2,)), dma((2,)),
                dma((2, 4)), dma((2, 2)),
                dma((2, local_heads + 1)), dma((2, 4 * local_heads)),
                dma, dma((3,)),
            ],
            compiler_params=pltpu.CompilerParams(collective_id=0, has_side_effects=True, vmem_limit_bytes=VMEM_LIMIT),
        )(hidden, w_q, w_k, w_v, w_o, ln_gain.reshape(-1, LANES), q_gain[None, :], k_gain[None, :], angle_all)

    row_spec = P(('dp', 'sp'), None)
    return jax.shard_map(device_step, mesh=mesh, in_specs=(row_spec, P(), P(), P(), P(), P(), P(), P()), out_specs=row_spec, check_vma=False)
```
